32 devices in a mesh: dp: 8 (over z, x), tensor: 4 (over y, core).
Axes of the slice: x: 2, y: 2, z: 4, core: 2. Of those that a mesh axis runs over, the one named last changes fastest.
Arguments:
- tokens: bfloat16 [32, 512, 1024], P(('dp', 'tensor')), may hold values from -6 to 6
- segments: int32 [32, 512], P(('dp', 'tensor')), may hold values from 0 to 1, as said below
- separators: int32 [32, 2], P(('dp', 'tensor')), may hold values from 2 to 511, as said below
- lengths: int32 [32], P(('dp', 'tensor')), may hold values from 128 to 512, as said below
- type_table: bfloat16 [2, 1024], replicated, may hold values from -3 to 3
- qkv_weight: bfloat16 [1024, 3072], replicated, may hold values from -0.25 to 0.25
- qv_bias: bfloat16 [2, 1024], replicated, may hold values from -3 to 3
- out_weight: bfloat16 [1024, 1024], replicated, may hold values from -0.75 to 0.75
- out_bias: bfloat16 [1024], replicated, may hold values from -3 to 3
- gain_one: float32 [1024], replicated, may hold values from 0.5 to 1.5
- shift_one: bfloat16 [1024], replicated, may hold values from -3 to 3
- in_weight: bfloat16 [1024, 4096], P(None, 'tensor'), may hold values from -0.1875 to 0.1875
- in_bias: bfloat16 [4096], P('tensor'), may hold values from -3 to 3
- ffn_weight: bfloat16 [4096, 1024], P('tensor'), may hold values from -0.09375 to 0.09375
- ffn_bias: bfloat16 [1024], replicated, may hold values from -3 to 3
- gain_two: float32 [1024], replicated, may hold values from 0.5 to 1.5
- shift_two: bfloat16 [1024], replicated, may hold values from -3 to 3
- cotangent: bfloat16 [32, 512, 1024], P(('dp', 'tensor')), may hold values from -6 to 6
Outputs:
- activations: bfloat16 [32, 512, 1024], P(('dp', 'tensor'))
- tokens_grad: float32 [32, 512, 1024], P(('dp', 'tensor'))
- qv_bias_grad: float32 [2, 1024], replicated
- out_bias_grad: float32 [1024], replicated
- shift_one_grad: float32 [1024], replicated
- in_bias_grad: float32 [4096], P('tensor')
- ffn_bias_grad: float32 [1024], replicated
- shift_two_grad: float32 [1024], replicated
The draws below stay inside these ranges and needn't reach their ends.
Inputs may be any that keep to these rules, and one draw needn't show every extreme that they name: `lengths`: some pair has exactly 512 real tokens. `separators`: column 0 is the first separator, from 2 to the pair's length minus 3; column 1 is the pair's length minus 1. `segments`: 0 up to and including the first separator and at padded positions, 1 after it up to the pair's length minus 1.
All inputs are finite; a program needn't handle non-finite values.
Results may differ from the reference program's by a relative error of at most 0.014.
The reference program's roundings to bfloat16 on the way count: a program that leaves them out, or rounds other values in their place, can miss the bound.
Values may be sent and summed in bfloat16 or wider, within the bound.
A program may use at most 128 MiB of HBM per device.

```python
import jax
import jax.numpy as jnp
from jax import lax

D = 1024
HEADS = 16
FF = 4096
SEQ = 512
PAIRS = 32


def pair_layout(key):
    length_key = jax.random.fold_in(key, 101)
    full_key = jax.random.fold_in(key, 202)
    split_key = jax.random.fold_in(key, 303)
    lengths = jax.random.randint(length_key, (PAIRS,), SEQ // 4, SEQ + 1)
    full = jax.random.randint(full_key, (), 0, PAIRS)
    lengths = jnp.where(jnp.arange(PAIRS) == full, SEQ, lengths).astype(jnp.int32)
    first_end = jax.random.randint(split_key, (PAIRS,), 2, lengths - 2).astype(jnp.int32)
    separators = jnp.stack([first_end, lengths - 1], axis=1).astype(jnp.int32)
    positions = jnp.arange(SEQ).astype(jnp.int32)[None, :]
    segments = ((positions > first_end[:, None]) & (positions < lengths[:, None])).astype(jnp.int32)
    return (lengths, separators, segments)


def draw_lengths(key, part):
    return pair_layout(key)[0]


def draw_separators(key, part):
    return pair_layout(key)[1]


def draw_segments(key, part):
    return pair_layout(key)[2]


def steps_of(key, shape, cuts, low, high):
    loudness, own = 1.0, jax.random.fold_in(key, 6)
    for dim, shards_of in cuts:
        steps = jnp.exp(jax.random.uniform(jax.random.fold_in(own, dim), (shards_of,), jnp.float32, low / len(cuts), high / len(cuts)))
        loudness = loudness * jnp.repeat(steps, shape[dim] // shards_of).reshape([-1 if axis == dim else 1 for axis in range(len(shape))])
    return loudness


def bell_draw(stream_key, dims, deviation, limit, shards=(), held_as=jnp.bfloat16):
    entries = deviation * jax.random.normal(stream_key, dims, jnp.float32)
    if shards:
        entries = entries * steps_of(stream_key, dims, shards, -0.22, 0.18)
    return jnp.clip(entries, -limit, limit).astype(held_as)


def setup_inputs(seed: int = 0) -> dict:
    splits = jax.random.split(jax.random.key(seed), 19)
    tokens = bell_draw(splits[0], (PAIRS, SEQ, D), 1.0, 6.0, ((0, 32),))
    segments = draw_segments(jax.random.fold_in(splits[18], 71), 0)
    separators = draw_separators(jax.random.fold_in(splits[18], 71), 0)
    lengths = draw_lengths(jax.random.fold_in(splits[18], 71), 0)
    type_table = bell_draw(splits[4], (2, D), 0.5, 3.0)
    qkv_weight = bell_draw(splits[5], (D, 3 * D), (D // 2) ** -0.5, 0.25)
    qv_bias = bell_draw(splits[6], (2, D), 0.5, 3.0)
    out_weight = bell_draw(splits[7], (D, D), (D // 16) ** -0.5, 0.75)
    out_bias = bell_draw(splits[8], (D,), 0.5, 3.0)
    gain_one = jnp.clip(1.0 + 0.1 * jax.random.normal(splits[9], (D,), jnp.float32), 0.5, 1.5)
    shift_one = bell_draw(splits[10], (D,), 0.5, 3.0)
    in_weight = bell_draw(splits[11], (D, FF), D ** -0.5, 0.1875, ((1, 4),))
    in_bias = bell_draw(splits[12], (FF,), 0.5, 3.0, ((0, 4),))
    ffn_weight = bell_draw(splits[13], (FF, D), FF ** -0.5, 0.09375, ((0, 4),))
    ffn_bias = bell_draw(splits[14], (D,), 0.5, 3.0)
    gain_two = jnp.clip(1.0 + 0.1 * jax.random.normal(splits[15], (D,), jnp.float32), 0.5, 1.5)
    shift_two = bell_draw(splits[16], (D,), 0.5, 3.0)
    cotangent = bell_draw(splits[17], (PAIRS, SEQ, D), 1.0, 6.0, ((0, 32),))
    return dict(tokens=tokens, segments=segments, separators=separators, lengths=lengths, type_table=type_table, qkv_weight=qkv_weight, qv_bias=qv_bias, out_weight=out_weight, out_bias=out_bias, gain_one=gain_one, shift_one=shift_one, in_weight=in_weight, in_bias=in_bias, ffn_weight=ffn_weight, ffn_bias=ffn_bias, gain_two=gain_two, shift_two=shift_two, cotangent=cotangent)


@jax.custom_vjp
def low(v):
    return lax.optimization_barrier(v.astype(jnp.bfloat16)).astype(jnp.float32)

@jax.custom_vjp
def low_back(v):
    return v

def low_keep(v):
    return (low(v), None)

def low_pass(kept, grad):
    return (grad,)

def back_keep(v):
    return (v, None)

def back_low(kept, grad):
    return (low(grad),)
low.defvjp(low_keep, low_pass)
low_back.defvjp(back_keep, back_low)
highest = lax.Precision.HIGHEST
root_half = 0.7071067811865476
eps_norm = 1e-06

def gelu_erf(value):
    return 0.5 * value * (1.0 + jax.scipy.special.erf(value * root_half))

def normalize(rows, gain, shift):
    centered = rows - lax.optimization_barrier(jnp.mean(rows, axis=-1, keepdims=True))
    spread = lax.optimization_barrier(jnp.mean(centered * centered, axis=-1, keepdims=True))
    return centered * lax.rsqrt(spread + eps_norm) * gain + shift

def attend_pair(items):
    query, key_rows, value, valid = items
    scale = query.shape[-1] ** (-0.5)
    scores = low_back(scale * jnp.einsum('qhd,khd->hqk', query, key_rows, precision=highest))
    scores = jnp.where(valid[None, None, :], scores, -1e+30)
    top = lax.optimization_barrier(jnp.max(scores, axis=-1, keepdims=True))
    total_log = top + jnp.log(lax.optimization_barrier(jnp.sum(jnp.exp(scores - top), axis=-1, keepdims=True)))
    probs = jnp.exp(scores - total_log)
    return jnp.einsum('hqk,khd->qhd', low(probs), value, precision=highest)

def forward(rows, biases, segments, lengths, weights):
    qv_bias, out_bias, shift_one, in_bias, ffn_bias, shift_two = biases
    type_table, qkv_weight, out_weight, gain_one, in_weight, ffn_weight, gain_two = weights
    pairs, seq, width = rows.shape
    second = segments.astype(jnp.float32)[..., None]
    embedded = (rows + (1.0 - second) * type_table[0] + second * type_table[1]).reshape(-1, width)
    packed = jnp.dot(low(embedded), qkv_weight, precision=highest)
    query = low_back(low(packed[:, :width] + qv_bias[0]))
    key_rows = low_back(low(packed[:, width:2 * width]))
    value = low_back(low(packed[:, 2 * width:] + qv_bias[1]))
    shaped = (pairs, seq, HEADS, width // HEADS)
    positions = jnp.arange(seq).astype(jnp.int32)
    valid = positions[None, :] < lengths[:, None]
    mixed = lax.map(jax.checkpoint(attend_pair), (query.reshape(shaped), key_rows.reshape(shaped), value.reshape(shaped), valid))
    mixed = low_back(low(mixed.reshape(-1, width)))
    branch = low_back(jnp.dot(mixed, out_weight, precision=highest) + out_bias)
    first = normalize(embedded + branch, gain_one, shift_one)
    inner = low_back(jnp.dot(low(first), in_weight, precision=highest) + in_bias)
    outer = low_back(jnp.dot(low(gelu_erf(inner)), ffn_weight, precision=highest) + ffn_bias)
    return normalize(first + outer, gain_two, shift_two).reshape(pairs, seq, width)

def keep_mask(lengths, separators, seq):
    positions = jnp.arange(seq).astype(jnp.int32)[None, :]
    keep = (positions < lengths[:, None]) & (positions > 0)
    keep = keep & (positions != separators[:, 0:1]) & (positions != separators[:, 1:2])
    return keep.astype(jnp.float32)

def reference(tokens, segments, separators, lengths, type_table, qkv_weight, qv_bias, out_weight, out_bias, gain_one, shift_one, in_weight, in_bias, ffn_weight, ffn_bias, gain_two, shift_two, cotangent):
    weights = tuple((item.astype(jnp.float32) for item in (type_table, qkv_weight, out_weight, gain_one, in_weight, ffn_weight, gain_two)))
    biases = tuple((item.astype(jnp.float32) for item in (qv_bias, out_bias, shift_one, in_bias, ffn_bias, shift_two)))
    group = 8 if PAIRS % 8 == 0 else 1
    count = PAIRS // group

    def split(array):
        return array.reshape((count, group) + array.shape[1:])

    def step(totals, items):
        rows, segs, lens, seps, grads = items

        def local(rows_in, bias_in):
            return forward(rows_in, bias_in, segs, lens, weights)
        result, pullback = jax.vjp(local, rows.astype(jnp.float32), biases)
        mask = keep_mask(lens, seps, SEQ)
        grad_rows, grad_biases = pullback(grads.astype(jnp.float32) * mask[..., None])
        totals = jax.tree.map(jnp.add, totals, grad_biases)
        return (totals, (result.astype(jnp.bfloat16), grad_rows))
    zeros = tuple((jnp.zeros(item.shape, jnp.float32) for item in biases))
    totals, (outputs, grad_tokens) = lax.scan(step, zeros, (split(tokens), split(segments), split(lengths), split(separators), split(cotangent)))
    activations = outputs.reshape(PAIRS, SEQ, D)
    tokens_grad = grad_tokens.reshape(PAIRS, SEQ, D)
    return (activations, tokens_grad, totals[0], totals[1], totals[2], totals[3], totals[4], totals[5])
```

```python
import jax
import jax.numpy as jnp
from jax import lax
from jax.sharding import PartitionSpec as P

HEADS = 16


root_half = 0.7071067811865476
inv_root_tau = 0.3989422804014327
eps_norm = 1e-06


def gelu_erf(value):
    return 0.5 * value * (1.0 + jax.scipy.special.erf(value * root_half))


def gelu_slope(value):
    return 0.5 * (1.0 + jax.scipy.special.erf(value * root_half)) + value * inv_root_tau * jnp.exp(
        -0.5 * value * value
    )


def norm_forward(rows, gain, shift):
    centered = rows - jnp.mean(rows, axis=-1, keepdims=True)
    scale = lax.rsqrt(jnp.mean(centered * centered, axis=-1, keepdims=True) + eps_norm)
    normed = centered * scale
    return (normed * gain + shift, normed, scale)


def norm_backward(grad, normed, scale, gain):
    scaled = grad * gain
    centered = scaled - jnp.mean(scaled, axis=-1, keepdims=True)
    return scale * (centered - normed * jnp.mean(scaled * normed, axis=-1, keepdims=True))


def masked_scores(query, key_rows, valid):
    scale = query.shape[-1] ** (-0.5)
    scores = scale * jnp.einsum("qhd,khd->hqk", query, key_rows, preferred_element_type=jnp.float32)
    return jnp.where(valid[None, None, :], scores, -1e30)


def attend_forward(items):
    query, key_rows, value, valid = items
    scores = masked_scores(query, key_rows, valid)
    top = jnp.max(scores, axis=-1, keepdims=True)
    total_log = top + jnp.log(jnp.sum(jnp.exp(scores - top), axis=-1, keepdims=True))
    probs = jnp.exp(scores - total_log).astype(jnp.bfloat16)
    mixed = jnp.einsum("hqk,khd->qhd", probs, value, preferred_element_type=jnp.float32)
    return (mixed.astype(jnp.bfloat16), total_log)


def attend_backward(items):
    query, key_rows, value, valid, total_log, grad_mixed = items
    scale = query.shape[-1] ** (-0.5)
    probs = jnp.exp(masked_scores(query, key_rows, valid) - total_log)
    grad_probs = jnp.einsum("qhd,khd->hqk", grad_mixed, value, preferred_element_type=jnp.float32)
    inner_sum = jnp.sum(probs * grad_probs, axis=-1, keepdims=True)
    grad_scores = (probs * (grad_probs - inner_sum)).astype(jnp.bfloat16)
    grad_query = scale * jnp.einsum(
        "hqk,khd->qhd", grad_scores, key_rows, preferred_element_type=jnp.float32
    )
    grad_keys = scale * jnp.einsum(
        "hqk,qhd->khd", grad_scores, query, preferred_element_type=jnp.float32
    )
    grad_values = jnp.einsum(
        "hqk,qhd->khd", probs.astype(jnp.bfloat16), grad_mixed, preferred_element_type=jnp.float32
    )
    return (
        grad_query.astype(jnp.bfloat16),
        grad_keys.astype(jnp.bfloat16),
        grad_values.astype(jnp.bfloat16),
    )


def local(
    tokens,
    segments,
    separators,
    lengths,
    type_table,
    qkv_weight,
    qv_bias,
    out_weight,
    out_bias,
    gain_one,
    shift_one,
    in_weight,
    in_bias,
    ffn_weight,
    ffn_bias,
    gain_two,
    shift_two,
    cotangent,
):
    pairs, seq, width = tokens.shape
    flat = pairs * seq
    second = segments.astype(jnp.float32)[..., None]
    table = type_table.astype(jnp.float32)
    embedded = (tokens.astype(jnp.float32) + (1.0 - second) * table[0] + second * table[1]).reshape(
        flat, width
    )
    in_full = lax.all_gather(in_weight, "tensor", axis=1, tiled=True)
    ffn_full = lax.all_gather(ffn_weight, "tensor", axis=0, tiled=True)
    bias_full = lax.all_gather(in_bias, "tensor", axis=0, tiled=True)
    packed = jnp.dot(embedded.astype(jnp.bfloat16), qkv_weight, preferred_element_type=jnp.float32)
    attn_bias = qv_bias.astype(jnp.float32)
    query = (packed[:, :width] + attn_bias[0]).astype(jnp.bfloat16)
    key_rows = packed[:, width : 2 * width].astype(jnp.bfloat16)
    value = (packed[:, 2 * width :] + attn_bias[1]).astype(jnp.bfloat16)
    shaped = (pairs, seq, HEADS, width // HEADS)
    query = query.reshape(shaped)
    key_rows = key_rows.reshape(shaped)
    value = value.reshape(shaped)
    positions = jnp.arange(seq, dtype=jnp.int32)
    valid = positions[None, :] < lengths[:, None]
    mixed, total_log = lax.map(attend_forward, (query, key_rows, value, valid))
    mixed = mixed.reshape(flat, width)
    branch = jnp.dot(mixed, out_weight, preferred_element_type=jnp.float32) + out_bias.astype(
        jnp.float32
    )
    first, normed_one, scale_one = norm_forward(
        embedded + branch, gain_one, shift_one.astype(jnp.float32)
    )
    first_low = first.astype(jnp.bfloat16)
    in_shift = bias_full.astype(jnp.float32)
    inner = (
        jnp.einsum(
            "psd,df->psf",
            first_low.reshape(pairs, seq, width),
            in_full,
            preferred_element_type=jnp.float32,
        )
        + in_shift
    )
    hidden = gelu_erf(inner).astype(jnp.bfloat16)
    rows = hidden
    outer = jnp.einsum("psf,fd->psd", rows, ffn_full, preferred_element_type=jnp.float32).reshape(
        flat, width
    )
    final, normed_two, scale_two = norm_forward(
        first + outer + ffn_bias.astype(jnp.float32), gain_two, shift_two.astype(jnp.float32)
    )
    activations = final.astype(jnp.bfloat16).reshape(pairs, seq, width)
    keep = valid & (positions[None, :] > 0)
    keep = (
        keep
        & (positions[None, :] != separators[:, 0:1])
        & (positions[None, :] != separators[:, 1:2])
    )
    grad_final = (cotangent.astype(jnp.float32) * keep.astype(jnp.float32)[..., None]).reshape(
        flat, width
    )
    grad_shift_two = jnp.sum(grad_final, axis=0)
    grad_second = norm_backward(grad_final, normed_two, scale_two, gain_two)
    grad_ffn = grad_second.astype(jnp.bfloat16)
    grad_ffn_bias = jnp.sum(grad_ffn.astype(jnp.float32), axis=0)
    back = jnp.einsum(
        "psd,fd->psf",
        grad_ffn.reshape(pairs, seq, width),
        ffn_full,
        preferred_element_type=jnp.float32,
    )
    grad_inner = (back * gelu_slope(inner)).astype(jnp.bfloat16)
    grad_in_part = jnp.sum(grad_inner.astype(jnp.float32), axis=(0, 1))
    rows = grad_inner
    grad_first = jnp.einsum(
        "psf,df->psd", rows, in_full, preferred_element_type=jnp.float32
    ).reshape(flat, width)
    grad_first = grad_first + grad_second
    grad_shift_one = jnp.sum(grad_first, axis=0)
    grad_sum_one = norm_backward(grad_first, normed_one, scale_one, gain_one)
    grad_branch = grad_sum_one.astype(jnp.bfloat16)
    grad_out_bias = jnp.sum(grad_branch.astype(jnp.float32), axis=0)
    grad_mixed = jnp.einsum(
        "ne,de->nd", grad_branch, out_weight, preferred_element_type=jnp.float32
    ).astype(jnp.bfloat16)
    grad_query, grad_keys, grad_values = lax.map(
        attend_backward, (query, key_rows, value, valid, total_log, grad_mixed.reshape(shaped))
    )
    grad_query = grad_query.reshape(flat, width)
    grad_keys = grad_keys.reshape(flat, width)
    grad_values = grad_values.reshape(flat, width)
    grad_packed = jnp.concatenate([grad_query, grad_keys, grad_values], axis=1)
    tokens_grad = (
        jnp.einsum("nc,dc->nd", grad_packed, qkv_weight, preferred_element_type=jnp.float32)
        + grad_sum_one
    )
    grad_qv = jnp.stack(
        [
            jnp.sum(grad_query.astype(jnp.float32), axis=0),
            jnp.sum(grad_values.astype(jnp.float32), axis=0),
        ]
    )
    totals = lax.psum(
        (grad_qv, grad_out_bias, grad_shift_one, grad_ffn_bias, grad_shift_two, grad_in_part),
        ("dp", "tensor"),
    )
    units = in_bias.shape[0]
    grad_in_bias = lax.dynamic_slice_in_dim(
        totals[5], lax.axis_index("tensor") * units, units, axis=0
    )
    return (
        activations,
        tokens_grad.reshape(pairs, seq, width),
        totals[0],
        totals[1],
        totals[2],
        grad_in_bias,
        totals[3],
        totals[4],
    )


def solution(mesh):
    return jax.shard_map(
        local,
        mesh=mesh,
        in_specs=(
            P(("dp", "tensor"), None, None),
            P(("dp", "tensor"), None),
            P(("dp", "tensor"), None),
            P(("dp", "tensor")),
            P(),
            P(),
            P(),
            P(),
            P(),
            P(),
            P(),
            P(None, "tensor"),
            P("tensor"),
            P("tensor", None),
            P(),
            P(),
            P(),
            P(("dp", "tensor"), None, None),
        ),
        out_specs=(
            P(("dp", "tensor"), None, None),
            P(("dp", "tensor"), None, None),
            P(),
            P(),
            P(),
            P("tensor"),
            P(),
            P(),
        ),
        check_vma=False,
    )
```

```python
import functools

import jax
import jax.numpy as jnp
from jax import lax
from jax.experimental import pallas as pl
from jax.experimental.pallas import tpu as pltpu
from jax.sharding import PartitionSpec as P

HEADS = 16
TILE = 256
LANES = 128
BLOCK = 64
F32 = jnp.float32
BF16 = jnp.bfloat16
MESH = pl.DeviceIdType.MESH
NT = (((1,), (1,)), ((), ()))
root_half = 0.7071067811865476
inv_root_tau = 0.3989422804014327
eps_norm = 1e-06
STOP = 99


def dot(a, b):
    return jnp.dot(a, b, preferred_element_type=F32)


def dot_nt(a, b):
    return lax.dot_general(a, b, NT, preferred_element_type=F32)


def mean_rows(value):
    return jnp.sum(value, axis=-1, keepdims=True) * (1.0 / value.shape[-1])


def cols(n, size=TILE):
    return pl.ds(pl.multiple_of(n * size, size), size)


def fold8(value):
    return jnp.sum(value.reshape(value.shape[0] // 8, 8, value.shape[1]), axis=0)


def total8(value):
    return jnp.sum(value, axis=0, keepdims=True)


def flip(index, bit):
    return index + bit * (1 - 2 * (index // bit % 2))


def kernel(
    ranks, group,
    lengths, separators, small, in_b, tokens, cot, qkv_w, out_w, in_w, ffn_w,
    act_out, grad_out, qv_out, outb_out, shift1_out, inb_out, ffnb_out, shift2_out,
    qkvw, outw, inw, ffw, inb, q, k, v, pt, slope, hid, a0, a1, f0, f1, f2, tok, cotb, act, sc1, cs, csqv,
    ginb, rinb, ibuf, irec, tsum, sbuf, srec, tqv, qbuf, qrec,
    wsem, lsem, send, recv,
):
    rows, width = tok.shape
    tiles = width // TILE
    hd = width // HEADS
    chunks = inw.shape[0]
    units = in_w.shape[1]
    part = units // 4
    line = group // 2
    brow = units // LANES
    prow = part // LANES
    per = units // TILE
    length = lengths[0]
    sep0, sep1 = separators[0, 0], separators[0, 1]
    dp, tensor = lax.axis_index("dp"), lax.axis_index("tensor")
    y, core = tensor // 2, tensor % 2
    bits = [1 << b for b in range(ranks.bit_length() - 1)]

    def place(d, other):
        return (dp, (y + d + line) % line * 2 + (core + other) % 2)

    def rank(bit):
        return (flip(dp, bit), tensor)

    barrier = pltpu.get_barrier_semaphore()
    friends = [place(s // 2, s % 2) for s in range(1, group)] + [rank(b) for b in bits]
    for f in friends:
        pl.semaphore_signal(barrier, inc=1, device_id=f, device_id_type=MESH)

    count = [0]

    def remote(src, dst, device):
        i = count[0]
        count[0] += 1
        return pltpu.make_async_remote_copy(
            src_ref=src, dst_ref=dst, send_sem=send.at[i], recv_sem=recv.at[i], device_id=device, device_id_type=MESH
        )

    def natural(p):
        return (p + dp) % 2 + (p // 2 + dp // 2) % 2 * 2

    def piece(slot, p, i):
        u = slot * units + p * part
        if i < 2:
            return inw.at[u // TILE, pl.ds(i * width // 2, width // 2), pl.ds(u % TILE, part)]
        return ffw.at[pl.ds(u + (i - 2) * part // 2, part // 2), :]

    def source(p, i):
        u = pl.multiple_of(natural(p) * part, part)
        if i < 2:
            return in_w.at[pl.ds(i * width // 2, width // 2), pl.ds(u, part)]
        return ffn_w.at[pl.ds(u + (i - 2) * part // 2, part // 2), :]

    def load(i, src, dst):
        c = pltpu.make_async_copy(src, dst, lsem.at[i])
        c.start()
        return c

    c_tok = load(0, tokens, tok)
    c_qkv = []
    for n in range(3 * tiles):
        c = pltpu.make_async_copy(qkv_w.at[:, n * TILE : (n + 1) * TILE], qkvw.at[n], wsem.at[n])
        c.start()
        c_qkv.append(c)
    c_in = []
    for n in range(per):
        c = pltpu.make_async_copy(in_w.at[:, n * TILE : (n + 1) * TILE], inw.at[n], wsem.at[3 * tiles + n])
        c.start()
        c_in.append(c)
    c_out = load(1, out_w, outw)
    c_ffn = load(2, ffn_w, ffw.at[pl.ds(0, units), :])
    c_b = load(3, in_b, inb.at[pl.ds(0, brow)])
    c_cot = load(4, cot, cotb)

    far = range(1, line)
    direct = {d: [remote(source(p, i), piece(2 * d, p, i), place(-d, 0)) for p, i in ((0, 0), (0, 1), (0, 2), (0, 3), (3, 2), (3, 3))] for d in far}
    to_x = {d: [remote(piece(2 * d, p, i), piece(2 * d, p + 1, i), rank(1)) for p, i in ((0, 0), (0, 1), (0, 2), (0, 3), (2, 0))] for d in far}
    to_z = {d: [remote(piece(2 * d, p, i), piece(2 * d, p + 2, i), rank(2)) for p, i in ((0, 0), (0, 1), (0, 2), (0, 3), (1, 1))] for d in far}
    pass_on = {d: {(p, i): remote(piece(2 * d, p, i), piece(2 * d + 1, p, i), place(0, 1)) for p in range(4) for i in range(4)} for d in far}
    core_in = [remote(in_w.at[:, n * TILE : (n + 1) * TILE], inw.at[per + n], place(0, 1)) for n in range(per)]
    core_ffn = remote(ffn_w, ffw.at[pl.ds(units, units), :], place(0, 1))
    bias = [remote(in_b, inb.at[pl.ds(s * brow, brow)], place(-(s // 2), s % 2)) for s in range(1, group)]

    def relay(step):
        for d in far:
            yd, xd, zd, on = direct[d], to_x[d], to_z[d], pass_on[d]
            if step < 4:
                yd[step].wait_recv()
                xd[step].start()
                zd[step].start()
                on[0, step].start()
            if step == 1:
                zd[0].wait_recv()
                xd[4].start()
                on[2, 0].start()
                xd[0].wait_recv()
                on[1, 0].start()
            if step == 2:
                xd[1].wait_recv()
                zd[4].start()
                on[1, 1].start()
                zd[1].wait_recv()
                on[2, 1].start()
            if step == 3:
                xd[4].wait_recv()
                on[3, 0].start()
                zd[4].wait_recv()
                on[3, 1].start()
            if step >= 4:
                yd[step].wait_recv()
                on[3, step - 2].start()
                xd[step - 2].wait_recv()
                on[1, step - 2].start()
                zd[step - 2].wait_recv()
                on[2, step - 2].start()

    c_tok.wait()

    @pl.loop(0, rows // BLOCK)
    def _(i):
        r = cols(i, BLOCK)
        pos = lax.broadcasted_iota(jnp.int32, (BLOCK, width), 0) + i * BLOCK
        second = (pos > sep0) & (pos < length)
        e = tok[r, :].astype(F32) + jnp.where(second, small[1:2, :], small[0:1, :])
        f0[r, :] = e
        a0[r, :] = e.astype(BF16)

    pl.semaphore_wait(barrier, len(friends))
    for d in far:
        for c in direct[d]:
            c.start()
    for c in core_in + [core_ffn] + bias:
        c.start()

    for c in c_qkv:
        c.wait()

    @pl.loop(0, tiles)
    def _(n):
        q[n] = (dot(a0[...], qkvw[n]) + small[2:3, cols(n)]).astype(BF16) * jnp.asarray(hd**-0.5, BF16)

    @pl.loop(0, tiles)
    def _(n):
        k[n] = dot(a0[...], qkvw[n + tiles]).astype(BF16)

    @pl.loop(0, tiles)
    def _(n):
        v[n] = (dot(a0[...], qkvw[n + 2 * tiles]) + small[3:4, cols(n)]).astype(BF16)

    relay(0)

    low_half = lax.broadcasted_iota(jnp.int32, (rows, LANES), 1) < hd
    zero = jnp.zeros((rows, LANES), BF16)
    heads = TILE // hd

    def halves(pair):
        return jnp.where(low_half, pair, zero), jnp.where(low_half, zero, pair)

    @pl.loop(0, tiles)
    def _(n):
        vt = v[n].T
        outs = []
        for p in range(TILE // LANES):
            k2 = k[n, :, p * LANES : (p + 1) * LANES]
            for e, qm in enumerate(halves(q[n, :, p * LANES : (p + 1) * LANES])):
                h = 2 * p + e
                s = dot_nt(k2, qm)
                kpos = lax.broadcasted_iota(jnp.int32, s.shape, 0)
                s = jnp.where(kpos < length, s, -1e30)
                top = jnp.max(s, axis=0, keepdims=True)
                ex = jnp.exp(s - top)
                prob = (ex * (1.0 / jnp.sum(ex, axis=0, keepdims=True))).astype(BF16)
                pt[n * heads + h] = prob
                outs.append(dot(vt[h * hd : (h + 1) * hd], prob))
        a1[:, cols(n)] = jnp.concatenate(outs, axis=0).astype(BF16).T

        @pl.when(n == tiles // 2)
        def _():
            relay(1)

    c_out.wait()

    @pl.loop(0, tiles)
    def _(n):
        f1[:, cols(n)] = dot(a1[...], outw[:, cols(n)]) + small[4:5, cols(n)] + f0[:, cols(n)]

    @pl.loop(0, rows // BLOCK)
    def _(i):
        r = cols(i, BLOCK)
        x = f1[r, :]
        x = x - mean_rows(x)
        scale = lax.rsqrt(mean_rows(x * x) + eps_norm)
        normed = x * scale
        f0[r, :] = normed
        a0[r, :] = (normed * small[5:6, :] + small[6:7, :]).astype(BF16)
        sc1[r, :] = jnp.broadcast_to(scale, (BLOCK, LANES))

    relay(2)

    def hidden_units(c, first, second):
        x = dot(a0[...], inw[c]) + jnp.concatenate([inb[first], inb[second]], axis=1)
        cdf = 0.5 * (1.0 + lax.erf(x * root_half))
        hid[c] = (x * cdf).astype(BF16)
        slope[c] = cdf + x * (inv_root_tau * jnp.exp(-0.5 * x * x))

    for c in c_in + [c_b]:
        c.wait()
    for c in core_in + bias:
        c.wait_recv()

    @pl.loop(0, 2 * per)
    def _(c):
        hidden_units(c, 2 * c, 2 * c + 1)

    relay(3)
    for d in far:
        for p in range(4):
            pass_on[d][p, 0].wait_recv()
            pass_on[d][p, 1].wait_recv()

    def shuffled(r):
        return r // brow * brow + natural(r % brow // prow) * prow + r % prow

    @pl.loop(2 * per, chunks)
    def _(c):
        hidden_units(c, shuffled(2 * c), shuffled(2 * c + 1))

    relay(4)
    c_ffn.wait()
    core_ffn.wait_recv()

    @pl.loop(0, tiles)
    def _(t):
        acc = dot(hid[0], ffw[0:TILE, cols(t)])
        for c in range(1, 2 * per):
            acc += dot(hid[c], ffw[c * TILE : (c + 1) * TILE, cols(t)])
        f1[:, cols(t)] = acc

    relay(5)
    for d in far:
        for p in range(4):
            pass_on[d][p, 2].wait_recv()
            pass_on[d][p, 3].wait_recv()

    @pl.loop(0, tiles)
    def _(t):
        acc = f1[:, cols(t)]
        for c in range(2 * per, chunks):
            acc += dot(hid[c], ffw[c * TILE : (c + 1) * TILE, cols(t)])
        f1[:, cols(t)] = acc

    c_cot.wait()
    cs[...] = jnp.zeros_like(cs)

    @pl.loop(0, rows // BLOCK)
    def _(i):
        r = cols(i, BLOCK)
        pos = lax.broadcasted_iota(jnp.int32, (BLOCK, width), 0) + i * BLOCK
        keep = (pos > 0) & (pos < length) & (pos != sep0) & (pos != sep1)
        x = f0[r, :] * small[5:6, :] + small[6:7, :] + f1[r, :] + small[7:8, :]
        x = x - mean_rows(x)
        scale = lax.rsqrt(mean_rows(x * x) + eps_norm)
        normed = x * scale
        act[r, :] = (normed * small[8:9, :] + small[9:10, :]).astype(BF16)
        g = jnp.where(keep, cotb[r, :].astype(F32), 0.0)
        s = g * small[8:9, :]
        gs = scale * (s - mean_rows(s) - normed * mean_rows(s * normed))
        low = gs.astype(BF16)
        f2[r, :] = gs
        a1[r, :] = low
        cs[0] += fold8(g)
        cs[1] += fold8(low.astype(F32))

    c_act = load(5, act, act_out)

    @pl.loop(0, chunks)
    def _(c):
        gi = (dot_nt(a1[...], ffw[cols(c), :]) * slope[c]).astype(BF16)
        hid[c] = gi
        s = total8(gi.astype(F32))
        ginb[2 * c] = s[:, :LANES]
        ginb[2 * c + 1] = s[:, LANES:]

    @pl.loop(0, tiles)
    def _(t):
        acc = dot_nt(hid[0], inw[0, cols(t), :])
        for c in range(1, chunks):
            acc += dot_nt(hid[c], inw[c, cols(t), :])
        f1[:, cols(t)] = acc

    @pl.loop(0, rows // BLOCK)
    def _(i):
        r = cols(i, BLOCK)
        g = f1[r, :] + f2[r, :]
        s = g * small[5:6, :]
        normed = f0[r, :]
        gs = sc1[r, 0:1] * (s - mean_rows(s) - normed * mean_rows(s * normed))
        low = gs.astype(BF16)
        f2[r, :] = gs
        a0[r, :] = low
        cs[2] += fold8(g)
        cs[3] += fold8(low.astype(F32))

    for i in range(4):
        tsum[0, i : i + 1, :] = total8(cs[i])
    peers = [(s, place(s // 2, s % 2)) for s in range(1, group)]
    t_sum = [remote(tsum.at[0], tsum.at[s], dev) for s, dev in peers]
    t_inb = [remote(ginb.at[pl.ds(s * brow, brow)], rinb.at[s], dev) for s, dev in peers]
    d_sum = [remote(sbuf.at[b], srec.at[b], rank(bit)) for b, bit in enumerate(bits)]
    d_inb = [remote(ibuf.at[b], irec.at[b], rank(bit)) for b, bit in enumerate(bits)]
    t_qv = [remote(tqv.at[0], tqv.at[s], dev) for s, dev in peers]
    d_qv = [remote(qbuf.at[b], qrec.at[b], rank(bit)) for b, bit in enumerate(bits)]
    steps = len(bits) + 1

    def over_tensor(ref):
        acc = None
        for t in range(group):
            s = (y - t // 2 + line) % line * 2 + (core + t) % 2
            acc = ref[s] if acc is None else acc + ref[s]
        return acc

    def reduce_sums(step):
        if step == 0:
            for c in t_sum + t_inb:
                c.wait_recv()
            sbuf[0] = over_tensor(tsum)
            for r in range(brow):
                u = natural(r // prow) * prow + r % prow
                acc = ginb[r] + rinb[1, r]
                for s in range(2, group):
                    acc += rinb[s, u]
                ibuf[0, r] = acc
        else:
            d_sum[step - 1].wait_recv()
            d_inb[step - 1].wait_recv()
            sbuf[step] = sbuf[step - 1] + srec[step - 1]
            ibuf[step] = ibuf[step - 1] + irec[step - 1]
        if step < steps - 1:
            d_sum[step].start()
            d_inb[step].start()

    def reduce_qv(step):
        if step == 0:
            for c in t_qv:
                c.wait_recv()
            qbuf[0] = over_tensor(tqv)
        else:
            d_qv[step - 1].wait_recv()
            qbuf[step] = qbuf[step - 1] + qrec[step - 1]
        if step < steps - 1:
            d_qv[step].start()

    for c in t_sum + t_inb:
        c.start()

    @pl.loop(0, tiles)
    def _(n):
        a1[:, cols(n)] = dot_nt(a0[...], outw[cols(n), :]).astype(BF16)

    @pl.loop(0, tiles)
    def _(n):
        kt = k[n].T
        dqs, dks, dvs = [], [], []
        for p in range(TILE // LANES):
            v2 = v[n, :, p * LANES : (p + 1) * LANES]
            qs = halves(q[n, :, p * LANES : (p + 1) * LANES])
            gs = halves(a1[:, cols(2 * n + p, LANES)])
            dk, dv = None, None
            for e in range(2):
                h = 2 * p + e
                dprob = dot_nt(v2, gs[e])
                low = pt[n * heads + h]
                prob = low.astype(F32)
                t = prob * dprob
                ds = (t - prob * jnp.sum(t, axis=0, keepdims=True)).astype(BF16)
                dvh = dot(low, gs[e])
                dkh = dot(ds, qs[e])
                dv = dvh if dv is None else dv + dvh
                dk = dkh if dk is None else dk + dkh
                dqs.append(dot(kt[h * hd : (h + 1) * hd], ds))
            dks.append(dk)
            dvs.append(dv)
        dq = (jnp.concatenate(dqs, axis=0) * hd**-0.5).astype(BF16).T
        dv = jnp.concatenate(dvs, axis=1).astype(BF16)
        q[n] = dq
        k[n] = jnp.concatenate(dks, axis=1).astype(BF16)
        v[n] = dv
        csqv[0, :, cols(n)] = fold8(dq.astype(F32))
        csqv[1, :, cols(n)] = fold8(dv.astype(F32))
        for s in range(min(steps, tiles)):

            @pl.when(n == s)
            def _(s=s):
                reduce_sums(s)

    for s in range(tiles, steps):
        reduce_sums(s)
    for i in range(2):
        tqv[0, i : i + 1, :] = total8(csqv[i])
    for c in t_qv:
        c.start()

    @pl.loop(0, tiles)
    def _(t):
        acc = f2[:, cols(t)]
        for n in range(tiles):
            for i, ref in enumerate((q, k, v)):
                acc += dot_nt(ref[n], qkvw[n + i * tiles, cols(t), :])
        f1[:, cols(t)] = acc
        for s in range(tiles - 1):

            @pl.when(t == s + 1)
            def _(s=s):
                reduce_qv(s)

    c_grad = load(6, f1, grad_out)
    for s in range(tiles - 1, steps):
        reduce_qv(s)
    shift2_out[...] = sbuf[steps - 1, 0:1]
    ffnb_out[...] = sbuf[steps - 1, 1:2]
    shift1_out[...] = sbuf[steps - 1, 2:3]
    outb_out[...] = sbuf[steps - 1, 3:4]
    inb_out[...] = ibuf[steps - 1]
    qv_out[...] = qbuf[steps - 1]

    for d in far:
        for c in direct[d] + to_x[d] + to_z[d] + list(pass_on[d].values()):
            c.wait_send()
    for c in core_in + [core_ffn] + bias + t_sum + t_inb + d_sum + d_inb + t_qv + d_qv:
        c.wait_send()
    c_act.wait()
    c_grad.wait()
    assert count[0] <= send.shape[0]


def step(
    ranks, group,
    tokens, segments, separators, lengths, type_table, qkv_weight, qv_bias, out_weight, out_bias, gain_one, shift_one,
    in_weight, in_bias, ffn_weight, ffn_bias, gain_two, shift_two, cotangent,
):
    pairs, rows, width = tokens.shape
    units = in_weight.shape[1]
    hidden = units * group
    chunks, tiles = hidden // TILE, width // TILE
    brow = units // LANES
    stages = ranks.bit_length() - 1
    line = group // 2
    copies = (line - 1) * 32 + units // TILE + 1 + 4 * (group - 1) + 3 * stages
    rowsets = (type_table, qv_bias, out_bias, gain_one, shift_one, ffn_bias, gain_two, shift_two)
    small = jnp.concatenate([x.astype(F32).reshape(-1, width) for x in rowsets], axis=0)
    V = pltpu.VMEM
    inside = pl.BlockSpec(memory_space=V)
    outside = pl.BlockSpec(memory_space=pl.ANY)
    scalar = pl.BlockSpec(memory_space=pltpu.SMEM)
    vector = jax.ShapeDtypeStruct((1, width), F32)
    act, grad, qv, outb, shift1, inb, ffnb, shift2 = pl.pallas_call(
        functools.partial(kernel, ranks, group),
        out_shape=(
            jax.ShapeDtypeStruct((rows, width), BF16),
            jax.ShapeDtypeStruct((rows, width), F32),
            jax.ShapeDtypeStruct((2, width), F32),
            vector,
            vector,
            jax.ShapeDtypeStruct((brow, 1, LANES), F32),
            vector,
            vector,
        ),
        in_specs=[scalar, scalar, inside] + [outside] * 7,
        out_specs=(outside, outside) + (inside,) * 6,
        scratch_shapes=[
            V((3 * tiles, width, TILE), BF16),
            V((width, width), BF16),
            V((chunks, width, TILE), BF16),
            V((hidden, width), BF16),
            V((hidden // LANES, 1, LANES), F32),
            V((tiles, rows, TILE), BF16),
            V((tiles, rows, TILE), BF16),
            V((tiles, rows, TILE), BF16),
            V((HEADS, rows, rows), BF16),
            V((chunks, rows, TILE), F32),
            V((chunks, rows, TILE), BF16),
            V((rows, width), BF16),
            V((rows, width), BF16),
            V((rows, width), F32),
            V((rows, width), F32),
            V((rows, width), F32),
            V((rows, width), BF16),
            V((rows, width), BF16),
            V((rows, width), BF16),
            V((rows, LANES), F32),
            V((4, 8, width), F32),
            V((2, 8, width), F32),
            V((hidden // LANES, 1, LANES), F32),
            V((group, brow, 1, LANES), F32),
            V((stages + 1, brow, 1, LANES), F32),
            V((stages, brow, 1, LANES), F32),
            V((group, 4, width), F32),
            V((stages + 1, 4, width), F32),
            V((stages, 4, width), F32),
            V((group, 2, width), F32),
            V((stages + 1, 2, width), F32),
            V((stages, 2, width), F32),
            pltpu.SemaphoreType.DMA((3 * tiles + units // TILE,)),
            pltpu.SemaphoreType.DMA((8,)),
            pltpu.SemaphoreType.DMA((copies,)),
            pltpu.SemaphoreType.DMA((copies,)),
        ],
        compiler_params=pltpu.CompilerParams(collective_id=0, has_side_effects=True, vmem_limit_bytes=67043328),
    )(
        lengths,
        separators,
        small,
        in_bias.astype(F32).reshape(brow, 1, LANES),
        tokens.reshape(rows, width),
        cotangent.reshape(rows, width),
        qkv_weight,
        out_weight,
        in_weight,
        ffn_weight,
    )
    return (
        act.reshape(pairs, rows, width),
        grad.reshape(pairs, rows, width),
        qv,
        outb.reshape(width),
        shift1.reshape(width),
        inb.reshape(units),
        ffnb.reshape(width),
        shift2.reshape(width),
    )


def solution(mesh):
    both = ("dp", "tensor")
    rows = P(both, None, None)
    return jax.shard_map(
        functools.partial(step, mesh.shape["dp"], mesh.shape["tensor"]),
        mesh=mesh,
        in_specs=(rows, P(both, None), P(both, None), P(both))
        + (P(),) * 7
        + (P(None, "tensor"), P("tensor"), P("tensor", None))
        + (P(),) * 3
        + (rows,),
        out_specs=(rows, rows, P(), P(), P(), P("tensor"), P(), P()),
        check_vma=False,
    )
```

```python
import functools

import jax
import jax.numpy as jnp
from jax import lax
from jax.experimental import pallas as pl
from jax.experimental.pallas import tpu as pltpu
from jax.sharding import PartitionSpec as P

HEADS = 16
TILE = 256
LANES = 128
BLOCK = 64
F32 = jnp.float32
BF16 = jnp.bfloat16
MESH = pl.DeviceIdType.MESH
NT = (((1,), (1,)), ((), ()))
root_half = 0.7071067811865476
inv_root_tau = 0.3989422804014327
eps_norm = 1e-06
STOP = 99


def dot(a, b):
    return jnp.dot(a, b, preferred_element_type=F32)


def dot_nt(a, b):
    return lax.dot_general(a, b, NT, preferred_element_type=F32)


def mean_rows(value):
    return jnp.sum(value, axis=-1, keepdims=True) * (1.0 / value.shape[-1])


def cols(n, size=TILE):
    return pl.ds(pl.multiple_of(n * size, size), size)


def fold8(value):
    return jnp.sum(value.reshape(value.shape[0] // 8, 8, value.shape[1]), axis=0)


def total8(value):
    return jnp.sum(value, axis=0, keepdims=True)


def flip(index, bit):
    return index + bit * (1 - 2 * (index // bit % 2))


def kernel(
    ranks, group,
    lengths, separators, table, qv_b, out_b, gain1, shift1, ffn_b, gain2, shift2, in_b, tokens, cot, qkv_w, out_w, in_w, ffn_w,
    act_out, grad_out, sums_out, qv_out, inb_out,
    qkvw, outw, inw, ffw, inb, q, k, v, pt, slope, hid, a0, a1, f0, f1, f2, tok, cotb, act, sc1, cs, csqv,
    small, ginb, rinb, ibuf, tsum, sbuf, tqv, qbuf,
    raw, inraw, wsem, lsem, send, recv,
):
    rows, width = tok.shape
    tiles = width // TILE
    hd = width // HEADS
    chunks = inw.shape[0]
    units = in_w.shape[1]
    part = units // 4
    line = group // 2
    brow = units // LANES
    prow = part // LANES
    per = units // TILE
    length = lengths[0]
    sep0, sep1 = separators[0, 0], separators[0, 1]
    dp, tensor = lax.axis_index("dp"), lax.axis_index("tensor")
    y, core = tensor // 2, tensor % 2
    near = min(ranks, 8)
    bits = [1 << b for b in range(near.bit_length() - 1)]
    wide = [1 << b for b in range(ranks.bit_length() - 1) if 1 << b >= near]

    def place(d, other):
        return (dp, (y + d + line) % line * 2 + (core + other) % 2)

    def mixed(offset):
        return sum((offset // b + dp // b) % 2 * b for b in bits)

    def rank(offset):
        return (dp // near * near + mixed(offset) if offset < near else flip(dp, offset), tensor)

    barrier = pltpu.get_barrier_semaphore()
    friends = [place(s // 2, s % 2) for s in range(1, group)] + [rank(o) for o in list(range(1, near)) + wide]
    for f in friends:
        pl.semaphore_signal(barrier, inc=1, device_id=f, device_id_type=MESH)

    count = [0]

    def remote(src, dst, device):
        i = count[0]
        count[0] += 1
        return pltpu.make_async_remote_copy(
            src_ref=src, dst_ref=dst, send_sem=send.at[i], recv_sem=recv.at[i], device_id=device, device_id_type=MESH
        )

    def natural(p):
        return (p + dp) % 2 + (p // 2 + dp // 2) % 2 * 2

    def piece(slot, p, i):
        u = slot * units + p * part
        if i < 2:
            return inw.at[u // TILE, pl.ds(i * width // 2, width // 2), pl.ds(u % TILE, part)]
        return ffw.at[pl.ds(u + (i - 2) * part // 2, part // 2), :]

    def source(p, i):
        u = pl.multiple_of(natural(p) * part, part)
        if i < 2:
            return in_w.at[pl.ds(i * width // 2, width // 2), pl.ds(u, part)]
        return ffn_w.at[pl.ds(u + (i - 2) * part // 2, part // 2), :]

    def load(i, src, dst):
        c = pltpu.make_async_copy(src, dst, lsem.at[i])
        c.start()
        return c

    c_small = [load(8 + i, src, dst) for i, (src, dst) in enumerate(zip((table, qv_b, out_b, gain1, shift1, ffn_b, gain2, shift2), raw))]
    c_tok = load(0, tokens, tok)
    c_qkv = []
    for n in range(3 * tiles):
        c = pltpu.make_async_copy(qkv_w.at[:, n * TILE : (n + 1) * TILE], qkvw.at[n], wsem.at[n])
        c.start()
        c_qkv.append(c)
    c_in = []
    for n in range(per):
        c = pltpu.make_async_copy(in_w.at[:, n * TILE : (n + 1) * TILE], inw.at[n], wsem.at[3 * tiles + n])
        c.start()
        c_in.append(c)
    c_out = load(1, out_w, outw)
    c_ffn = load(2, ffn_w, ffw.at[pl.ds(0, units), :])
    c_b = load(3, in_b, inraw[0])
    c_cot = load(4, cot, cotb)

    far = range(1, line)
    direct = {d: [remote(source(p, i), piece(2 * d, p, i), place(-d, 0)) for p, i in ((0, 0), (0, 1), (0, 2), (0, 3), (3, 2), (3, 3))] for d in far}
    to_x = {d: [remote(piece(2 * d, p, i), piece(2 * d, p + 1, i), rank(1)) for p, i in ((0, 0), (0, 1), (0, 2), (0, 3), (2, 0))] for d in far}
    to_z = {d: [remote(piece(2 * d, p, i), piece(2 * d, p + 2, i), rank(2)) for p, i in ((0, 0), (0, 1), (0, 2), (0, 3), (1, 1))] for d in far}
    pass_on = {d: {(p, i): remote(piece(2 * d, p, i), piece(2 * d + 1, p, i), place(0, 1)) for p in range(4) for i in range(4)} for d in far}
    core_in = [remote(in_w.at[:, n * TILE : (n + 1) * TILE], inw.at[per + n], place(0, 1)) for n in range(per)]
    core_ffn = remote(ffn_w, ffw.at[pl.ds(units, units), :], place(0, 1))
    bias = [remote(in_b, inraw[s], place(-(s // 2), s % 2)) for s in range(1, group)]

    def relay(step):
        for d in far:
            yd, xd, zd, on = direct[d], to_x[d], to_z[d], pass_on[d]
            if step in ("0", "1", "2", "3"):
                i = int(step)
                yd[i].wait_recv()
                xd[i].start()
                zd[i].start()
                on[0, i].start()
            if step == "in0":
                zd[0].wait_recv()
                xd[4].start()
                on[2, 0].start()
                xd[0].wait_recv()
                on[1, 0].start()
            if step == "in1":
                xd[1].wait_recv()
                zd[4].start()
                on[1, 1].start()
                zd[1].wait_recv()
                on[2, 1].start()
            if step == "in":
                xd[4].wait_recv()
                on[3, 0].start()
                zd[4].wait_recv()
                on[3, 1].start()
            if step in ("4", "5"):
                i = int(step)
                yd[i].wait_recv()
                on[3, i - 2].start()
                xd[i - 2].wait_recv()
                on[1, i - 2].start()
                zd[i - 2].wait_recv()
                on[2, i - 2].start()

    pl.semaphore_wait(barrier, len(friends))
    for c in bias:
        c.start()
    for d in far:
        for c in direct[d]:
            c.start()
    for c in core_in + [core_ffn]:
        c.start()

    for c in c_small:
        c.wait()
    small[0:2, :] = raw[0][...].astype(F32)
    small[2:4, :] = raw[1][...].astype(F32)
    for i in range(2, 8):
        small[2 + i : 3 + i, :] = raw[i][...].astype(F32).reshape(1, width)
    c_tok.wait()

    @pl.loop(0, rows // BLOCK)
    def _(i):
        r = cols(i, BLOCK)
        pos = lax.broadcasted_iota(jnp.int32, (BLOCK, width), 0) + i * BLOCK
        second = (pos > sep0) & (pos < length)
        e = tok[r, :].astype(F32) + jnp.where(second, small[1:2, :], small[0:1, :])
        f0[r, :] = e
        a0[r, :] = e.astype(BF16)

    for c in c_qkv[:tiles]:
        c.wait()

    @pl.loop(0, tiles)
    def _(n):
        q[n] = (dot(a0[...], qkvw[n]) + small[2:3, cols(n)]).astype(BF16) * jnp.asarray(hd**-0.5, BF16)

    for c in c_qkv[tiles : 2 * tiles]:
        c.wait()

    @pl.loop(0, tiles)
    def _(n):
        k[n] = dot(a0[...], qkvw[n + tiles]).astype(BF16)

    for c in c_qkv[2 * tiles :]:
        c.wait()

    @pl.loop(0, tiles)
    def _(n):
        v[n] = (dot(a0[...], qkvw[n + 2 * tiles]) + small[3:4, cols(n)]).astype(BF16)

    relay("0")

    low_half = lax.broadcasted_iota(jnp.int32, (rows, LANES), 1) < hd
    zero = jnp.zeros((rows, LANES), BF16)
    heads = TILE // hd

    def halves(pair):
        return jnp.where(low_half, pair, zero), jnp.where(low_half, zero, pair)

    @pl.loop(0, tiles)
    def _(n):
        vt = v[n].T
        outs = []
        for p in range(TILE // LANES):
            k2 = k[n, :, p * LANES : (p + 1) * LANES]
            for e, qm in enumerate(halves(q[n, :, p * LANES : (p + 1) * LANES])):
                h = 2 * p + e
                s = dot_nt(k2, qm)
                kpos = lax.broadcasted_iota(jnp.int32, s.shape, 0)
                s = jnp.where(kpos < length, s, -1e30)
                top = jnp.max(s, axis=0, keepdims=True)
                ex = jnp.exp(s - top)
                prob = (ex * (1.0 / jnp.sum(ex, axis=0, keepdims=True))).astype(BF16)
                pt[n * heads + h] = prob
                outs.append(dot(vt[h * hd : (h + 1) * hd], prob))
        a1[:, cols(n)] = jnp.concatenate(outs, axis=0).astype(BF16).T

        @pl.when(n == 1)
        def _():
            relay("1")

        @pl.when(n == 2)
        def _():
            relay("in0")

    c_out.wait()

    @pl.loop(0, tiles)
    def _(n):
        f1[:, cols(n)] = dot(a1[...], outw[:, cols(n)]) + small[4:5, cols(n)] + f0[:, cols(n)]

    relay("in1")
    relay("2")

    @pl.loop(0, rows // BLOCK)
    def _(i):
        r = cols(i, BLOCK)
        x = f1[r, :]
        x = x - mean_rows(x)
        scale = lax.rsqrt(mean_rows(x * x) + eps_norm)
        normed = x * scale
        f0[r, :] = normed
        a0[r, :] = (normed * small[5:6, :] + small[6:7, :]).astype(BF16)
        sc1[r, :] = jnp.broadcast_to(scale, (BLOCK, LANES))

    def hidden_units(c, first, second):
        x = dot(a0[...], inw[c]) + jnp.concatenate([inb[first], inb[second]], axis=1)
        cdf = 0.5 * (1.0 + lax.erf(x * root_half))
        hid[c] = (x * cdf).astype(BF16)
        slope[c] = cdf + x * (inv_root_tau * jnp.exp(-0.5 * x * x))

    for c in c_in + [c_b]:
        c.wait()
    for c in core_in + bias:
        c.wait_recv()
    for t in range(group):
        b = inraw[t][...].astype(F32).reshape(1, units)
        for r in range(brow):
            inb[t * brow + r] = b[:, r * LANES : (r + 1) * LANES]

    @pl.loop(0, 2 * per)
    def _(c):
        hidden_units(c, 2 * c, 2 * c + 1)

        @pl.when(c == 2 * per - 4)
        def _():
            relay("3")

    def shuffled(r):
        return r // brow * brow + natural(r % brow // prow) * prow + r % prow

    def units_of(i):
        for d in far:
            for p in range(4):
                if (p * part) // TILE == i:
                    pass_on[d][p, 0].wait_recv()
                    pass_on[d][p, 1].wait_recv()

        @pl.loop(2, group)
        def _(t):
            c = t * per + i
            hidden_units(c, shuffled(2 * c), shuffled(2 * c + 1))

    early = per - 1
    for i in range(early):
        units_of(i)
    relay("in")
    c_ffn.wait()
    core_ffn.wait_recv()

    @pl.loop(0, tiles)
    def _(t):
        acc = dot(hid[0], ffw[0:TILE, cols(t)])
        for c in range(1, 2 * per):
            acc += dot(hid[c], ffw[c * TILE : (c + 1) * TILE, cols(t)])
        f1[:, cols(t)] = acc

    relay("4")
    for i in range(early, per):
        units_of(i)
    relay("5")
    for d in far:
        for p in range(4):
            pass_on[d][p, 2].wait_recv()
            pass_on[d][p, 3].wait_recv()

    @pl.loop(0, tiles)
    def _(t):
        acc = f1[:, cols(t)]
        for c in range(2 * per, chunks):
            acc += dot(hid[c], ffw[c * TILE : (c + 1) * TILE, cols(t)])
        f1[:, cols(t)] = acc

    c_cot.wait()
    cs[...] = jnp.zeros_like(cs)

    @pl.loop(0, rows // BLOCK)
    def _(i):
        r = cols(i, BLOCK)
        pos = lax.broadcasted_iota(jnp.int32, (BLOCK, width), 0) + i * BLOCK
        keep = (pos > 0) & (pos < length) & (pos != sep0) & (pos != sep1)
        x = f0[r, :] * small[5:6, :] + small[6:7, :] + f1[r, :] + small[7:8, :]
        x = x - mean_rows(x)
        scale = lax.rsqrt(mean_rows(x * x) + eps_norm)
        normed = x * scale
        act[r, :] = (normed * small[8:9, :] + small[9:10, :]).astype(BF16)
        g = jnp.where(keep, cotb[r, :].astype(F32), 0.0)
        s = g * small[8:9, :]
        gs = scale * (s - mean_rows(s) - normed * mean_rows(s * normed))
        low = gs.astype(BF16)
        f2[r, :] = gs
        a1[r, :] = low
        cs[0] += fold8(g)
        cs[1] += fold8(low.astype(F32))

    c_act = load(5, act, act_out)

    @pl.loop(0, chunks)
    def _(c):
        gi = (dot_nt(a1[...], ffw[cols(c), :]) * slope[c]).astype(BF16)
        hid[c] = gi
        s = total8(gi.astype(F32))
        ginb[2 * c] = s[:, :LANES]
        ginb[2 * c + 1] = s[:, LANES:]

    @pl.loop(0, tiles)
    def _(t):
        acc = dot_nt(hid[0], inw[0, cols(t), :])
        for c in range(1, chunks):
            acc += dot_nt(hid[c], inw[c, cols(t), :])
        f1[:, cols(t)] = acc

    @pl.loop(0, rows // BLOCK)
    def _(i):
        r = cols(i, BLOCK)
        g = f1[r, :] + f2[r, :]
        s = g * small[5:6, :]
        normed = f0[r, :]
        gs = sc1[r, 0:1] * (s - mean_rows(s) - normed * mean_rows(s * normed))
        low = gs.astype(BF16)
        f2[r, :] = gs
        a0[r, :] = low
        cs[2] += fold8(g)
        cs[3] += fold8(low.astype(F32))

    for i in range(4):
        tsum[0, i : i + 1, :] = total8(cs[i])
    peers = [(s, place(s // 2, s % 2)) for s in range(1, group)]
    t_sum = [remote(tsum.at[0], tsum.at[s], dev) for s, dev in peers]
    t_inb = [remote(ginb.at[pl.ds(s * brow, brow)], rinb.at[s], dev) for s, dev in peers]
    hops = [list(range(1, near))] + [[w] for w in wide]
    steps = len(hops) + 1

    def spread(ref):
        copies, base = [], 0
        for hop in hops:
            copies.append([remote(ref.at[base], ref.at[base + i + 1], rank(o)) for i, o in enumerate(hop)])
            base += len(hop) + 1
        return copies

    d_sum, d_inb, d_qv = spread(sbuf), spread(ibuf), spread(qbuf)
    t_qv = [remote(tqv.at[0], tqv.at[s], dev) for s, dev in peers]

    def over_tensor(ref):
        acc = None
        for t in range(group):
            s = (y - t // 2 + line) % line * 2 + (core + t) % 2
            acc = ref[s] if acc is None else acc + ref[s]
        return acc

    def over_hop(ref, hop):
        if hop == 0:
            acc = ref[mixed(0)]
            for o in range(1, near):
                acc += ref[mixed(o)]
            return acc
        base = near + 2 * (hop - 1)
        return ref[base] + ref[base + 1]

    def go(step, buffers, copies, totals):
        if step == 0:
            for ref, value in zip(buffers, totals()):
                ref[0] = value
        else:
            for ref, cs_ in zip(buffers, copies):
                for c in cs_[step - 1]:
                    c.wait_recv()
                ref[near + 2 * (step - 1)] = over_hop(ref, step - 1)
        if step < steps - 1:
            for cs_ in copies:
                for c in cs_[step]:
                    c.start()

    def first_sums():
        for c in t_sum + t_inb:
            c.wait_recv()
        parts = []
        for r in range(brow):
            u = natural(r // prow) * prow + r % prow
            acc = ginb[r] + rinb[1, r]
            for s in range(2, group):
                acc += rinb[s, u]
            parts.append(acc)
        return over_tensor(tsum), jnp.stack(parts)

    def first_qv():
        for c in t_qv:
            c.wait_recv()
        return (over_tensor(tqv),)

    def reduce_sums(step):
        go(step, (sbuf, ibuf), (d_sum, d_inb), first_sums)

    def reduce_qv(step):
        go(step, (qbuf,), (d_qv,), first_qv)

    for c in t_sum + t_inb:
        c.start()

    @pl.loop(0, tiles)
    def _(n):
        a1[:, cols(n)] = dot_nt(a0[...], outw[cols(n), :]).astype(BF16)

    @pl.loop(0, tiles)
    def _(n):
        kt = k[n].T
        dqs, dks, dvs = [], [], []
        for p in range(TILE // LANES):
            v2 = v[n, :, p * LANES : (p + 1) * LANES]
            qs = halves(q[n, :, p * LANES : (p + 1) * LANES])
            gs = halves(a1[:, cols(2 * n + p, LANES)])
            dk, dv = None, None
            for e in range(2):
                h = 2 * p + e
                dprob = dot_nt(v2, gs[e])
                low = pt[n * heads + h]
                prob = low.astype(F32)
                t = prob * dprob
                ds = (t - prob * jnp.sum(t, axis=0, keepdims=True)).astype(BF16)
                dvh = dot(low, gs[e])
                dkh = dot(ds, qs[e])
                dv = dvh if dv is None else dv + dvh
                dk = dkh if dk is None else dk + dkh
                dqs.append(dot(kt[h * hd : (h + 1) * hd], ds))
            dks.append(dk)
            dvs.append(dv)
        dq = (jnp.concatenate(dqs, axis=0) * hd**-0.5).astype(BF16).T
        dv = jnp.concatenate(dvs, axis=1).astype(BF16)
        q[n] = dq
        k[n] = jnp.concatenate(dks, axis=1).astype(BF16)
        v[n] = dv
        csqv[0, :, cols(n)] = fold8(dq.astype(F32))
        csqv[1, :, cols(n)] = fold8(dv.astype(F32))
        for s in range(min(steps, tiles)):

            @pl.when(n == s)
            def _(s=s):
                reduce_sums(s)

    for s in range(tiles, steps):
        reduce_sums(s)
    for i in range(2):
        tqv[0, i : i + 1, :] = total8(csqv[i])
    for c in t_qv:
        c.start()

    @pl.loop(0, tiles)
    def _(t):
        acc = f2[:, cols(t)]
        for n in range(tiles):
            for i, ref in enumerate((q, k, v)):
                acc += dot_nt(ref[n], qkvw[n + i * tiles, cols(t), :])
        f1[:, cols(t)] = acc
        for s in range(min(steps, tiles - 1)):

            @pl.when(t == s + 1)
            def _(s=s):
                reduce_qv(s)

    c_grad = load(6, f1, grad_out)
    for s in range(min(steps, tiles - 1), steps):
        reduce_qv(s)
    last = near + 2 * (steps - 2)
    outs = [load(7, sbuf.at[last], sums_out), load(16, qbuf.at[last], qv_out), load(17, ibuf.at[last], inb_out)]

    for d in far:
        for c in direct[d] + to_x[d] + to_z[d] + list(pass_on[d].values()):
            c.wait_send()
    for c in core_in + [core_ffn] + bias + t_sum + t_inb + t_qv + sum(d_sum + d_inb + d_qv, []):
        c.wait_send()
    for c in [c_act, c_grad] + outs:
        c.wait()
    assert count[0] <= send.shape[0]


def finish(act, grad, sums, qv, inb, act_out, grad_out, qv_out, outb_out, shift1_out, inb_out, ffnb_out, shift2_out, abuf, gbuf, sbuf, qbuf, ibuf, into, out):
    pieces = 4
    size = act.shape[0] // pieces
    plan = [(sums, sbuf, None), (qv, qbuf, qv_out), (inb, ibuf, inb_out)]
    for i in range(pieces):
        r = pl.ds(i * size, size)
        plan.append((grad.at[r, :], gbuf.at[r, :], grad_out.at[r, :]))
        plan.append((act.at[r, :], abuf.at[r, :], act_out.at[r, :]))
    first = [pltpu.make_async_copy(src, mid, into.at[i]) for i, (src, mid, _) in enumerate(plan)]
    for c in first:
        c.start()
    second = []
    for i, (_, mid, dst) in enumerate(plan):
        first[i].wait()
        if dst is not None:
            second.append(pltpu.make_async_copy(mid, dst, out.at[i]))
            second[-1].start()
        else:
            for j, ref in enumerate((shift2_out, ffnb_out, shift1_out, outb_out)):
                second.append(pltpu.make_async_copy(mid.at[j : j + 1, :], ref, out.at[len(plan) + j]))
                second[-1].start()
    for c in second:
        c.wait()


def step(
    ranks, group,
    tokens, segments, separators, lengths, type_table, qkv_weight, qv_bias, out_weight, out_bias, gain_one, shift_one,
    in_weight, in_bias, ffn_weight, ffn_bias, gain_two, shift_two, cotangent,
):
    pairs, rows, width = tokens.shape
    units = in_weight.shape[1]
    hidden = units * group
    chunks, tiles = hidden // TILE, width // TILE
    brow = units // LANES
    line = group // 2
    near = min(ranks, 8)
    far_bits = (ranks // near).bit_length() - 1
    slots = near + 2 * far_bits + 1
    copies = (line - 1) * 32 + units // TILE + 1 + 4 * (group - 1) + 3 * (near - 1 + far_bits)
    vectors = (type_table, qv_bias, out_bias, gain_one, shift_one, ffn_bias, gain_two, shift_two)
    V = pltpu.VMEM
    outside = pl.BlockSpec(memory_space=pl.ANY)
    scalar = pl.BlockSpec(memory_space=pltpu.SMEM)
    act, grad, sums, qv, inb = pl.pallas_call(
        functools.partial(kernel, ranks, group),
        out_shape=(
            jax.ShapeDtypeStruct((rows, width), BF16),
            jax.ShapeDtypeStruct((rows, width), F32),
            jax.ShapeDtypeStruct((4, width), F32),
            jax.ShapeDtypeStruct((2, width), F32),
            jax.ShapeDtypeStruct((brow, 1, LANES), F32),
        ),
        in_specs=[scalar, scalar] + [outside] * 15,
        out_specs=(outside,) * 5,
        scratch_shapes=[
            V((3 * tiles, width, TILE), BF16),
            V((width, width), BF16),
            V((chunks, width, TILE), BF16),
            V((hidden, width), BF16),
            V((hidden // LANES, 1, LANES), F32),
            V((tiles, rows, TILE), BF16),
            V((tiles, rows, TILE), BF16),
            V((tiles, rows, TILE), BF16),
            V((HEADS, rows, rows), BF16),
            V((chunks, rows, TILE), F32),
            V((chunks, rows, TILE), BF16),
            V((rows, width), BF16),
            V((rows, width), BF16),
            V((rows, width), F32),
            V((rows, width), F32),
            V((rows, width), F32),
            V((rows, width), BF16),
            V((rows, width), BF16),
            V((rows, width), BF16),
            V((rows, LANES), F32),
            V((4, 8, width), F32),
            V((2, 8, width), F32),
            V((10, width), F32),
            V((hidden // LANES, 1, LANES), F32),
            V((group, brow, 1, LANES), F32),
            V((slots, brow, 1, LANES), F32),
            V((group, 4, width), F32),
            V((slots, 4, width), F32),
            V((group, 2, width), F32),
            V((slots, 2, width), F32),
            [V(x.shape, x.dtype) for x in vectors],
            [V((units,), BF16)] * group,
            pltpu.SemaphoreType.DMA((3 * tiles + units // TILE,)),
            pltpu.SemaphoreType.DMA((18,)),
            pltpu.SemaphoreType.DMA((copies,)),
            pltpu.SemaphoreType.DMA((copies,)),
        ],
        compiler_params=pltpu.CompilerParams(collective_id=0, has_side_effects=True, vmem_limit_bytes=67043328),
    )(
        lengths,
        separators,
        *vectors,
        in_bias,
        tokens.reshape(rows, width),
        cotangent.reshape(rows, width),
        qkv_weight,
        out_weight,
        in_weight,
        ffn_weight,
    )
    vector = jax.ShapeDtypeStruct((1, width), F32)
    act, grad, qv, outb, shift1, inb, ffnb, shift2 = pl.pallas_call(
        finish,
        out_shape=(
            jax.ShapeDtypeStruct((rows, width), BF16),
            jax.ShapeDtypeStruct((rows, width), F32),
            jax.ShapeDtypeStruct((2, width), F32),
            vector,
            vector,
            jax.ShapeDtypeStruct((brow, 1, LANES), F32),
            vector,
            vector,
        ),
        in_specs=[outside] * 5,
        out_specs=(outside,) * 8,
        scratch_shapes=[
            V((rows, width), BF16),
            V((rows, width), F32),
            V((4, width), F32),
            V((2, width), F32),
            V((brow, 1, LANES), F32),
            pltpu.SemaphoreType.DMA((16,)),
            pltpu.SemaphoreType.DMA((16,)),
        ],
    )(act, grad, sums, qv, inb)
    return (
        act.reshape(pairs, rows, width),
        grad.reshape(pairs, rows, width),
        qv,
        outb.reshape(width),
        shift1.reshape(width),
        inb.reshape(units),
        ffnb.reshape(width),
        shift2.reshape(width),
    )


def solution(mesh):
    both = ("dp", "tensor")
    rows = P(both, None, None)
    return jax.shard_map(
        functools.partial(step, mesh.shape["dp"], mesh.shape["tensor"]),
        mesh=mesh,
        in_specs=(rows, P(both, None), P(both, None), P(both))
        + (P(),) * 7
        + (P(None, "tensor"), P("tensor"), P("tensor", None))
        + (P(),) * 3
        + (rows,),
        out_specs=(rows, rows, P(), P(), P(), P("tensor"), P(), P()),
        check_vma=False,
    )
```

```python
import functools

import jax
import jax.numpy as jnp
from jax import lax
from jax.experimental import pallas as pl
from jax.experimental.pallas import tpu as pltpu
from jax.sharding import PartitionSpec as P

HEADS = 16
TILE = 256
LANES = 128
BLOCK = 64
F32 = jnp.float32
BF16 = jnp.bfloat16
MESH = pl.DeviceIdType.MESH
NT = (((1,), (1,)), ((), ()))
root_half = 0.7071067811865476
inv_root_tau = 0.3989422804014327
eps_norm = 1e-06
STOP = 99


def dot(a, b):
    return jnp.dot(a, b, preferred_element_type=F32)


def dot_nt(a, b):
    return lax.dot_general(a, b, NT, preferred_element_type=F32)


def mean_rows(value):
    return jnp.sum(value, axis=-1, keepdims=True) * (1.0 / value.shape[-1])


def cols(n, size=TILE):
    return pl.ds(pl.multiple_of(n * size, size), size)


def fold8(value):
    return jnp.sum(value.reshape(value.shape[0] // 8, 8, value.shape[1]), axis=0)


def total8(value):
    return jnp.sum(value, axis=0, keepdims=True)


def flip(index, bit):
    return index + bit * (1 - 2 * (index // bit % 2))


def kernel(
    ranks, group,
    lengths, separators, table, qv_b, out_b, gain1, shift1, ffn_b, gain2, shift2, in_b, tokens, cot, qkv_w, out_w, in_w, ffn_w,
    act_out, grad_out, sums_out, qv_out, inb_out,
    qkvw, outw, inw, ffw, inb, q, k, v, pt, slope, hid, a0, a1, f0, f1, f2, tok, cotb, act, sc1, cs, csqv,
    small, ginb, rinb, ibuf, tsum, sbuf, tqv, qbuf,
    raw, inraw, len_s, sep_s, wsem, lsem, send, recv,
):
    rows, width = tok.shape
    tiles = width // TILE
    hd = width // HEADS
    chunks = inw.shape[0]
    units = in_w.shape[1]
    part = units // 4
    line = group // 2
    brow = units // LANES
    prow = part // LANES
    per = units // TILE
    dp, tensor = lax.axis_index("dp"), lax.axis_index("tensor")
    y, core = tensor // 2, tensor % 2
    near = min(ranks, 8)
    bits = [1 << b for b in range(near.bit_length() - 1)]
    wide = [1 << b for b in range(ranks.bit_length() - 1) if 1 << b >= near]

    def place(d, other):
        return (dp, (y + d + line) % line * 2 + (core + other) % 2)

    def mixed(offset):
        return sum((offset // b + dp // b) % 2 * b for b in bits)

    def rank(offset):
        return (dp // near * near + mixed(offset) if offset < near else flip(dp, offset), tensor)

    barrier = pltpu.get_barrier_semaphore()
    friends = [place(s // 2, s % 2) for s in range(1, group)] + [rank(o) for o in list(range(1, near)) + wide]
    for f in friends:
        pl.semaphore_signal(barrier, inc=1, device_id=f, device_id_type=MESH)

    count = [0]

    def remote(src, dst, device):
        i = count[0]
        count[0] += 1
        return pltpu.make_async_remote_copy(
            src_ref=src, dst_ref=dst, send_sem=send.at[i], recv_sem=recv.at[i], device_id=device, device_id_type=MESH
        )

    def natural(p):
        return (p + dp) % 2 + (p // 2 + dp // 2) % 2 * 2

    def piece(slot, p, i):
        u = slot * units + p * part
        if i < 2:
            return inw.at[u // TILE, pl.ds(i * width // 2, width // 2), pl.ds(u % TILE, part)]
        return ffw.at[pl.ds(u + (i - 2) * part // 2, part // 2), :]

    def source(p, i):
        u = pl.multiple_of(natural(p) * part, part)
        if i < 2:
            return in_w.at[pl.ds(i * width // 2, width // 2), pl.ds(u, part)]
        return ffn_w.at[pl.ds(u + (i - 2) * part // 2, part // 2), :]

    def load(i, src, dst):
        c = pltpu.make_async_copy(src, dst, lsem.at[i])
        c.start()
        return c

    c_small = [load(8 + i, src, dst) for i, (src, dst) in enumerate(zip((table, qv_b, out_b, gain1, shift1, ffn_b, gain2, shift2), raw))]
    c_tok = load(0, tokens, tok)
    c_small += [load(18, lengths, len_s), load(19, separators, sep_s)]
    c_qkv = []
    for n in range(3 * tiles):
        c = pltpu.make_async_copy(qkv_w.at[:, n * TILE : (n + 1) * TILE], qkvw.at[n], wsem.at[n])
        c.start()
        c_qkv.append(c)
    c_in = []
    for n in range(per):
        c = pltpu.make_async_copy(in_w.at[:, n * TILE : (n + 1) * TILE], inw.at[n], wsem.at[3 * tiles + n])
        c.start()
        c_in.append(c)
    c_out = load(1, out_w, outw)
    c_ffn = load(2, ffn_w, ffw.at[pl.ds(0, units), :])
    c_b = load(3, in_b, inraw[0])
    c_cot = load(4, cot, cotb)

    far = range(1, line)
    direct = {d: [remote(source(p, i), piece(2 * d, p, i), place(-d, 0)) for p, i in ((0, 0), (0, 1), (0, 2), (0, 3), (3, 2), (3, 3))] for d in far}
    to_x = {d: [remote(piece(2 * d, p, i), piece(2 * d, p + 1, i), rank(1)) for p, i in ((0, 0), (0, 1), (0, 2), (0, 3), (2, 0))] for d in far}
    to_z = {d: [remote(piece(2 * d, p, i), piece(2 * d, p + 2, i), rank(2)) for p, i in ((0, 0), (0, 1), (0, 2), (0, 3), (1, 1))] for d in far}
    pass_on = {d: {(p, i): remote(piece(2 * d, p, i), piece(2 * d + 1, p, i), place(0, 1)) for p in range(4) for i in range(4)} for d in far}
    core_in = [remote(in_w.at[:, n * TILE : (n + 1) * TILE], inw.at[per + n], place(0, 1)) for n in range(per)]
    core_ffn = remote(ffn_w, ffw.at[pl.ds(units, units), :], place(0, 1))
    bias = [remote(in_b, inraw[s], place(-(s // 2), s % 2)) for s in range(1, group)]

    def relay(step):
        for d in far:
            yd, xd, zd, on = direct[d], to_x[d], to_z[d], pass_on[d]
            if step in ("0", "1", "2", "3"):
                i = int(step)
                yd[i].wait_recv()
                xd[i].start()
                zd[i].start()
                on[0, i].start()
            if step == "in0":
                zd[0].wait_recv()
                xd[4].start()
                on[2, 0].start()
                xd[0].wait_recv()
                on[1, 0].start()
            if step == "in1":
                xd[1].wait_recv()
                zd[4].start()
                on[1, 1].start()
                zd[1].wait_recv()
                on[2, 1].start()
            if step == "in":
                xd[4].wait_recv()
                on[3, 0].start()
                zd[4].wait_recv()
                on[3, 1].start()
            if step in ("4", "5"):
                i = int(step)
                yd[i].wait_recv()
                on[3, i - 2].start()
                xd[i - 2].wait_recv()
                on[1, i - 2].start()
                zd[i - 2].wait_recv()
                on[2, i - 2].start()

    pl.semaphore_wait(barrier, len(friends))
    for c in bias:
        c.start()
    for d in far:
        for c in direct[d]:
            c.start()
    for c in core_in + [core_ffn]:
        c.start()

    for c in c_small:
        c.wait()
    length = len_s[0]
    sep0, sep1 = sep_s[0, 0], sep_s[0, 1]
    small[0:2, :] = raw[0][...].astype(F32)
    small[2:4, :] = raw[1][...].astype(F32)
    for i in range(2, 8):
        small[2 + i : 3 + i, :] = raw[i][...].astype(F32).reshape(1, width)
    c_tok.wait()

    @pl.loop(0, rows // BLOCK, unroll=2)
    def _(i):
        r = cols(i, BLOCK)
        pos = lax.broadcasted_iota(jnp.int32, (BLOCK, width), 0) + i * BLOCK
        second = (pos > sep0) & (pos < length)
        e = tok[r, :].astype(F32) + jnp.where(second, small[1:2, :], small[0:1, :])
        f0[r, :] = e
        a0[r, :] = e.astype(BF16)

    for c in c_qkv[:tiles]:
        c.wait()

    @pl.loop(0, tiles, unroll=2)
    def _(n):
        q[n] = (dot(a0[...], qkvw[n]) + small[2:3, cols(n)]).astype(BF16) * jnp.asarray(hd**-0.5, BF16)

    for c in c_qkv[tiles : 2 * tiles]:
        c.wait()

    @pl.loop(0, tiles, unroll=2)
    def _(n):
        k[n] = dot(a0[...], qkvw[n + tiles]).astype(BF16)

    for c in c_qkv[2 * tiles :]:
        c.wait()

    @pl.loop(0, tiles, unroll=2)
    def _(n):
        v[n] = (dot(a0[...], qkvw[n + 2 * tiles]) + small[3:4, cols(n)]).astype(BF16)

    relay("0")

    low_half = lax.broadcasted_iota(jnp.int32, (rows, LANES), 1) < hd
    zero = jnp.zeros((rows, LANES), BF16)
    heads = TILE // hd

    def halves(pair):
        return jnp.where(low_half, pair, zero), jnp.where(low_half, zero, pair)

    @pl.loop(0, tiles)
    def _(n):
        vt = v[n].T
        outs = []
        for p in range(TILE // LANES):
            k2 = k[n, :, p * LANES : (p + 1) * LANES]
            for e, qm in enumerate(halves(q[n, :, p * LANES : (p + 1) * LANES])):
                h = 2 * p + e
                s = dot_nt(k2, qm)
                kpos = lax.broadcasted_iota(jnp.int32, s.shape, 0)
                s = jnp.where(kpos < length, s, -1e30)
                top = jnp.max(s, axis=0, keepdims=True)
                ex = jnp.exp(s - top)
                prob = (ex * (1.0 / jnp.sum(ex, axis=0, keepdims=True))).astype(BF16)
                pt[n * heads + h] = prob
                outs.append(dot(vt[h * hd : (h + 1) * hd], prob))
        a1[:, cols(n)] = jnp.concatenate(outs, axis=0).astype(BF16).T

        @pl.when(n == 1)
        def _():
            relay("1")

        @pl.when(n == 2)
        def _():
            relay("in0")

    relay("2")

    c_out.wait()

    @pl.loop(0, tiles, unroll=2)
    def _(n):
        f1[:, cols(n)] = dot(a1[...], outw[:, cols(n)]) + small[4:5, cols(n)] + f0[:, cols(n)]


    @pl.loop(0, rows // BLOCK, unroll=2)
    def _(i):
        r = cols(i, BLOCK)
        x = f1[r, :]
        x = x - mean_rows(x)
        scale = lax.rsqrt(mean_rows(x * x) + eps_norm)
        normed = x * scale
        f0[r, :] = normed
        a0[r, :] = (normed * small[5:6, :] + small[6:7, :]).astype(BF16)
        sc1[r, :] = jnp.broadcast_to(scale, (BLOCK, LANES))

    relay("in1")

    def hidden_units(c, first, second):
        x = dot(a0[...], inw[c]) + jnp.concatenate([inb[first], inb[second]], axis=1)
        cdf = 0.5 * (1.0 + lax.erf(x * root_half))
        hid[c] = (x * cdf).astype(BF16)
        slope[c] = cdf + x * (inv_root_tau * jnp.exp(-0.5 * x * x))

    for c in c_in + [c_b]:
        c.wait()
    for c in core_in + bias:
        c.wait_recv()
    for t in range(group):
        b = inraw[t][...].astype(F32).reshape(1, units)
        for r in range(brow):
            inb[t * brow + r] = b[:, r * LANES : (r + 1) * LANES]

    @pl.loop(0, 2 * per)
    def _(c):
        hidden_units(c, 2 * c, 2 * c + 1)

        @pl.when(c == 2 * per - 4)
        def _():
            relay("3")

    def shuffled(r):
        return r // brow * brow + natural(r % brow // prow) * prow + r % prow

    def units_of(i):
        for d in far:
            for p in range(4):
                if (p * part) // TILE == i:
                    pass_on[d][p, 0].wait_recv()
                    pass_on[d][p, 1].wait_recv()

        @pl.loop(2, group)
        def _(t):
            c = t * per + i
            hidden_units(c, shuffled(2 * c), shuffled(2 * c + 1))

    early = per - 1
    for i in range(early):
        units_of(i)
    relay("in")
    c_ffn.wait()
    core_ffn.wait_recv()

    @pl.loop(0, tiles)
    def _(t):
        acc = dot(hid[0], ffw[0:TILE, cols(t)])
        for c in range(1, 2 * per):
            acc += dot(hid[c], ffw[c * TILE : (c + 1) * TILE, cols(t)])
        f1[:, cols(t)] = acc

    relay("4")
    for i in range(early, per):
        units_of(i)
    half = part // 2
    blocks = [(t * units + p * part + h * half, h > 0 and p > 0) for t in range(2, group) for p in range(4) for h in range(2)]
    if half % LANES:
        ready, late = [], [u for u, _ in blocks]
    else:
        ready, late = [u for u, last in blocks if not last], [u for u, last in blocks if last]

    def contract(t, acc, starts):
        step = max(1, TILE // half)
        for i in range(0, len(starts), step):
            us = starts[i : i + step]
            if us == list(range(us[0], us[0] + TILE, half)) and us[0] % TILE == 0:
                left, right = hid[us[0] // TILE], ffw[us[0] : us[0] + TILE, cols(t)]
            else:
                left = jnp.concatenate([hid[u // TILE, :, u % TILE : u % TILE + half] for u in us], axis=1)
                right = jnp.concatenate([ffw[u : u + half, cols(t)] for u in us], axis=0)
            acc += dot(left, right)
        return acc

    if ready:
        for d in far:
            for p in range(4):
                pass_on[d][p, 2].wait_recv()
            pass_on[d][0, 3].wait_recv()

        @pl.loop(0, tiles)
        def _(t):
            f1[:, cols(t)] = contract(t, f1[:, cols(t)], ready)

    relay("5")
    for d in far:
        for p in range(4):
            if not ready:
                pass_on[d][p, 2].wait_recv()
            if p > 0 or not ready:
                pass_on[d][p, 3].wait_recv()

    @pl.loop(0, tiles)
    def _(t):
        f1[:, cols(t)] = contract(t, f1[:, cols(t)], late)

    c_cot.wait()
    cs[...] = jnp.zeros_like(cs)

    @pl.loop(0, rows // BLOCK, unroll=2)
    def _(i):
        r = cols(i, BLOCK)
        pos = lax.broadcasted_iota(jnp.int32, (BLOCK, 1), 0) + i * BLOCK
        keep = ((pos > 0) & (pos < length) & (pos != sep0) & (pos != sep1)).astype(F32)
        x = f0[r, :] * small[5:6, :] + small[6:7, :] + f1[r, :] + small[7:8, :]
        x = x - mean_rows(x)
        scale = lax.rsqrt(mean_rows(x * x) + eps_norm)
        normed = x * scale
        act[r, :] = (normed * small[8:9, :] + small[9:10, :]).astype(BF16)
        g = cotb[r, :].astype(F32) * keep
        s = g * small[8:9, :]
        gs = scale * (s - mean_rows(s) - normed * mean_rows(s * normed))
        low = gs.astype(BF16)
        f2[r, :] = gs
        a1[r, :] = low
        cs[0] += fold8(g)
        cs[1] += fold8(low.astype(F32))

    c_act = load(5, act, act_out)

    @pl.loop(0, chunks, unroll=2)
    def _(c):
        gi = (dot_nt(a1[...], ffw[cols(c), :]) * slope[c]).astype(BF16)
        hid[c] = gi
        s = total8(gi.astype(F32))
        ginb[2 * c] = s[:, :LANES]
        ginb[2 * c + 1] = s[:, LANES:]

    @pl.loop(0, tiles)
    def _(t):
        acc = dot_nt(hid[0], inw[0, cols(t), :])
        for c in range(1, chunks):
            acc += dot_nt(hid[c], inw[c, cols(t), :])
        f1[:, cols(t)] = acc

    @pl.loop(0, rows // BLOCK, unroll=2)
    def _(i):
        r = cols(i, BLOCK)
        g = f1[r, :] + f2[r, :]
        s = g * small[5:6, :]
        normed = f0[r, :]
        gs = sc1[r, 0:1] * (s - mean_rows(s) - normed * mean_rows(s * normed))
        low = gs.astype(BF16)
        f2[r, :] = gs
        a0[r, :] = low
        cs[2] += fold8(g)
        cs[3] += fold8(low.astype(F32))

    for i in range(4):
        tsum[0, i : i + 1, :] = total8(cs[i])
    peers = [(s, place(s // 2, s % 2)) for s in range(1, group)]
    t_sum = [remote(tsum.at[0], tsum.at[s], dev) for s, dev in peers]
    t_inb = [remote(ginb.at[pl.ds(s * brow, brow)], rinb.at[s], dev) for s, dev in peers]
    hops = [list(range(1, near))] + [[w] for w in wide]
    steps = len(hops) + 1

    def spread(ref):
        copies, base = [], 0
        for hop in hops:
            copies.append([remote(ref.at[base], ref.at[base + i + 1], rank(o)) for i, o in enumerate(hop)])
            base += len(hop) + 1
        return copies

    d_sum, d_inb, d_qv = spread(sbuf), spread(ibuf), spread(qbuf)
    t_qv = [remote(tqv.at[0], tqv.at[s], dev) for s, dev in peers]

    def over_tensor(ref):
        acc = None
        for t in range(group):
            s = (y - t // 2 + line) % line * 2 + (core + t) % 2
            acc = ref[s] if acc is None else acc + ref[s]
        return acc

    def over_hop(ref, hop):
        if hop == 0:
            acc = ref[mixed(0)]
            for o in range(1, near):
                acc += ref[mixed(o)]
            return acc
        base = near + 2 * (hop - 1)
        return ref[base] + ref[base + 1]

    def go(step, buffers, copies, totals):
        if step == 0:
            for ref, value in zip(buffers, totals()):
                ref[0] = value
        else:
            for ref, cs_ in zip(buffers, copies):
                for c in cs_[step - 1]:
                    c.wait_recv()
                ref[near + 2 * (step - 1)] = over_hop(ref, step - 1)
        if step < steps - 1:
            for cs_ in copies:
                for c in cs_[step]:
                    c.start()

    def first_sums():
        for c in t_sum + t_inb:
            c.wait_recv()
        parts = []
        for r in range(brow):
            u = natural(r // prow) * prow + r % prow
            acc = ginb[r] + rinb[1, r]
            for s in range(2, group):
                acc += rinb[s, u]
            parts.append(acc)
        return over_tensor(tsum), jnp.stack(parts)

    def first_qv():
        for c in t_qv:
            c.wait_recv()
        return (over_tensor(tqv),)

    def reduce_sums(step):
        go(step, (sbuf, ibuf), (d_sum, d_inb), first_sums)

    def reduce_qv(step):
        go(step, (qbuf,), (d_qv,), first_qv)

    for c in t_sum + t_inb:
        c.start()

    @pl.loop(0, tiles, unroll=2)
    def _(n):
        a1[:, cols(n)] = dot_nt(a0[...], outw[cols(n), :]).astype(BF16)

    @pl.loop(0, tiles)
    def _(n):
        kt = k[n].T
        dqs, dvs = [], []
        for p in range(TILE // LANES):
            v2 = v[n, :, p * LANES : (p + 1) * LANES]
            gs = halves(a1[:, cols(2 * n + p, LANES)])
            dv = None
            for e in range(2):
                h = 2 * p + e
                dprob = dot_nt(v2, gs[e])
                low = pt[n * heads + h]
                prob = low.astype(F32)
                t = prob * dprob
                ds = (t - prob * jnp.sum(t, axis=0, keepdims=True)).astype(BF16)
                dvh = dot(low, gs[e])
                pt[n * heads + h] = ds
                dv = dvh if dv is None else dv + dvh
                dqs.append(dot(kt[h * hd : (h + 1) * hd], ds))
            dvs.append(dv)
        dq = (jnp.concatenate(dqs, axis=0) * hd**-0.5).astype(BF16).T
        dv = jnp.concatenate(dvs, axis=1).astype(BF16)
        hid[n] = dq
        v[n] = dv
        csqv[0, :, cols(n)] = fold8(dq.astype(F32))
        csqv[1, :, cols(n)] = fold8(dv.astype(F32))
        for s, at in ((0, 0), (1, tiles - 1)):

            @pl.when(n == at)
            def _(s=s):
                reduce_sums(s)

    for s in range(2, steps):
        reduce_sums(s)
    for i in range(2):
        tqv[0, i : i + 1, :] = total8(csqv[i])
    for c in t_qv:
        c.start()

    @pl.loop(0, tiles, unroll=2)
    def _(n):
        dks = []
        for p in range(TILE // LANES):
            lo, hi = halves(q[n, :, p * LANES : (p + 1) * LANES])
            dks.append(dot(pt[n * heads + 2 * p], lo) + dot(pt[n * heads + 2 * p + 1], hi))
        k[n] = jnp.concatenate(dks, axis=1).astype(BF16)

    reduce_qv(0)

    @pl.loop(0, tiles, unroll=2)
    def _(t):
        acc = f2[:, cols(t)]
        for n in range(tiles):
            for i, ref in enumerate((hid, k, v)):
                acc += dot_nt(ref[n], qkvw[n + i * tiles, cols(t), :])
        f1[:, cols(t)] = acc
        pltpu.make_async_copy(f1.at[:, cols(t)], grad_out.at[:, cols(t)], lsem.at[20 + t]).start()

    for s in range(1, steps):
        reduce_qv(s)
    last = near + 2 * (steps - 2)
    outs = [load(7, sbuf.at[last], sums_out), load(16, qbuf.at[last], qv_out), load(17, ibuf.at[last], inb_out)]

    for d in far:
        for c in direct[d] + to_x[d] + to_z[d] + list(pass_on[d].values()):
            c.wait_send()
    for c in core_in + [core_ffn] + bias + t_sum + t_inb + t_qv + sum(d_sum + d_inb + d_qv, []):
        c.wait_send()
    c_grad = [pltpu.make_async_copy(f1.at[:, cols(t)], grad_out.at[:, cols(t)], lsem.at[20 + t]) for t in range(tiles)]
    for c in [c_act] + c_grad + outs:
        c.wait()
    assert count[0] <= send.shape[0]


def finish(act, grad, sums, qv, inb, act_out, grad_out, qv_out, outb_out, shift1_out, inb_out, ffnb_out, shift2_out, abuf, gbuf, sbuf, qbuf, ibuf, into, out):
    pieces = 4
    size = act.shape[0] // pieces
    plan = [(sums, sbuf, None), (qv, qbuf, qv_out), (inb, ibuf, inb_out)]
    for i in range(pieces):
        r = pl.ds(i * size, size)
        plan.append((grad.at[r, :], gbuf.at[r, :], grad_out.at[r, :]))
        plan.append((act.at[r, :], abuf.at[r, :], act_out.at[r, :]))
    first = [pltpu.make_async_copy(src, mid, into.at[i]) for i, (src, mid, _) in enumerate(plan)]
    for c in first:
        c.start()
    second = []
    for i, (_, mid, dst) in enumerate(plan):
        first[i].wait()
        if dst is not None:
            second.append(pltpu.make_async_copy(mid, dst, out.at[i]))
            second[-1].start()
        else:
            for j, ref in enumerate((shift2_out, ffnb_out, shift1_out, outb_out)):
                second.append(pltpu.make_async_copy(mid.at[j : j + 1, :], ref, out.at[len(plan) + j]))
                second[-1].start()
    for c in second:
        c.wait()


def step(
    ranks, group,
    tokens, segments, separators, lengths, type_table, qkv_weight, qv_bias, out_weight, out_bias, gain_one, shift_one,
    in_weight, in_bias, ffn_weight, ffn_bias, gain_two, shift_two, cotangent,
):
    pairs, rows, width = tokens.shape
    units = in_weight.shape[1]
    hidden = units * group
    chunks, tiles = hidden // TILE, width // TILE
    brow = units // LANES
    line = group // 2
    near = min(ranks, 8)
    far_bits = (ranks // near).bit_length() - 1
    slots = near + 2 * far_bits + 1
    copies = (line - 1) * 32 + units // TILE + 1 + 4 * (group - 1) + 3 * (near - 1 + far_bits)
    vectors = (type_table, qv_bias, out_bias, gain_one, shift_one, ffn_bias, gain_two, shift_two)
    V = pltpu.VMEM
    outside = pl.BlockSpec(memory_space=pl.ANY)
    act, grad, sums, qv, inb = pl.pallas_call(
        functools.partial(kernel, ranks, group),
        out_shape=(
            jax.ShapeDtypeStruct((rows, width), BF16),
            jax.ShapeDtypeStruct((rows, width), F32),
            jax.ShapeDtypeStruct((4, width), F32),
            jax.ShapeDtypeStruct((2, width), F32),
            jax.ShapeDtypeStruct((brow, 1, LANES), F32),
        ),
        in_specs=[outside] * 17,
        out_specs=(outside,) * 5,
        scratch_shapes=[
            V((3 * tiles, width, TILE), BF16),
            V((width, width), BF16),
            V((chunks, width, TILE), BF16),
            V((hidden, width), BF16),
            V((hidden // LANES, 1, LANES), F32),
            V((tiles, rows, TILE), BF16),
            V((tiles, rows, TILE), BF16),
            V((tiles, rows, TILE), BF16),
            V((HEADS, rows, rows), BF16),
            V((chunks, rows, TILE), F32),
            V((chunks, rows, TILE), BF16),
            V((rows, width), BF16),
            V((rows, width), BF16),
            V((rows, width), F32),
            V((rows, width), F32),
            V((rows, width), F32),
            V((rows, width), BF16),
            V((rows, width), BF16),
            V((rows, width), BF16),
            V((rows, LANES), F32),
            V((4, 8, width), F32),
            V((2, 8, width), F32),
            V((10, width), F32),
            V((hidden // LANES, 1, LANES), F32),
            V((group, brow, 1, LANES), F32),
            V((slots, brow, 1, LANES), F32),
            V((group, 4, width), F32),
            V((slots, 4, width), F32),
            V((group, 2, width), F32),
            V((slots, 2, width), F32),
            [V(x.shape, x.dtype) for x in vectors],
            [V((units,), BF16)] * group,
            pltpu.SMEM((1,), jnp.int32),
            pltpu.SMEM((1, 2), jnp.int32),
            pltpu.SemaphoreType.DMA((3 * tiles + units // TILE,)),
            pltpu.SemaphoreType.DMA((20 + tiles,)),
            pltpu.SemaphoreType.DMA((copies,)),
            pltpu.SemaphoreType.DMA((copies,)),
        ],
        compiler_params=pltpu.CompilerParams(collective_id=0, has_side_effects=True, vmem_limit_bytes=67043328),
    )(
        lengths,
        separators,
        *vectors,
        in_bias,
        tokens.reshape(rows, width),
        cotangent.reshape(rows, width),
        qkv_weight,
        out_weight,
        in_weight,
        ffn_weight,
    )
    vector = jax.ShapeDtypeStruct((1, width), F32)
    act, grad, qv, outb, shift1, inb, ffnb, shift2 = pl.pallas_call(
        finish,
        out_shape=(
            jax.ShapeDtypeStruct((rows, width), BF16),
            jax.ShapeDtypeStruct((rows, width), F32),
            jax.ShapeDtypeStruct((2, width), F32),
            vector,
            vector,
            jax.ShapeDtypeStruct((brow, 1, LANES), F32),
            vector,
            vector,
        ),
        in_specs=[outside] * 5,
        out_specs=(outside,) * 8,
        scratch_shapes=[
            V((rows, width), BF16),
            V((rows, width), F32),
            V((4, width), F32),
            V((2, width), F32),
            V((brow, 1, LANES), F32),
            pltpu.SemaphoreType.DMA((16,)),
            pltpu.SemaphoreType.DMA((16,)),
        ],
    )(act, grad, sums, qv, inb)
    return (
        act.reshape(pairs, rows, width),
        grad.reshape(pairs, rows, width),
        qv,
        outb.reshape(width),
        shift1.reshape(width),
        inb.reshape(units),
        ffnb.reshape(width),
        shift2.reshape(width),
    )


def solution(mesh):
    both = ("dp", "tensor")
    rows = P(both, None, None)
    return jax.shard_map(
        functools.partial(step, mesh.shape["dp"], mesh.shape["tensor"]),
        mesh=mesh,
        in_specs=(rows, P(both, None), P(both, None), P(both))
        + (P(),) * 7
        + (P(None, "tensor"), P("tensor"), P("tensor", None))
        + (P(),) * 3
        + (rows,),
        out_specs=(rows, rows, P(), P(), P(), P("tensor"), P(), P()),
        check_vma=False,
    )
```

```python
import functools

import jax
import jax.numpy as jnp
from jax import lax
from jax.experimental import pallas as pl
from jax.experimental.pallas import tpu as pltpu
from jax.sharding import PartitionSpec as P

HEADS = 16
TILE = 256
LANES = 128
BLOCK = 64
F32 = jnp.float32
BF16 = jnp.bfloat16
MESH = pl.DeviceIdType.MESH
NT = (((1,), (1,)), ((), ()))
root_half = 0.7071067811865476
inv_root_tau = 0.3989422804014327
eps_norm = 1e-06
STOP = 99


def dot(a, b):
    return jnp.dot(a, b, preferred_element_type=F32)


def dot_nt(a, b):
    return lax.dot_general(a, b, NT, preferred_element_type=F32)


def mean_rows(value):
    return jnp.sum(value, axis=-1, keepdims=True) * (1.0 / value.shape[-1])


def cols(n, size=TILE):
    return pl.ds(pl.multiple_of(n * size, size), size)


def fold8(value):
    return jnp.sum(value.reshape(value.shape[0] // 8, 8, value.shape[1]), axis=0)


def total8(value):
    return jnp.sum(value, axis=0, keepdims=True)


def flip(index, bit):
    return index + bit * (1 - 2 * (index // bit % 2))


def kernel(
    ranks, group,
    lengths, separators, table, qv_b, out_b, gain1, shift1, ffn_b, gain2, shift2, in_b, tokens, cot, qkv_w, out_w, in_w, ffn_w,
    act_out, grad_out, sums_out, qv_out, inb_out,
    qkvw, outw, inw, ffw, inb, q, k, v, pt, slope, hid, a0, a1, f0, f1, f2, tok, cotb, sc1, cs, csqv,
    small, ginb, rinb, ibuf, tsum, sbuf, tqv, qbuf,
    raw, inraw, len_s, sep_s, mask, mixt, wsem, lsem, send, recv,
):
    rows, width = tok.shape
    tiles = width // TILE
    hd = width // HEADS
    chunks = inw.shape[0]
    units = in_w.shape[1]
    part = units // 4
    line = group // 2
    brow = units // LANES
    prow = part // LANES
    per = units // TILE
    dp, tensor = lax.axis_index("dp"), lax.axis_index("tensor")
    y, core = tensor // 2, tensor % 2
    near = min(ranks, 8)
    bits = [1 << b for b in range(near.bit_length() - 1)]
    wide = [1 << b for b in range(ranks.bit_length() - 1) if 1 << b >= near]

    def place(d, other):
        return (dp, (y + d + line) % line * 2 + (core + other) % 2)

    def mixed(offset):
        return sum((offset // b + dp // b) % 2 * b for b in bits)

    def rank(offset):
        return (dp // near * near + mixed(offset) if offset < near else flip(dp, offset), tensor)

    barrier = pltpu.get_barrier_semaphore()
    friends = [place(s // 2, s % 2) for s in range(1, group)] + [rank(o) for o in list(range(1, near)) + wide]
    for f in friends:
        pl.semaphore_signal(barrier, inc=1, device_id=f, device_id_type=MESH)

    count = [0]

    def remote(src, dst, device):
        i = count[0]
        count[0] += 1
        return pltpu.make_async_remote_copy(
            src_ref=src, dst_ref=dst, send_sem=send.at[i], recv_sem=recv.at[i], device_id=device, device_id_type=MESH
        )

    def natural(p):
        return (p + dp) % 2 + (p // 2 + dp // 2) % 2 * 2

    cut = width // 4

    def piece(slot, p, i):
        u = slot * units + p * part
        if i == "in":
            return inw.at[u // TILE, :, pl.ds(u % TILE, part)]
        if i < 4:
            return inw.at[u // TILE, pl.ds(i * cut, cut), pl.ds(u % TILE, part)]
        return ffw.at[pl.ds(u + (i - 4) * part // 2, part // 2), :]

    def source(p, i):
        u = pl.multiple_of(natural(p) * part, part)
        if i < 4:
            return in_w.at[pl.ds(i * cut, cut), pl.ds(u, part)]
        return ffn_w.at[pl.ds(u + (i - 4) * part // 2, part // 2), :]

    def load(i, src, dst):
        c = pltpu.make_async_copy(src, dst, lsem.at[i])
        c.start()
        return c

    c_small = [load(8 + i, src, dst) for i, (src, dst) in enumerate(zip((table, qv_b, out_b, gain1, shift1, ffn_b, gain2, shift2), raw))]
    c_tok = load(0, tokens, tok)
    c_small += [load(18, lengths, len_s), load(19, separators, sep_s)]
    c_qkv = []
    for n in range(3 * tiles):
        c = pltpu.make_async_copy(qkv_w.at[:, n * TILE : (n + 1) * TILE], qkvw.at[n], wsem.at[n])
        c.start()
        c_qkv.append(c)
    c_in = []
    for n in range(per):
        c = pltpu.make_async_copy(in_w.at[:, n * TILE : (n + 1) * TILE], inw.at[n], wsem.at[3 * tiles + n])
        c.start()
        c_in.append(c)
    c_out = load(1, out_w, outw)
    c_ffn = load(2, ffn_w, ffw.at[pl.ds(0, units), :])
    c_b = load(3, in_b, inraw[0])
    c_cot = load(4, cot, cotb)

    far = range(1, line)
    near_pieces = [(0, i) for i in range(6)]
    direct = {d: [remote(source(p, i), piece(2 * d, p, i), place(-d, 0)) for p, i in near_pieces + [(3, 4), (3, 5)]] for d in far}
    to_x = {d: [remote(piece(2 * d, p, i), piece(2 * d, p + 1, i), rank(1)) for p, i in near_pieces + [(2, 0), (2, 1)]] for d in far}
    to_z = {d: [remote(piece(2 * d, p, i), piece(2 * d, p + 2, i), rank(2)) for p, i in near_pieces + [(1, 2), (1, 3)]] for d in far}
    pass_on = {d: {(p, i): remote(piece(2 * d, p, i), piece(2 * d + 1, p, i), place(0, 1)) for p in range(4) for i in ("in", 4, 5)} for d in far}
    core_in = [remote(in_w.at[:, n * TILE : (n + 1) * TILE], inw.at[per + n], place(0, 1)) for n in range(per)]
    core_ffn = remote(ffn_w, ffw.at[pl.ds(units, units), :], place(0, 1))
    bias = [remote(in_b, inraw[s], place(-(s // 2), s % 2)) for s in range(1, group)]

    def relay(step):
        for d in far:
            yd, xd, zd, on = direct[d], to_x[d], to_z[d], pass_on[d]
            if step in range(6):
                yd[step].wait_recv()
                xd[step].start()
                zd[step].start()
                if step >= 3:
                    on[0, "in" if step == 3 else step].start()
            if step == "dx":
                zd[0].wait_recv()
                zd[1].wait_recv()
                xd[6].start()
                xd[7].start()
            if step == "dz":
                for i in range(4):
                    xd[i].wait_recv()
                zd[6].start()
                zd[7].start()
                on[1, "in"].start()
                zd[2].wait_recv()
                zd[3].wait_recv()
                on[2, "in"].start()
            if step == "diag":
                for i in (6, 7):
                    xd[i].wait_recv()
                    zd[i].wait_recv()
                on[3, "in"].start()
            if step in ("f4", "f5"):
                i = int(step[1])
                yd[i + 2].wait_recv()
                on[3, i].start()
                xd[i].wait_recv()
                on[1, i].start()
                zd[i].wait_recv()
                on[2, i].start()

    pl.semaphore_wait(barrier, len(friends))
    for c in bias:
        c.start()
    for d in far:
        for c in direct[d]:
            c.start()
    for c in core_in + [core_ffn]:
        c.start()

    for c in c_small:
        c.wait()
    length = len_s[0]
    sep0, sep1 = sep_s[0, 0], sep_s[0, 1]
    small[0:2, :] = raw[0][...].astype(F32)
    small[2:4, :] = raw[1][...].astype(F32)
    for i in range(2, 8):
        small[2 + i : 3 + i, :] = raw[i][...].astype(F32).reshape(1, width)
    c_tok.wait()

    @pl.loop(0, rows // BLOCK, unroll=2)
    def _(i):
        r = cols(i, BLOCK)
        pos = lax.broadcasted_iota(jnp.int32, (BLOCK, width), 0) + i * BLOCK
        second = (pos > sep0) & (pos < length)
        e = tok[r, :].astype(F32) + jnp.where(second, small[1:2, :], small[0:1, :])
        f0[r, :] = e
        a0[r, :] = e.astype(BF16)

    for c in c_qkv[:tiles]:
        c.wait()

    @pl.loop(0, tiles, unroll=2)
    def _(n):
        q[n] = (dot(a0[...], qkvw[n]) + small[2:3, cols(n)]).astype(BF16) * jnp.asarray(hd**-0.5, BF16)

    for c in c_qkv[tiles : 2 * tiles]:
        c.wait()

    @pl.loop(0, tiles, unroll=2)
    def _(n):
        k[n] = dot(a0[...], qkvw[n + tiles]).astype(BF16)

    relay(0)
    for c in c_qkv[2 * tiles :]:
        c.wait()

    @pl.loop(0, tiles, unroll=2)
    def _(n):
        v[n] = (dot(a0[...], qkvw[n + 2 * tiles]) + small[3:4, cols(n)]).astype(BF16)

    mask[...] = jnp.where(lax.broadcasted_iota(jnp.int32, (rows, LANES), 0) < length, 0.0, -1e30)
    low_half = lax.broadcasted_iota(jnp.int32, (rows, LANES), 1) < hd
    zero = jnp.zeros((rows, LANES), BF16)
    heads = TILE // hd

    def halves(pair):
        return jnp.where(low_half, pair, zero), jnp.where(low_half, zero, pair)

    @pl.loop(0, tiles)
    def _(n):
        vt = v[n].T
        hide = jnp.concatenate([mask[...]] * (rows // LANES), axis=1)
        pairs = [(k[n, :, p * LANES : (p + 1) * LANES], qm) for p in range(TILE // LANES) for qm in halves(q[n, :, p * LANES : (p + 1) * LANES])]
        scores = [dot_nt(*pairs[0])]
        for h in range(heads):
            if h + 1 < heads:
                scores.append(dot_nt(*pairs[h + 1]))
            s = scores[h] + hide
            ex = jnp.exp(s - jnp.max(s, axis=0, keepdims=True))
            prob = (ex * (1.0 / jnp.sum(ex, axis=0, keepdims=True))).astype(BF16)
            pt[n * heads + h] = prob
            mixt[n, h * hd : (h + 1) * hd] = dot(vt[h * hd : (h + 1) * hd], prob)
        a1[:, cols(n)] = mixt[n].astype(BF16).T

        for i, at in enumerate((0, 1, 2)):

            @pl.when(n == at)
            def _(i=i):
                relay(i + 1)

    relay("dx")

    c_out.wait()

    @pl.loop(0, tiles, unroll=2)
    def _(n):
        f1[:, cols(n)] = dot(a1[...], outw[:, cols(n)]) + small[4:5, cols(n)] + f0[:, cols(n)]

    relay("dz")

    @pl.loop(0, rows // BLOCK, unroll=2)
    def _(i):
        r = cols(i, BLOCK)
        x = f1[r, :]
        x = x - mean_rows(x)
        scale = lax.rsqrt(mean_rows(x * x) + eps_norm)
        normed = x * scale
        f0[r, :] = normed
        a0[r, :] = (normed * small[5:6, :] + small[6:7, :]).astype(BF16)
        sc1[r, :] = jnp.broadcast_to(scale, (BLOCK, LANES))

    relay(4)

    def hidden_units(c, first, second):
        x = dot(a0[...], inw[c]) + jnp.concatenate([inb[first], inb[second]], axis=1)
        cdf = 0.5 * (1.0 + lax.erf(x * root_half))
        hid[c] = (x * cdf).astype(BF16)
        slope[c] = cdf + x * (inv_root_tau * jnp.exp(-0.5 * x * x))

    for c in c_in + [c_b]:
        c.wait()
    for c in core_in + bias:
        c.wait_recv()
    for t in range(group):
        b = inraw[t][...].astype(F32).reshape(1, units)
        for r in range(brow):
            inb[t * brow + r] = b[:, r * LANES : (r + 1) * LANES]

    @pl.loop(0, 2 * per, unroll=2)
    def _(c):
        hidden_units(c, 2 * c, 2 * c + 1)

    def shuffled(r):
        return r // brow * brow + natural(r % brow // prow) * prow + r % prow

    def units_of(i):
        for d in far:
            for p in range(4):
                if (p * part) // TILE == i:
                    pass_on[d][p, "in"].wait_recv()

        @pl.loop(2, group, unroll=2)
        def _(t):
            c = t * per + i
            hidden_units(c, shuffled(2 * c), shuffled(2 * c + 1))

    units_of(0)
    relay(5)
    for i in range(1, per):
        if i == per - 2 or per == 2:
            relay("diag")
        units_of(i)
    c_ffn.wait()
    core_ffn.wait_recv()

    @pl.loop(0, tiles)
    def _(t):
        acc = dot(hid[0], ffw[0:TILE, cols(t)])
        for c in range(1, 2 * per):
            acc += dot(hid[c], ffw[c * TILE : (c + 1) * TILE, cols(t)])
        f1[:, cols(t)] = acc

        @pl.when(t == tiles - 2)
        def _():
            relay("f4")

    half = part // 2
    blocks = [(t * units + p * part + h * half, h > 0 and p > 0) for t in range(2, group) for p in range(4) for h in range(2)]
    if half % LANES:
        ready, late = [], [u for u, _ in blocks]
    else:
        ready, late = [u for u, last in blocks if not last], [u for u, last in blocks if last]

    def contract(t, acc, starts):
        step = max(1, TILE // half)
        for i in range(0, len(starts), step):
            us = starts[i : i + step]
            if us == list(range(us[0], us[0] + TILE, half)) and us[0] % TILE == 0:
                left, right = hid[us[0] // TILE], ffw[us[0] : us[0] + TILE, cols(t)]
            else:
                left = jnp.concatenate([hid[u // TILE, :, u % TILE : u % TILE + half] for u in us], axis=1)
                right = jnp.concatenate([ffw[u : u + half, cols(t)] for u in us], axis=0)
            acc += dot(left, right)
        return acc

    if ready:
        for d in far:
            for p in range(4):
                pass_on[d][p, 4].wait_recv()
            pass_on[d][0, 5].wait_recv()

        @pl.loop(0, tiles)
        def _(t):
            f1[:, cols(t)] = contract(t, f1[:, cols(t)], ready)

    relay("f5")
    for d in far:
        for p in range(4):
            if not ready:
                pass_on[d][p, 4].wait_recv()
            if p > 0 or not ready:
                pass_on[d][p, 5].wait_recv()

    @pl.loop(0, tiles)
    def _(t):
        f1[:, cols(t)] = contract(t, f1[:, cols(t)], late)

    c_cot.wait()
    cs[...] = jnp.zeros_like(cs)

    @pl.loop(0, rows // BLOCK, unroll=2)
    def _(i):
        r = cols(i, BLOCK)
        pos = lax.broadcasted_iota(jnp.int32, (BLOCK, 1), 0) + i * BLOCK
        keep = ((pos > 0) & (pos < length) & (pos != sep0) & (pos != sep1)).astype(F32)
        x = f0[r, :] * small[5:6, :] + small[6:7, :] + f1[r, :] + small[7:8, :]
        x = x - mean_rows(x)
        scale = lax.rsqrt(mean_rows(x * x) + eps_norm)
        normed = x * scale
        tok[r, :] = (normed * small[8:9, :] + small[9:10, :]).astype(BF16)
        g = cotb[r, :].astype(F32) * keep
        s = g * small[8:9, :]
        gs = scale * (s - mean_rows(s) - normed * mean_rows(s * normed))
        low = gs.astype(BF16)
        f2[r, :] = gs
        a1[r, :] = low
        cs[0] += fold8(g)
        cs[1] += fold8(low.astype(F32))

    c_act = load(5, tok, act_out)

    @pl.loop(0, chunks, unroll=2)
    def _(c):
        gi = (dot_nt(a1[...], ffw[cols(c), :]) * slope[c]).astype(BF16)
        hid[c] = gi
        s = total8(gi.astype(F32))
        ginb[2 * c] = s[:, :LANES]
        ginb[2 * c + 1] = s[:, LANES:]

    @pl.loop(0, tiles)
    def _(t):
        acc = dot_nt(hid[0], inw[0, cols(t), :])
        for c in range(1, chunks):
            acc += dot_nt(hid[c], inw[c, cols(t), :])
        f1[:, cols(t)] = acc

    @pl.loop(0, rows // BLOCK, unroll=2)
    def _(i):
        r = cols(i, BLOCK)
        g = f1[r, :] + f2[r, :]
        s = g * small[5:6, :]
        normed = f0[r, :]
        gs = sc1[r, 0:1] * (s - mean_rows(s) - normed * mean_rows(s * normed))
        low = gs.astype(BF16)
        f2[r, :] = gs
        a0[r, :] = low
        cs[2] += fold8(g)
        cs[3] += fold8(low.astype(F32))

    for i in range(4):
        tsum[0, i : i + 1, :] = total8(cs[i])
    peers = [(s, place(s // 2, s % 2)) for s in range(1, group)]
    t_sum = [remote(tsum.at[0], tsum.at[s], dev) for s, dev in peers]
    t_inb = [remote(ginb.at[pl.ds(s * brow, brow)], rinb.at[s], dev) for s, dev in peers]
    hops = [list(range(1, near))] + [[w] for w in wide]
    steps = len(hops) + 1

    def spread(ref):
        copies, base = [], 0
        for hop in hops:
            copies.append([remote(ref.at[base], ref.at[base + i + 1], rank(o)) for i, o in enumerate(hop)])
            base += len(hop) + 1
        return copies

    d_sum, d_inb, d_qv = spread(sbuf), spread(ibuf), spread(qbuf)
    t_qv = [remote(tqv.at[0], tqv.at[s], dev) for s, dev in peers]

    def over_tensor(ref):
        acc = None
        for t in range(group):
            s = (y - t // 2 + line) % line * 2 + (core + t) % 2
            acc = ref[s] if acc is None else acc + ref[s]
        return acc

    def over_hop(ref, hop):
        if hop == 0:
            acc = ref[mixed(0)]
            for o in range(1, near):
                acc += ref[mixed(o)]
            return acc
        base = near + 2 * (hop - 1)
        return ref[base] + ref[base + 1]

    def go(step, buffers, copies, totals):
        if step == 0:
            for ref, value in zip(buffers, totals()):
                ref[0] = value
        else:
            for ref, cs_ in zip(buffers, copies):
                for c in cs_[step - 1]:
                    c.wait_recv()
                ref[near + 2 * (step - 1)] = over_hop(ref, step - 1)
        if step < steps - 1:
            for cs_ in copies:
                for c in cs_[step]:
                    c.start()

    def first_sums():
        for c in t_sum + t_inb:
            c.wait_recv()
        parts = []
        for r in range(brow):
            u = natural(r // prow) * prow + r % prow
            acc = ginb[r] + rinb[1, r]
            for s in range(2, group):
                acc += rinb[s, u]
            parts.append(acc)
        return over_tensor(tsum), jnp.stack(parts)

    def first_qv():
        for c in t_qv:
            c.wait_recv()
        return (over_tensor(tqv),)

    def reduce_sums(step):
        go(step, (sbuf, ibuf), (d_sum, d_inb), first_sums)

    def reduce_qv(step):
        go(step, (qbuf,), (d_qv,), first_qv)

    for c in t_sum + t_inb:
        c.start()

    @pl.loop(0, tiles, unroll=2)
    def _(n):
        a1[:, cols(n)] = dot_nt(a0[...], outw[cols(n), :]).astype(BF16)

    @pl.loop(0, tiles)
    def _(n):
        kt = k[n].T
        gt = a1[:, cols(n)].T.astype(F32)
        inner = jnp.sum((gt * mixt[n]).reshape(heads, hd, rows), axis=1)
        pairs = [(v[n, :, p * LANES : (p + 1) * LANES], gm) for p in range(TILE // LANES) for gm in halves(a1[:, cols(2 * n + p, LANES)])]
        dqs, dvh = [], []
        dprobs = [dot_nt(*pairs[0])]
        for h in range(heads):
            if h + 1 < heads:
                dprobs.append(dot_nt(*pairs[h + 1]))
            low = pt[n * heads + h]
            ds = (low.astype(F32) * (dprobs[h] - inner[h : h + 1])).astype(BF16)
            dvh.append(dot(low, pairs[h][1]))
            pt[n * heads + h] = ds
            dqs.append(dot(kt[h * hd : (h + 1) * hd], ds))
        dvs = [dvh[2 * p] + dvh[2 * p + 1] for p in range(TILE // LANES)]
        dq = (jnp.concatenate(dqs, axis=0) * hd**-0.5).astype(BF16).T
        dv = jnp.concatenate(dvs, axis=1).astype(BF16)
        hid[n] = dq
        v[n] = dv
        csqv[0, :, cols(n)] = fold8(dq.astype(F32))
        csqv[1, :, cols(n)] = fold8(dv.astype(F32))
        @pl.when(n == 0)
        def _():
            reduce_sums(0)

    for i in range(2):
        tqv[0, i : i + 1, :] = total8(csqv[i])
    for c in t_qv:
        c.start()

    @pl.loop(0, tiles, unroll=2)
    def _(n):
        dks = []
        for p in range(TILE // LANES):
            lo, hi = halves(q[n, :, p * LANES : (p + 1) * LANES])
            dks.append(dot(pt[n * heads + 2 * p], lo) + dot(pt[n * heads + 2 * p + 1], hi))
        k[n] = jnp.concatenate(dks, axis=1).astype(BF16)

    reduce_qv(0)

    @pl.loop(0, tiles, unroll=2)
    def _(t):
        acc = f2[:, cols(t)]
        for n in range(tiles):
            for i, ref in enumerate((hid, k, v)):
                acc += dot_nt(ref[n], qkvw[n + i * tiles, cols(t), :])
        f1[:, cols(t)] = acc
        pltpu.make_async_copy(f1.at[:, cols(t)], grad_out.at[:, cols(t)], lsem.at[20 + t]).start()

    for s in range(1, steps):
        reduce_sums(s)
        reduce_qv(s)
    last = near + 2 * (steps - 2)
    outs = [load(7, sbuf.at[last], sums_out), load(16, qbuf.at[last], qv_out), load(17, ibuf.at[last], inb_out)]

    for d in far:
        for c in direct[d] + to_x[d] + to_z[d] + list(pass_on[d].values()):
            c.wait_send()
    for c in core_in + [core_ffn] + bias + t_sum + t_inb + t_qv + sum(d_sum + d_inb + d_qv, []):
        c.wait_send()
    c_grad = [pltpu.make_async_copy(f1.at[:, cols(t)], grad_out.at[:, cols(t)], lsem.at[20 + t]) for t in range(tiles)]
    for c in [c_act] + c_grad + outs:
        c.wait()
    assert count[0] <= send.shape[0]


def finish(act, grad, sums, qv, inb, act_out, grad_out, qv_out, outb_out, shift1_out, inb_out, ffnb_out, shift2_out, abuf, gbuf, sbuf, qbuf, ibuf, into, out):
    pieces = 4
    size = act.shape[0] // pieces
    plan = [(sums, sbuf, None), (qv, qbuf, qv_out), (inb, ibuf, inb_out)]
    for i in range(pieces):
        r = pl.ds(i * size, size)
        plan.append((grad.at[r, :], gbuf.at[r, :], grad_out.at[r, :]))
        plan.append((act.at[r, :], abuf.at[r, :], act_out.at[r, :]))
    first = [pltpu.make_async_copy(src, mid, into.at[i]) for i, (src, mid, _) in enumerate(plan)]
    for c in first:
        c.start()
    second = []
    for i, (_, mid, dst) in enumerate(plan):
        first[i].wait()
        if dst is not None:
            second.append(pltpu.make_async_copy(mid, dst, out.at[i]))
            second[-1].start()
        else:
            for j, ref in enumerate((shift2_out, ffnb_out, shift1_out, outb_out)):
                second.append(pltpu.make_async_copy(mid.at[j : j + 1, :], ref, out.at[len(plan) + j]))
                second[-1].start()
    for c in second:
        c.wait()


def step(
    ranks, group,
    tokens, segments, separators, lengths, type_table, qkv_weight, qv_bias, out_weight, out_bias, gain_one, shift_one,
    in_weight, in_bias, ffn_weight, ffn_bias, gain_two, shift_two, cotangent,
):
    pairs, rows, width = tokens.shape
    units = in_weight.shape[1]
    hidden = units * group
    chunks, tiles = hidden // TILE, width // TILE
    brow = units // LANES
    line = group // 2
    near = min(ranks, 8)
    far_bits = (ranks // near).bit_length() - 1
    slots = near + 2 * far_bits + 1
    copies = (line - 1) * 36 + units // TILE + 1 + 4 * (group - 1) + 3 * (near - 1 + far_bits)
    vectors = (type_table, qv_bias, out_bias, gain_one, shift_one, ffn_bias, gain_two, shift_two)
    V = pltpu.VMEM
    outside = pl.BlockSpec(memory_space=pl.ANY)
    act, grad, sums, qv, inb = pl.pallas_call(
        functools.partial(kernel, ranks, group),
        out_shape=(
            jax.ShapeDtypeStruct((rows, width), BF16),
            jax.ShapeDtypeStruct((rows, width), F32),
            jax.ShapeDtypeStruct((4, width), F32),
            jax.ShapeDtypeStruct((2, width), F32),
            jax.ShapeDtypeStruct((brow, 1, LANES), F32),
        ),
        in_specs=[outside] * 17,
        out_specs=(outside,) * 5,
        scratch_shapes=[
            V((3 * tiles, width, TILE), BF16),
            V((width, width), BF16),
            V((chunks, width, TILE), BF16),
            V((hidden, width), BF16),
            V((hidden // LANES, 1, LANES), F32),
            V((tiles, rows, TILE), BF16),
            V((tiles, rows, TILE), BF16),
            V((tiles, rows, TILE), BF16),
            V((HEADS, rows, rows), BF16),
            V((chunks, rows, TILE), F32),
            V((chunks, rows, TILE), BF16),
            V((rows, width), BF16),
            V((rows, width), BF16),
            V((rows, width), F32),
            V((rows, width), F32),
            V((rows, width), F32),
            V((rows, width), BF16),
            V((rows, width), BF16),
            V((rows, LANES), F32),
            V((4, 8, width), F32),
            V((2, 8, width), F32),
            V((10, width), F32),
            V((hidden // LANES, 1, LANES), F32),
            V((group, brow, 1, LANES), F32),
            V((slots, brow, 1, LANES), F32),
            V((group, 4, width), F32),
            V((slots, 4, width), F32),
            V((group, 2, width), F32),
            V((slots, 2, width), F32),
            [V(x.shape, x.dtype) for x in vectors],
            [V((units,), BF16)] * group,
            pltpu.SMEM((1,), jnp.int32),
            pltpu.SMEM((1, 2), jnp.int32),
            V((rows, LANES), F32),
            V((tiles, TILE, rows), F32),
            pltpu.SemaphoreType.DMA((3 * tiles + units // TILE,)),
            pltpu.SemaphoreType.DMA((20 + tiles,)),
            pltpu.SemaphoreType.DMA((copies,)),
            pltpu.SemaphoreType.DMA((copies,)),
        ],
        compiler_params=pltpu.CompilerParams(collective_id=0, has_side_effects=True, vmem_limit_bytes=67043328),
    )(
        lengths,
        separators,
        *vectors,
        in_bias,
        tokens.reshape(rows, width),
        cotangent.reshape(rows, width),
        qkv_weight,
        out_weight,
        in_weight,
        ffn_weight,
    )
    vector = jax.ShapeDtypeStruct((1, width), F32)
    act, grad, qv, outb, shift1, inb, ffnb, shift2 = pl.pallas_call(
        finish,
        out_shape=(
            jax.ShapeDtypeStruct((rows, width), BF16),
            jax.ShapeDtypeStruct((rows, width), F32),
            jax.ShapeDtypeStruct((2, width), F32),
            vector,
            vector,
            jax.ShapeDtypeStruct((brow, 1, LANES), F32),
            vector,
            vector,
        ),
        in_specs=[outside] * 5,
        out_specs=(outside,) * 8,
        scratch_shapes=[
            V((rows, width), BF16),
            V((rows, width), F32),
            V((4, width), F32),
            V((2, width), F32),
            V((brow, 1, LANES), F32),
            pltpu.SemaphoreType.DMA((16,)),
            pltpu.SemaphoreType.DMA((16,)),
        ],
    )(act, grad, sums, qv, inb)
    return (
        act.reshape(pairs, rows, width),
        grad.reshape(pairs, rows, width),
        qv,
        outb.reshape(width),
        shift1.reshape(width),
        inb.reshape(units),
        ffnb.reshape(width),
        shift2.reshape(width),
    )


def solution(mesh):
    both = ("dp", "tensor")
    rows = P(both, None, None)
    return jax.shard_map(
        functools.partial(step, mesh.shape["dp"], mesh.shape["tensor"]),
        mesh=mesh,
        in_specs=(rows, P(both, None), P(both, None), P(both))
        + (P(),) * 7
        + (P(None, "tensor"), P("tensor"), P("tensor", None))
        + (P(),) * 3
        + (rows,),
        out_specs=(rows, rows, P(), P(), P(), P("tensor"), P(), P()),
        check_vma=False,
    )
```

```python
import functools

import jax
import jax.numpy as jnp
from jax import lax
from jax.experimental import pallas as pl
from jax.experimental.pallas import tpu as pltpu
from jax.sharding import PartitionSpec as P

HEADS = 16
TILE = 256
LANES = 128
BLOCK = 64
F32 = jnp.float32
BF16 = jnp.bfloat16
MESH = pl.DeviceIdType.MESH
NT = (((1,), (1,)), ((), ()))
root_half = 0.7071067811865476
inv_root_tau = 0.3989422804014327
eps_norm = 1e-06
STOP = 99


def dot(a, b):
    return jnp.dot(a, b, preferred_element_type=F32)


def dot_nt(a, b):
    return lax.dot_general(a, b, NT, preferred_element_type=F32)


def mean_rows(value):
    return jnp.sum(value, axis=-1, keepdims=True) * (1.0 / value.shape[-1])


def cols(n, size=TILE):
    return pl.ds(pl.multiple_of(n * size, size), size)


def fold8(value):
    return jnp.sum(value.reshape(value.shape[0] // 8, 8, value.shape[1]), axis=0)


def total8(value):
    return jnp.sum(value, axis=0, keepdims=True)


def flip(index, bit):
    return index + bit * (1 - 2 * (index // bit % 2))


def kernel(
    ranks, group,
    lengths, separators, table, qv_b, out_b, gain1, shift1, ffn_b, gain2, shift2, in_b, tokens, cot, qkv_w, out_w, in_w, ffn_w,
    act_out, grad_out, sums_out, qv_out, inb_out,
    qkvw, outw, inw, ffw, inb, q, k, v, pt, slope, hid, a0, a1, f0, f1, f2, tok, cotb, sc1, cs, csqv,
    small, ginb, rinb, ibuf, tsum, sbuf, tqv, qbuf,
    raw, inraw, len_s, sep_s, mask, mixt, wsem, lsem, send, recv,
):
    rows, width = tok.shape
    tiles = width // TILE
    hd = width // HEADS
    chunks = inw.shape[0]
    units = in_w.shape[1]
    part = units // 4
    line = group // 2
    brow = units // LANES
    prow = part // LANES
    per = units // TILE
    dp, tensor = lax.axis_index("dp"), lax.axis_index("tensor")
    y, core = tensor // 2, tensor % 2
    near = min(ranks, 8)
    bits = [1 << b for b in range(near.bit_length() - 1)]
    wide = [1 << b for b in range(ranks.bit_length() - 1) if 1 << b >= near]

    def place(d, other):
        return (dp, (y + d + line) % line * 2 + (core + other) % 2)

    def mixed(offset):
        return sum((offset // b + dp // b) % 2 * b for b in bits)

    def rank(offset):
        return (dp // near * near + mixed(offset) if offset < near else flip(dp, offset), tensor)

    barrier = pltpu.get_barrier_semaphore()
    friends = [place(s // 2, s % 2) for s in range(1, group)] + [rank(o) for o in list(range(1, near)) + wide]
    for f in friends:
        pl.semaphore_signal(barrier, inc=1, device_id=f, device_id_type=MESH)

    count = [0]

    def remote(src, dst, device):
        i = count[0]
        count[0] += 1
        return pltpu.make_async_remote_copy(
            src_ref=src, dst_ref=dst, send_sem=send.at[i], recv_sem=recv.at[i], device_id=device, device_id_type=MESH
        )

    def natural(p):
        return (p + dp) % 2 + (p // 2 + dp // 2) % 2 * 2

    cut = width // 4

    def piece(slot, p, i):
        u = slot * units + p * part
        if i == "in":
            return inw.at[u // TILE, :, pl.ds(u % TILE, part)]
        if i < 4:
            return inw.at[u // TILE, pl.ds(i * cut, cut), pl.ds(u % TILE, part)]
        return ffw.at[pl.ds(u + (i - 4) * part // 2, part // 2), :]

    def source(p, i):
        u = pl.multiple_of(natural(p) * part, part)
        if i < 4:
            return in_w.at[pl.ds(i * cut, cut), pl.ds(u, part)]
        return ffn_w.at[pl.ds(u + (i - 4) * part // 2, part // 2), :]

    def load(i, src, dst):
        c = pltpu.make_async_copy(src, dst, lsem.at[i])
        c.start()
        return c

    c_small = [load(8 + i, src, dst) for i, (src, dst) in enumerate(zip((table, qv_b, out_b, gain1, shift1, ffn_b, gain2, shift2), raw))]
    c_tok = load(0, tokens, tok)
    c_small += [load(18, lengths, len_s), load(19, separators, sep_s)]
    c_qkv = [pltpu.make_async_copy(qkv_w.at[:, n * TILE : (n + 1) * TILE], qkvw.at[n], wsem.at[n]) for n in range(3 * tiles)]
    for c in c_qkv[:tiles]:
        c.start()

    far = range(1, line)
    near_pieces = [(0, i) for i in range(6)]
    direct = {d: [remote(source(p, i), piece(2 * d, p, i), place(-d, 0)) for p, i in near_pieces + [(3, 4), (3, 5)]] for d in far}
    to_x = {d: [remote(piece(2 * d, p, i), piece(2 * d, p + 1, i), rank(1)) for p, i in near_pieces + [(2, 0), (2, 1)]] for d in far}
    to_z = {d: [remote(piece(2 * d, p, i), piece(2 * d, p + 2, i), rank(2)) for p, i in near_pieces + [(1, 2), (1, 3)]] for d in far}
    pass_on = {d: {(p, i): remote(piece(2 * d, p, i), piece(2 * d + 1, p, i), place(0, 1)) for p in range(4) for i in ("in", 4, 5)} for d in far}
    core_in = [remote(in_w.at[:, n * TILE : (n + 1) * TILE], inw.at[per + n], place(0, 1)) for n in range(per)]
    core_ffn = remote(ffn_w, ffw.at[pl.ds(units, units), :], place(0, 1))
    bias = [remote(in_b, inraw[s], place(-(s // 2), s % 2)) for s in range(1, group)]

    def relay(step):
        for d in far:
            yd, xd, zd, on = direct[d], to_x[d], to_z[d], pass_on[d]
            if step in range(6):
                yd[step].wait_recv()
                xd[step].start()
                zd[step].start()
                if step >= 3:
                    on[0, "in" if step == 3 else step].start()
            if step == "dx":
                zd[0].wait_recv()
                zd[1].wait_recv()
                xd[6].start()
                xd[7].start()
            if step == "dz":
                for i in range(4):
                    xd[i].wait_recv()
                zd[6].start()
                zd[7].start()
                on[1, "in"].start()
                zd[2].wait_recv()
                zd[3].wait_recv()
                on[2, "in"].start()
            if step == "diag":
                for i in (6, 7):
                    xd[i].wait_recv()
                    zd[i].wait_recv()
                on[3, "in"].start()
            if step in ("f4", "f5"):
                i = int(step[1])
                yd[i + 2].wait_recv()
                on[3, i].start()
                xd[i].wait_recv()
                on[1, i].start()
                zd[i].wait_recv()
                on[2, i].start()

    pl.semaphore_wait(barrier, len(friends))
    for c in bias:
        c.start()
    for d in far:
        for c in direct[d]:
            c.start()
    for c in c_qkv[tiles:]:
        c.start()
    for c in core_in + [core_ffn]:
        c.start()
    c_out = load(1, out_w, outw)
    c_in = [pltpu.make_async_copy(in_w.at[:, n * TILE : (n + 1) * TILE], inw.at[n], wsem.at[3 * tiles + n]) for n in range(per)]
    for c in c_in:
        c.start()
    c_b = load(3, in_b, inraw[0])
    c_ffn = load(2, ffn_w, ffw.at[pl.ds(0, units), :])
    c_cot = load(4, cot, cotb)

    for c in c_small:
        c.wait()
    length = len_s[0]
    sep0, sep1 = sep_s[0, 0], sep_s[0, 1]
    small[0:2, :] = raw[0][...].astype(F32)
    small[2:4, :] = raw[1][...].astype(F32)
    for i in range(2, 8):
        small[2 + i : 3 + i, :] = raw[i][...].astype(F32).reshape(1, width)
    c_tok.wait()

    @pl.loop(0, rows // BLOCK, unroll=2)
    def _(i):
        r = cols(i, BLOCK)
        pos = lax.broadcasted_iota(jnp.int32, (BLOCK, width), 0) + i * BLOCK
        second = (pos > sep0) & (pos < length)
        e = tok[r, :].astype(F32) + jnp.where(second, small[1:2, :], small[0:1, :])
        f0[r, :] = e
        a0[r, :] = e.astype(BF16)

    for c in c_qkv[:tiles]:
        c.wait()

    @pl.loop(0, tiles, unroll=2)
    def _(n):
        q[n] = (dot(a0[...], qkvw[n]) + small[2:3, cols(n)]).astype(BF16) * jnp.asarray(hd**-0.5, BF16)

    for c in c_qkv[tiles : 2 * tiles]:
        c.wait()

    @pl.loop(0, tiles, unroll=2)
    def _(n):
        k[n] = dot(a0[...], qkvw[n + tiles]).astype(BF16)

    relay(0)
    for c in c_qkv[2 * tiles :]:
        c.wait()

    @pl.loop(0, tiles, unroll=2)
    def _(n):
        v[n] = (dot(a0[...], qkvw[n + 2 * tiles]) + small[3:4, cols(n)]).astype(BF16)

    mask[...] = jnp.where(lax.broadcasted_iota(jnp.int32, (rows, LANES), 0) < length, 0.0, -1e30)
    low_half = lax.broadcasted_iota(jnp.int32, (rows, LANES), 1) < hd
    zero = jnp.zeros((rows, LANES), BF16)
    heads = TILE // hd

    def halves(pair):
        return jnp.where(low_half, pair, zero), jnp.where(low_half, zero, pair)

    @pl.loop(0, tiles)
    def _(n):
        vt = v[n].T
        hide = jnp.concatenate([mask[...]] * (rows // LANES), axis=1)
        pairs = [(k[n, :, p * LANES : (p + 1) * LANES], qm) for p in range(TILE // LANES) for qm in halves(q[n, :, p * LANES : (p + 1) * LANES])]
        scores = [dot_nt(*pairs[0])]
        for h in range(heads):
            if h + 1 < heads:
                scores.append(dot_nt(*pairs[h + 1]))
            s = scores[h] + hide
            ex = jnp.exp(s - jnp.max(s, axis=0, keepdims=True))
            prob = (ex * (1.0 / jnp.sum(ex, axis=0, keepdims=True))).astype(BF16)
            pt[n * heads + h] = prob
            mixt[n, h * hd : (h + 1) * hd] = dot(vt[h * hd : (h + 1) * hd], prob)
        a1[:, cols(n)] = mixt[n].astype(BF16).T

        for i, at in enumerate((0, 1, 2)):

            @pl.when(n == at)
            def _(i=i):
                relay(i + 1)

    relay("dx")

    c_out.wait()

    @pl.loop(0, tiles, unroll=2)
    def _(n):
        f1[:, cols(n)] = dot(a1[...], outw[:, cols(n)]) + small[4:5, cols(n)] + f0[:, cols(n)]

    relay("dz")

    @pl.loop(0, rows // BLOCK, unroll=2)
    def _(i):
        r = cols(i, BLOCK)
        x = f1[r, :]
        x = x - mean_rows(x)
        scale = lax.rsqrt(mean_rows(x * x) + eps_norm)
        normed = x * scale
        f0[r, :] = normed
        a0[r, :] = (normed * small[5:6, :] + small[6:7, :]).astype(BF16)
        sc1[r, :] = jnp.broadcast_to(scale, (BLOCK, LANES))

    relay(4)

    def hidden_units(c, first, second):
        x = dot(a0[...], inw[c]) + jnp.concatenate([inb[first], inb[second]], axis=1)
        cdf = 0.5 * (1.0 + lax.erf(x * root_half))
        hid[c] = (x * cdf).astype(BF16)
        slope[c] = cdf + x * (inv_root_tau * jnp.exp(-0.5 * x * x))

    for c in c_in + [c_b]:
        c.wait()
    for c in core_in + bias:
        c.wait_recv()
    for t in range(group):
        b = inraw[t][...].astype(F32).reshape(1, units)
        for r in range(brow):
            inb[t * brow + r] = b[:, r * LANES : (r + 1) * LANES]

    @pl.loop(0, 2 * per, unroll=2)
    def _(c):
        hidden_units(c, 2 * c, 2 * c + 1)

    def shuffled(r):
        return r // brow * brow + natural(r % brow // prow) * prow + r % prow

    def units_of(i):
        for d in far:
            for p in range(4):
                if (p * part) // TILE == i:
                    pass_on[d][p, "in"].wait_recv()

        @pl.loop(2, group, unroll=2)
        def _(t):
            c = t * per + i
            hidden_units(c, shuffled(2 * c), shuffled(2 * c + 1))

    units_of(0)
    relay(5)
    for i in range(1, per - 1):
        units_of(i)
    relay("diag")
    c_ffn.wait()
    core_ffn.wait_recv()

    @pl.loop(0, tiles)
    def _(t):
        acc = dot(hid[0], ffw[0:TILE, cols(t)])
        for c in range(1, 2 * per):
            acc += dot(hid[c], ffw[c * TILE : (c + 1) * TILE, cols(t)])
        f1[:, cols(t)] = acc

    units_of(per - 1)
    relay("f4")

    half = part // 2
    blocks = [(t, p, h, t * units + p * part + h * half) for t in range(2, group) for p in range(4) for h in range(2)]

    def phase(t, p, h):
        if half % LANES:
            return 2
        passed = t % 2 if p else 0
        return passed + (h if p else 0)

    waves = [[u for t, p, h, u in blocks if phase(t, p, h) == w] for w in range(3)]

    def contract(t, acc, starts):
        step = max(1, TILE // half)
        for i in range(0, len(starts), step):
            us = starts[i : i + step]
            if us == list(range(us[0], us[0] + TILE, half)) and us[0] % TILE == 0:
                left, right = hid[us[0] // TILE], ffw[us[0] : us[0] + TILE, cols(t)]
            else:
                left = jnp.concatenate([hid[u // TILE, :, u % TILE : u % TILE + half] for u in us], axis=1)
                right = jnp.concatenate([ffw[u : u + half, cols(t)] for u in us], axis=0)
            acc += dot(left, right)
        return acc

    def add_wave(starts):
        if starts:

            @pl.loop(0, tiles)
            def _(t):
                f1[:, cols(t)] = contract(t, f1[:, cols(t)], starts)

    for d in far:
        pass_on[d][0, 4].wait_recv()
        pass_on[d][0, 5].wait_recv()
    add_wave(waves[0])
    relay("f5")
    for d in far:
        for p in range(1, 4):
            pass_on[d][p, 4].wait_recv()
    add_wave(waves[1])
    for d in far:
        for p in range(1, 4):
            pass_on[d][p, 5].wait_recv()
    add_wave(waves[2])

    c_cot.wait()
    cs[...] = jnp.zeros_like(cs)

    @pl.loop(0, rows // BLOCK, unroll=4)
    def _(i):
        r = cols(i, BLOCK)
        pos = lax.broadcasted_iota(jnp.int32, (BLOCK, 1), 0) + i * BLOCK
        keep = ((pos > 0) & (pos < length) & (pos != sep0) & (pos != sep1)).astype(F32)
        x = f0[r, :] * small[5:6, :] + small[6:7, :] + f1[r, :] + small[7:8, :]
        x = x - mean_rows(x)
        scale = lax.rsqrt(mean_rows(x * x) + eps_norm)
        normed = x * scale
        tok[r, :] = (normed * small[8:9, :] + small[9:10, :]).astype(BF16)
        g = cotb[r, :].astype(F32) * keep
        s = g * small[8:9, :]
        gs = scale * (s - mean_rows(s) - normed * mean_rows(s * normed))
        low = gs.astype(BF16)
        f2[r, :] = gs
        a1[r, :] = low
        cs[0] += fold8(g)
        cs[1] += fold8(low.astype(F32))

    c_act = load(5, tok, act_out)

    @pl.loop(0, chunks, unroll=4)
    def _(c):
        gi = (dot_nt(a1[...], ffw[cols(c), :]) * slope[c]).astype(BF16)
        hid[c] = gi
        s = total8(gi.astype(F32))
        ginb[2 * c] = s[:, :LANES]
        ginb[2 * c + 1] = s[:, LANES:]

    @pl.loop(0, tiles)
    def _(t):
        acc = dot_nt(hid[0], inw[0, cols(t), :])
        for c in range(1, chunks):
            acc += dot_nt(hid[c], inw[c, cols(t), :])
        f1[:, cols(t)] = acc

    @pl.loop(0, rows // BLOCK, unroll=4)
    def _(i):
        r = cols(i, BLOCK)
        g = f1[r, :] + f2[r, :]
        s = g * small[5:6, :]
        normed = f0[r, :]
        gs = sc1[r, 0:1] * (s - mean_rows(s) - normed * mean_rows(s * normed))
        low = gs.astype(BF16)
        f2[r, :] = gs
        a0[r, :] = low
        cs[2] += fold8(g)
        cs[3] += fold8(low.astype(F32))

    for i in range(4):
        tsum[0, i : i + 1, :] = total8(cs[i])
    peers = [(s, place(s // 2, s % 2)) for s in range(1, group)]
    t_sum = [remote(tsum.at[0], tsum.at[s], dev) for s, dev in peers]
    t_inb = [remote(ginb.at[pl.ds(s * brow, brow)], rinb.at[s], dev) for s, dev in peers]
    hops = [list(range(1, near))] + [[w] for w in wide]
    steps = len(hops) + 1

    def spread(ref):
        copies, base = [], 0
        for hop in hops:
            copies.append([remote(ref.at[base], ref.at[base + i + 1], rank(o)) for i, o in enumerate(hop)])
            base += len(hop) + 1
        return copies

    d_sum, d_inb, d_qv = spread(sbuf), spread(ibuf), spread(qbuf)
    t_qv = [remote(tqv.at[0], tqv.at[s], dev) for s, dev in peers]

    def over_tensor(ref):
        acc = None
        for t in range(group):
            s = (y - t // 2 + line) % line * 2 + (core + t) % 2
            acc = ref[s] if acc is None else acc + ref[s]
        return acc

    def over_hop(ref, hop):
        if hop == 0:
            acc = ref[mixed(0)]
            for o in range(1, near):
                acc += ref[mixed(o)]
            return acc
        base = near + 2 * (hop - 1)
        return ref[base] + ref[base + 1]

    def go(step, buffers, copies, totals):
        if step == 0:
            for ref, value in zip(buffers, totals()):
                ref[0] = value
        else:
            for ref, cs_ in zip(buffers, copies):
                for c in cs_[step - 1]:
                    c.wait_recv()
                ref[near + 2 * (step - 1)] = over_hop(ref, step - 1)
        if step < steps - 1:
            for cs_ in copies:
                for c in cs_[step]:
                    c.start()

    def first_sums():
        for c in t_sum + t_inb:
            c.wait_recv()
        parts = []
        for r in range(brow):
            u = natural(r // prow) * prow + r % prow
            acc = ginb[r] + rinb[1, r]
            for s in range(2, group):
                acc += rinb[s, u]
            parts.append(acc)
        return over_tensor(tsum), jnp.stack(parts)

    def first_qv():
        for c in t_qv:
            c.wait_recv()
        return (over_tensor(tqv),)

    def reduce_sums(step):
        go(step, (sbuf, ibuf), (d_sum, d_inb), first_sums)

    def reduce_qv(step):
        go(step, (qbuf,), (d_qv,), first_qv)

    for c in t_sum + t_inb:
        c.start()

    @pl.loop(0, tiles, unroll=2)
    def _(n):
        a1[:, cols(n)] = dot_nt(a0[...], outw[cols(n), :]).astype(BF16)

    @pl.loop(0, tiles)
    def _(n):
        kt = k[n].T
        gt = a1[:, cols(n)].T.astype(F32)
        inner = jnp.sum((gt * mixt[n]).reshape(heads, hd, rows), axis=1)
        pairs = [(v[n, :, p * LANES : (p + 1) * LANES], gm) for p in range(TILE // LANES) for gm in halves(a1[:, cols(2 * n + p, LANES)])]
        dqs, dvh = [], []
        dprobs = [dot_nt(*pairs[0])]
        for h in range(heads):
            if h + 1 < heads:
                dprobs.append(dot_nt(*pairs[h + 1]))
            low = pt[n * heads + h]
            ds = (low.astype(F32) * (dprobs[h] - inner[h : h + 1])).astype(BF16)
            dvh.append(dot(low, pairs[h][1]))
            pt[n * heads + h] = ds
            dqs.append(dot(kt[h * hd : (h + 1) * hd], ds))
        dvs = [dvh[2 * p] + dvh[2 * p + 1] for p in range(TILE // LANES)]
        dq = (jnp.concatenate(dqs, axis=0) * hd**-0.5).astype(BF16).T
        dv = jnp.concatenate(dvs, axis=1).astype(BF16)
        hid[n] = dq
        v[n] = dv
        csqv[0, :, cols(n)] = fold8(dq.astype(F32))
        csqv[1, :, cols(n)] = fold8(dv.astype(F32))
        @pl.when(n == 0)
        def _():
            reduce_sums(0)

    for i in range(2):
        tqv[0, i : i + 1, :] = total8(csqv[i])
    for c in t_qv:
        c.start()

    @pl.loop(0, tiles, unroll=2)
    def _(n):
        dks = []
        for p in range(TILE // LANES):
            lo, hi = halves(q[n, :, p * LANES : (p + 1) * LANES])
            dks.append(dot(pt[n * heads + 2 * p], lo) + dot(pt[n * heads + 2 * p + 1], hi))
        k[n] = jnp.concatenate(dks, axis=1).astype(BF16)

    reduce_qv(0)

    @pl.loop(0, tiles, unroll=2)
    def _(t):
        acc = f2[:, cols(t)]
        for n in range(tiles):
            for i, ref in enumerate((hid, k, v)):
                acc += dot_nt(ref[n], qkvw[n + i * tiles, cols(t), :])
        f1[:, cols(t)] = acc
        pltpu.make_async_copy(f1.at[:, cols(t)], grad_out.at[:, cols(t)], lsem.at[20 + t]).start()

    for s in range(1, steps):
        reduce_sums(s)
        reduce_qv(s)
    last = near + 2 * (steps - 2)
    outs = [load(7, sbuf.at[last], sums_out), load(16, qbuf.at[last], qv_out), load(17, ibuf.at[last], inb_out)]

    for d in far:
        for c in direct[d] + to_x[d] + to_z[d] + list(pass_on[d].values()):
            c.wait_send()
    for c in core_in + [core_ffn] + bias + t_sum + t_inb + t_qv + sum(d_sum + d_inb + d_qv, []):
        c.wait_send()
    c_grad = [pltpu.make_async_copy(f1.at[:, cols(t)], grad_out.at[:, cols(t)], lsem.at[20 + t]) for t in range(tiles)]
    for c in [c_act] + c_grad + outs:
        c.wait()
    assert count[0] <= send.shape[0]


def finish(act, grad, sums, qv, inb, act_out, grad_out, qv_out, outb_out, shift1_out, inb_out, ffnb_out, shift2_out, abuf, gbuf, sbuf, qbuf, ibuf, into, out):
    pieces = 4
    size = act.shape[0] // pieces
    plan = [(sums, sbuf, None), (qv, qbuf, qv_out), (inb, ibuf, inb_out)]
    for i in range(pieces):
        r = pl.ds(i * size, size)
        plan.append((grad.at[r, :], gbuf.at[r, :], grad_out.at[r, :]))
        plan.append((act.at[r, :], abuf.at[r, :], act_out.at[r, :]))
    first = [pltpu.make_async_copy(src, mid, into.at[i]) for i, (src, mid, _) in enumerate(plan)]
    for c in first:
        c.start()
    second = []
    for i, (_, mid, dst) in enumerate(plan):
        first[i].wait()
        if dst is not None:
            second.append(pltpu.make_async_copy(mid, dst, out.at[i]))
            second[-1].start()
        else:
            for j, ref in enumerate((shift2_out, ffnb_out, shift1_out, outb_out)):
                second.append(pltpu.make_async_copy(mid.at[j : j + 1, :], ref, out.at[len(plan) + j]))
                second[-1].start()
    for c in second:
        c.wait()


def step(
    ranks, group,
    tokens, segments, separators, lengths, type_table, qkv_weight, qv_bias, out_weight, out_bias, gain_one, shift_one,
    in_weight, in_bias, ffn_weight, ffn_bias, gain_two, shift_two, cotangent,
):
    pairs, rows, width = tokens.shape
    units = in_weight.shape[1]
    hidden = units * group
    chunks, tiles = hidden // TILE, width // TILE
    brow = units // LANES
    line = group // 2
    near = min(ranks, 8)
    far_bits = (ranks // near).bit_length() - 1
    slots = near + 2 * far_bits + 1
    copies = (line - 1) * 36 + units // TILE + 1 + 4 * (group - 1) + 3 * (near - 1 + far_bits)
    vectors = (type_table, qv_bias, out_bias, gain_one, shift_one, ffn_bias, gain_two, shift_two)
    V = pltpu.VMEM
    outside = pl.BlockSpec(memory_space=pl.ANY)
    act, grad, sums, qv, inb = pl.pallas_call(
        functools.partial(kernel, ranks, group),
        out_shape=(
            jax.ShapeDtypeStruct((rows, width), BF16),
            jax.ShapeDtypeStruct((rows, width), F32),
            jax.ShapeDtypeStruct((4, width), F32),
            jax.ShapeDtypeStruct((2, width), F32),
            jax.ShapeDtypeStruct((brow, 1, LANES), F32),
        ),
        in_specs=[outside] * 17,
        out_specs=(outside,) * 5,
        scratch_shapes=[
            V((3 * tiles, width, TILE), BF16),
            V((width, width), BF16),
            V((chunks, width, TILE), BF16),
            V((hidden, width), BF16),
            V((hidden // LANES, 1, LANES), F32),
            V((tiles, rows, TILE), BF16),
            V((tiles, rows, TILE), BF16),
            V((tiles, rows, TILE), BF16),
            V((HEADS, rows, rows), BF16),
            V((chunks, rows, TILE), F32),
            V((chunks, rows, TILE), BF16),
            V((rows, width), BF16),
            V((rows, width), BF16),
            V((rows, width), F32),
            V((rows, width), F32),
            V((rows, width), F32),
            V((rows, width), BF16),
            V((rows, width), BF16),
            V((rows, LANES), F32),
            V((4, 8, width), F32),
            V((2, 8, width), F32),
            V((10, width), F32),
            V((hidden // LANES, 1, LANES), F32),
            V((group, brow, 1, LANES), F32),
            V((slots, brow, 1, LANES), F32),
            V((group, 4, width), F32),
            V((slots, 4, width), F32),
            V((group, 2, width), F32),
            V((slots, 2, width), F32),
            [V(x.shape, x.dtype) for x in vectors],
            [V((units,), BF16)] * group,
            pltpu.SMEM((1,), jnp.int32),
            pltpu.SMEM((1, 2), jnp.int32),
            V((rows, LANES), F32),
            V((tiles, TILE, rows), F32),
            pltpu.SemaphoreType.DMA((3 * tiles + units // TILE,)),
            pltpu.SemaphoreType.DMA((20 + tiles,)),
            pltpu.SemaphoreType.DMA((copies,)),
            pltpu.SemaphoreType.DMA((copies,)),
        ],
        compiler_params=pltpu.CompilerParams(collective_id=0, has_side_effects=True, vmem_limit_bytes=67043328),
    )(
        lengths,
        separators,
        *vectors,
        in_bias,
        tokens.reshape(rows, width),
        cotangent.reshape(rows, width),
        qkv_weight,
        out_weight,
        in_weight,
        ffn_weight,
    )
    vector = jax.ShapeDtypeStruct((1, width), F32)
    act, grad, qv, outb, shift1, inb, ffnb, shift2 = pl.pallas_call(
        finish,
        out_shape=(
            jax.ShapeDtypeStruct((rows, width), BF16),
            jax.ShapeDtypeStruct((rows, width), F32),
            jax.ShapeDtypeStruct((2, width), F32),
            vector,
            vector,
            jax.ShapeDtypeStruct((brow, 1, LANES), F32),
            vector,
            vector,
        ),
        in_specs=[outside] * 5,
        out_specs=(outside,) * 8,
        scratch_shapes=[
            V((rows, width), BF16),
            V((rows, width), F32),
            V((4, width), F32),
            V((2, width), F32),
            V((brow, 1, LANES), F32),
            pltpu.SemaphoreType.DMA((16,)),
            pltpu.SemaphoreType.DMA((16,)),
        ],
    )(act, grad, sums, qv, inb)
    return (
        act.reshape(pairs, rows, width),
        grad.reshape(pairs, rows, width),
        qv,
        outb.reshape(width),
        shift1.reshape(width),
        inb.reshape(units),
        ffnb.reshape(width),
        shift2.reshape(width),
    )


def solution(mesh):
    both = ("dp", "tensor")
    rows = P(both, None, None)
    return jax.shard_map(
        functools.partial(step, mesh.shape["dp"], mesh.shape["tensor"]),
        mesh=mesh,
        in_specs=(rows, P(both, None), P(both, None), P(both))
        + (P(),) * 7
        + (P(None, "tensor"), P("tensor"), P("tensor", None))
        + (P(),) * 3
        + (rows,),
        out_specs=(rows, rows, P(), P(), P(), P("tensor"), P(), P()),
        check_vma=False,
    )
```

```python
import functools

import jax
import jax.numpy as jnp
from jax import lax
from jax.experimental import pallas as pl
from jax.experimental.pallas import tpu as pltpu
from jax.sharding import PartitionSpec as P

HEADS = 16
TILE = 256
LANES = 128
BLOCK = 64
F32 = jnp.float32
BF16 = jnp.bfloat16
MESH = pl.DeviceIdType.MESH
NT = (((1,), (1,)), ((), ()))
root_half = 0.7071067811865476
inv_root_tau = 0.3989422804014327
eps_norm = 1e-06
STOP = 99


def dot(a, b):
    return jnp.dot(a, b, preferred_element_type=F32)


def dot_nt(a, b):
    return lax.dot_general(a, b, NT, preferred_element_type=F32)


def mean_rows(value):
    return jnp.sum(value, axis=-1, keepdims=True) * (1.0 / value.shape[-1])


def cols(n, size=TILE):
    return pl.ds(pl.multiple_of(n * size, size), size)


def fold8(value):
    return jnp.sum(value.reshape(value.shape[0] // 8, 8, value.shape[1]), axis=0)


def total8(value):
    return jnp.sum(value, axis=0, keepdims=True)


def flip(index, bit):
    return index + bit * (1 - 2 * (index // bit % 2))


def kernel(
    ranks, group,
    lengths, separators, table, qv_b, out_b, gain1, shift1, ffn_b, gain2, shift2, in_b, tokens, cot, qkv_w, out_w, in_w, ffn_w,
    act_out, grad_out, sums_out, qv_out, inb_out,
    qkvw, outw, inw, ffw, inb, q, k, v, pt, slope, hid, a0, a1, f0, f1, f2, tok, cotb, sc1, cs, csqv,
    small, ginb, rinb, ibuf, tsum, sbuf, tqv, qbuf,
    raw, inraw, len_s, sep_s, mask, mixt, wsem, lsem, send, recv,
):
    rows, width = tok.shape
    tiles = width // TILE
    hd = width // HEADS
    chunks = inw.shape[0]
    units = in_w.shape[1]
    part = units // 4
    line = group // 2
    brow = units // LANES
    prow = part // LANES
    per = units // TILE
    dp, tensor = lax.axis_index("dp"), lax.axis_index("tensor")
    y, core = tensor // 2, tensor % 2
    near = min(ranks, 8)
    bits = [1 << b for b in range(near.bit_length() - 1)]
    wide = [1 << b for b in range(ranks.bit_length() - 1) if 1 << b >= near]

    def place(d, other):
        return (dp, (y + d + line) % line * 2 + (core + other) % 2)

    def mixed(offset):
        return sum((offset // b + dp // b) % 2 * b for b in bits)

    def rank(offset):
        return (dp // near * near + mixed(offset) if offset < near else flip(dp, offset), tensor)

    barrier = pltpu.get_barrier_semaphore()
    friends = [place(s // 2, s % 2) for s in range(1, group)] + [rank(o) for o in list(range(1, near)) + wide]
    for f in friends:
        pl.semaphore_signal(barrier, inc=1, device_id=f, device_id_type=MESH)

    count = [0]

    def remote(src, dst, device):
        i = count[0]
        count[0] += 1
        return pltpu.make_async_remote_copy(
            src_ref=src, dst_ref=dst, send_sem=send.at[i], recv_sem=recv.at[i], device_id=device, device_id_type=MESH
        )

    def natural(p):
        return (p + dp) % 2 + (p // 2 + dp // 2) % 2 * 2

    cut = width // 4

    def piece(slot, p, i):
        u = slot * units + p * part
        if i == "in":
            return inw.at[u // TILE, :, pl.ds(u % TILE, part)]
        if i < 4:
            return inw.at[u // TILE, pl.ds(i * cut, cut), pl.ds(u % TILE, part)]
        return ffw.at[pl.ds(u + (i - 4) * part // 2, part // 2), :]

    def source(p, i):
        u = pl.multiple_of(natural(p) * part, part)
        if i < 4:
            return in_w.at[pl.ds(i * cut, cut), pl.ds(u, part)]
        return ffn_w.at[pl.ds(u + (i - 4) * part // 2, part // 2), :]

    def load(i, src, dst):
        c = pltpu.make_async_copy(src, dst, lsem.at[i])
        c.start()
        return c

    c_small = [load(8 + i, src, dst) for i, (src, dst) in enumerate(zip((table, qv_b, out_b, gain1, shift1, ffn_b, gain2, shift2), raw))]
    c_tok = load(0, tokens, tok)
    c_small += [load(18, lengths, len_s), load(19, separators, sep_s)]
    c_qkv = [pltpu.make_async_copy(qkv_w.at[:, n * TILE : (n + 1) * TILE], qkvw.at[n], wsem.at[n]) for n in range(3 * tiles)]
    for c in c_qkv[:tiles]:
        c.start()

    far = range(1, line)
    near_pieces = [(0, i) for i in range(6)]
    direct = {d: [remote(source(p, i), piece(2 * d, p, i), place(-d, 0)) for p, i in near_pieces + [(3, 4), (3, 5)]] for d in far}
    to_x = {d: [remote(piece(2 * d, p, i), piece(2 * d, p + 1, i), rank(1)) for p, i in near_pieces + [(2, 0), (2, 1)]] for d in far}
    to_z = {d: [remote(piece(2 * d, p, i), piece(2 * d, p + 2, i), rank(2)) for p, i in near_pieces + [(1, 2), (1, 3)]] for d in far}
    pass_on = {d: {(p, i): remote(piece(2 * d, p, i), piece(2 * d + 1, p, i), place(0, 1)) for p in range(4) for i in ("in", 4, 5)} for d in far}
    core_in = [remote(in_w.at[:, n * TILE : (n + 1) * TILE], inw.at[per + n], place(0, 1)) for n in range(per)]
    core_ffn = remote(ffn_w, ffw.at[pl.ds(units, units), :], place(0, 1))
    bias = [remote(in_b, inraw[s], place(-(s // 2), s % 2)) for s in range(1, group)]

    def relay(step):
        for d in far:
            yd, xd, zd, on = direct[d], to_x[d], to_z[d], pass_on[d]
            if step in range(6):
                yd[step].wait_recv()
                xd[step].start()
                zd[step].start()
                if step >= 3:
                    on[0, "in" if step == 3 else step].start()
            if step == "dx":
                zd[0].wait_recv()
                zd[1].wait_recv()
                xd[6].start()
                xd[7].start()
            if step == "dz":
                for i in range(4):
                    xd[i].wait_recv()
                zd[6].start()
                zd[7].start()
                on[1, "in"].start()
                zd[2].wait_recv()
                zd[3].wait_recv()
                on[2, "in"].start()
            if step == "diag":
                for i in (6, 7):
                    xd[i].wait_recv()
                    zd[i].wait_recv()
                on[3, "in"].start()
            if step in ("f4", "f5"):
                i = int(step[1])
                yd[i + 2].wait_recv()
                on[3, i].start()
                xd[i].wait_recv()
                on[1, i].start()
                zd[i].wait_recv()
                on[2, i].start()

    pl.semaphore_wait(barrier, len(friends))
    for c in bias:
        c.start()
    for d in far:
        for c in direct[d]:
            c.start()
    for c in c_qkv[tiles:]:
        c.start()
    for c in core_in + [core_ffn]:
        c.start()
    c_out = load(1, out_w, outw)
    c_in = [pltpu.make_async_copy(in_w.at[:, n * TILE : (n + 1) * TILE], inw.at[n], wsem.at[3 * tiles + n]) for n in range(per)]
    for c in c_in:
        c.start()
    c_b = load(3, in_b, inraw[0])
    c_ffn = load(2, ffn_w, ffw.at[pl.ds(0, units), :])
    c_cot = load(4, cot, cotb)

    for c in c_small:
        c.wait()
    length = len_s[0]
    sep0, sep1 = sep_s[0, 0], sep_s[0, 1]
    small[0:2, :] = raw[0][...].astype(F32)
    small[2:4, :] = raw[1][...].astype(F32)
    for i in range(2, 8):
        small[2 + i : 3 + i, :] = raw[i][...].astype(F32).reshape(1, width)
    c_tok.wait()

    @pl.loop(0, rows // BLOCK, unroll=2)
    def _(i):
        r = cols(i, BLOCK)
        pos = lax.broadcasted_iota(jnp.int32, (BLOCK, width), 0) + i * BLOCK
        second = (pos > sep0) & (pos < length)
        e = tok[r, :].astype(F32) + jnp.where(second, small[1:2, :], small[0:1, :])
        f0[r, :] = e
        a0[r, :] = e.astype(BF16)

    for c in c_qkv[:tiles]:
        c.wait()

    @pl.loop(0, tiles, unroll=2)
    def _(n):
        q[n] = (dot(a0[...], qkvw[n]) + small[2:3, cols(n)]).astype(BF16) * jnp.asarray(hd**-0.5, BF16)

    for c in c_qkv[tiles : 2 * tiles]:
        c.wait()

    @pl.loop(0, tiles, unroll=2)
    def _(n):
        k[n] = dot(a0[...], qkvw[n + tiles]).astype(BF16)

    @pl.when(core == 1)
    def _():
        relay(0)

    for c in c_qkv[2 * tiles :]:
        c.wait()

    @pl.loop(0, tiles, unroll=2)
    def _(n):
        v[n] = (dot(a0[...], qkvw[n + 2 * tiles]) + small[3:4, cols(n)]).astype(BF16)

    @pl.when(core == 0)
    def _():
        relay(0)

    mask[...] = jnp.where(lax.broadcasted_iota(jnp.int32, (rows, LANES), 0) < length, 0.0, -1e30)
    low_half = lax.broadcasted_iota(jnp.int32, (rows, LANES), 1) < hd
    zero = jnp.zeros((rows, LANES), BF16)
    heads = TILE // hd

    def halves(pair):
        return jnp.where(low_half, pair, zero), jnp.where(low_half, zero, pair)

    @pl.loop(0, tiles)
    def _(n):
        vt = v[n].T
        hide = jnp.concatenate([mask[...]] * (rows // LANES), axis=1)
        pairs = [(k[n, :, p * LANES : (p + 1) * LANES], qm) for p in range(TILE // LANES) for qm in halves(q[n, :, p * LANES : (p + 1) * LANES])]
        scores = [dot_nt(*pairs[0])]
        for h in range(heads):
            if h + 1 < heads:
                scores.append(dot_nt(*pairs[h + 1]))
            s = scores[h] + hide
            ex = jnp.exp(s - jnp.max(s, axis=0, keepdims=True))
            prob = (ex * (1.0 / jnp.sum(ex, axis=0, keepdims=True))).astype(BF16)
            pt[n * heads + h] = prob
            mixt[n, h * hd : (h + 1) * hd] = dot(vt[h * hd : (h + 1) * hd], prob)
        a1[:, cols(n)] = mixt[n].astype(BF16).T

        for i, at in enumerate((0, 1, 2)):

            @pl.when(n == at)
            def _(i=i):
                relay(i + 1)

    relay("dx")

    c_out.wait()

    @pl.loop(0, tiles, unroll=2)
    def _(n):
        f1[:, cols(n)] = dot(a1[...], outw[:, cols(n)]) + small[4:5, cols(n)] + f0[:, cols(n)]

    relay("dz")

    @pl.loop(0, rows // BLOCK, unroll=2)
    def _(i):
        r = cols(i, BLOCK)
        x = f1[r, :]
        x = x - mean_rows(x)
        scale = lax.rsqrt(mean_rows(x * x) + eps_norm)
        normed = x * scale
        f0[r, :] = normed
        a0[r, :] = (normed * small[5:6, :] + small[6:7, :]).astype(BF16)
        sc1[r, :] = jnp.broadcast_to(scale, (BLOCK, LANES))

    relay(4)

    def hidden_units(c, first, second):
        x = dot(a0[...], inw[c]) + jnp.concatenate([inb[first], inb[second]], axis=1)
        cdf = 0.5 * (1.0 + lax.erf(x * root_half))
        hid[c] = (x * cdf).astype(BF16)
        slope[c] = cdf + x * (inv_root_tau * jnp.exp(-0.5 * x * x))

    for c in c_in + [c_b]:
        c.wait()
    for c in core_in + bias:
        c.wait_recv()
    for t in range(group):
        b = inraw[t][...].astype(F32).reshape(1, units)
        for r in range(brow):
            inb[t * brow + r] = b[:, r * LANES : (r + 1) * LANES]

    @pl.loop(0, 2 * per, unroll=2)
    def _(c):
        hidden_units(c, 2 * c, 2 * c + 1)

    def shuffled(r):
        return r // brow * brow + natural(r % brow // prow) * prow + r % prow

    def units_of(i):
        for d in far:
            for p in range(4):
                if (p * part) // TILE == i:
                    pass_on[d][p, "in"].wait_recv()

        @pl.loop(2, group, unroll=2)
        def _(t):
            c = t * per + i
            hidden_units(c, shuffled(2 * c), shuffled(2 * c + 1))

    units_of(0)
    relay(5)
    for i in range(1, per - 1):
        units_of(i)
    relay("diag")
    c_ffn.wait()
    core_ffn.wait_recv()

    @pl.loop(0, tiles)
    def _(t):
        acc = dot(hid[0], ffw[0:TILE, cols(t)])
        for c in range(1, 2 * per):
            acc += dot(hid[c], ffw[c * TILE : (c + 1) * TILE, cols(t)])
        f1[:, cols(t)] = acc

    units_of(per - 1)
    relay("f4")

    half = part // 2
    blocks = [(t, p, h, t * units + p * part + h * half) for t in range(2, group) for p in range(4) for h in range(2)]

    def phase(t, p, h):
        if half % LANES:
            return 3
        return 2 * h + t % 2 if p else 0

    waves = [[u for t, p, h, u in blocks if phase(t, p, h) == w] for w in range(4)]

    def contract(t, acc, starts):
        step = max(1, TILE // half)
        for i in range(0, len(starts), step):
            us = starts[i : i + step]
            if us == list(range(us[0], us[0] + TILE, half)) and us[0] % TILE == 0:
                left, right = hid[us[0] // TILE], ffw[us[0] : us[0] + TILE, cols(t)]
            else:
                left = jnp.concatenate([hid[u // TILE, :, u % TILE : u % TILE + half] for u in us], axis=1)
                right = jnp.concatenate([ffw[u : u + half, cols(t)] for u in us], axis=0)
            acc += dot(left, right)
        return acc

    def add_wave(starts):
        if starts:

            @pl.loop(0, tiles, unroll=2)
            def _(t):
                f1[:, cols(t)] = contract(t, f1[:, cols(t)], starts)

    for d in far:
        pass_on[d][0, 4].wait_recv()
        pass_on[d][0, 5].wait_recv()
    add_wave(waves[0])
    for d in far:
        for p in range(1, 4):
            pass_on[d][p, 4].wait_recv()
    add_wave(waves[1])
    relay("f5")
    add_wave(waves[2])
    for d in far:
        for p in range(1, 4):
            pass_on[d][p, 5].wait_recv()
    add_wave(waves[3])

    c_cot.wait()
    cs[...] = jnp.zeros_like(cs)

    @pl.loop(0, rows // BLOCK, unroll=4)
    def _(i):
        r = cols(i, BLOCK)
        pos = lax.broadcasted_iota(jnp.int32, (BLOCK, 1), 0) + i * BLOCK
        keep = ((pos > 0) & (pos < length) & (pos != sep0) & (pos != sep1)).astype(F32)
        x = f0[r, :] * small[5:6, :] + small[6:7, :] + f1[r, :] + small[7:8, :]
        x = x - mean_rows(x)
        scale = lax.rsqrt(mean_rows(x * x) + eps_norm)
        normed = x * scale
        tok[r, :] = (normed * small[8:9, :] + small[9:10, :]).astype(BF16)
        g = cotb[r, :].astype(F32) * keep
        s = g * small[8:9, :]
        gs = scale * (s - mean_rows(s) - normed * mean_rows(s * normed))
        low = gs.astype(BF16)
        f2[r, :] = gs
        a1[r, :] = low
        cs[0] += fold8(g)
        cs[1] += fold8(low.astype(F32))

    c_act = load(5, tok, act_out)

    @pl.loop(0, chunks, unroll=8)
    def _(c):
        gi = (dot_nt(a1[...], ffw[cols(c), :]) * slope[c]).astype(BF16)
        hid[c] = gi
        s = total8(gi.astype(F32))
        ginb[2 * c] = s[:, :LANES]
        ginb[2 * c + 1] = s[:, LANES:]

    @pl.loop(0, tiles)
    def _(t):
        acc = dot_nt(hid[0], inw[0, cols(t), :])
        for c in range(1, chunks):
            acc += dot_nt(hid[c], inw[c, cols(t), :])
        f1[:, cols(t)] = acc

    @pl.loop(0, rows // BLOCK, unroll=4)
    def _(i):
        r = cols(i, BLOCK)
        g = f1[r, :] + f2[r, :]
        s = g * small[5:6, :]
        normed = f0[r, :]
        gs = sc1[r, 0:1] * (s - mean_rows(s) - normed * mean_rows(s * normed))
        low = gs.astype(BF16)
        f2[r, :] = gs
        a0[r, :] = low
        cs[2] += fold8(g)
        cs[3] += fold8(low.astype(F32))

    for i in range(4):
        tsum[0, i : i + 1, :] = total8(cs[i])
    peers = [(s, place(s // 2, s % 2)) for s in range(1, group)]
    t_sum = [remote(tsum.at[0], tsum.at[s], dev) for s, dev in peers]
    t_inb = [remote(ginb.at[pl.ds(s * brow, brow)], rinb.at[s], dev) for s, dev in peers]
    hops = [list(range(1, near))] + [[w] for w in wide]
    steps = len(hops) + 1

    def spread(ref):
        copies, base = [], 0
        for hop in hops:
            copies.append([remote(ref.at[base], ref.at[base + i + 1], rank(o)) for i, o in enumerate(hop)])
            base += len(hop) + 1
        return copies

    d_sum, d_inb, d_qv = spread(sbuf), spread(ibuf), spread(qbuf)
    t_qv = [remote(tqv.at[0], tqv.at[s], dev) for s, dev in peers]

    def over_tensor(ref):
        acc = None
        for t in range(group):
            s = (y - t // 2 + line) % line * 2 + (core + t) % 2
            acc = ref[s] if acc is None else acc + ref[s]
        return acc

    def over_hop(ref, hop):
        if hop == 0:
            acc = ref[mixed(0)]
            for o in range(1, near):
                acc += ref[mixed(o)]
            return acc
        base = near + 2 * (hop - 1)
        return ref[base] + ref[base + 1]

    def go(step, buffers, copies, totals):
        if step == 0:
            for ref, value in zip(buffers, totals()):
                ref[0] = value
        else:
            for ref, cs_ in zip(buffers, copies):
                for c in cs_[step - 1]:
                    c.wait_recv()
                ref[near + 2 * (step - 1)] = over_hop(ref, step - 1)
        if step < steps - 1:
            for cs_ in copies:
                for c in cs_[step]:
                    c.start()

    def first_sums():
        for c in t_sum + t_inb:
            c.wait_recv()
        parts = []
        for r in range(brow):
            u = natural(r // prow) * prow + r % prow
            acc = ginb[r] + rinb[1, r]
            for s in range(2, group):
                acc += rinb[s, u]
            parts.append(acc)
        return over_tensor(tsum), jnp.stack(parts)

    def first_qv():
        for c in t_qv:
            c.wait_recv()
        return (over_tensor(tqv),)

    def reduce_sums(step):
        go(step, (sbuf, ibuf), (d_sum, d_inb), first_sums)

    def reduce_qv(step):
        go(step, (qbuf,), (d_qv,), first_qv)

    for c in t_sum + t_inb:
        c.start()

    @pl.loop(0, tiles, unroll=2)
    def _(n):
        a1[:, cols(n)] = dot_nt(a0[...], outw[cols(n), :]).astype(BF16)

    @pl.loop(0, tiles)
    def _(n):
        kt = k[n].T
        gt = a1[:, cols(n)].T.astype(F32)
        inner = jnp.sum((gt * mixt[n]).reshape(heads, hd, rows), axis=1)
        pairs = [(v[n, :, p * LANES : (p + 1) * LANES], gm) for p in range(TILE // LANES) for gm in halves(a1[:, cols(2 * n + p, LANES)])]
        dqs, dvh = [], []
        dprobs = [dot_nt(*pairs[0])]
        for h in range(heads):
            if h + 1 < heads:
                dprobs.append(dot_nt(*pairs[h + 1]))
            low = pt[n * heads + h]
            ds = (low.astype(F32) * (dprobs[h] - inner[h : h + 1])).astype(BF16)
            dvh.append(dot(low, pairs[h][1]))
            pt[n * heads + h] = ds
            dqs.append(dot(kt[h * hd : (h + 1) * hd], ds))
        dvs = [dvh[2 * p] + dvh[2 * p + 1] for p in range(TILE // LANES)]
        dq = (jnp.concatenate(dqs, axis=0) * hd**-0.5).astype(BF16).T
        dv = jnp.concatenate(dvs, axis=1).astype(BF16)
        hid[n] = dq
        v[n] = dv
        csqv[0, :, cols(n)] = fold8(dq.astype(F32))
        csqv[1, :, cols(n)] = fold8(dv.astype(F32))
        @pl.when(n == 0)
        def _():
            reduce_sums(0)

    for i in range(2):
        tqv[0, i : i + 1, :] = total8(csqv[i])
    for c in t_qv:
        c.start()

    @pl.loop(0, tiles, unroll=4)
    def _(n):
        dks = []
        for p in range(TILE // LANES):
            lo, hi = halves(q[n, :, p * LANES : (p + 1) * LANES])
            dks.append(dot(pt[n * heads + 2 * p], lo) + dot(pt[n * heads + 2 * p + 1], hi))
        k[n] = jnp.concatenate(dks, axis=1).astype(BF16)

    reduce_qv(0)

    @pl.loop(0, tiles, unroll=4)
    def _(t):
        acc = f2[:, cols(t)]
        for n in range(tiles):
            for i, ref in enumerate((hid, k, v)):
                acc += dot_nt(ref[n], qkvw[n + i * tiles, cols(t), :])
        f1[:, cols(t)] = acc
        pltpu.make_async_copy(f1.at[:, cols(t)], grad_out.at[:, cols(t)], lsem.at[20 + t]).start()

    for s in range(1, steps):
        reduce_sums(s)
        reduce_qv(s)
    last = near + 2 * (steps - 2)
    outs = [load(7, sbuf.at[last], sums_out), load(16, qbuf.at[last], qv_out), load(17, ibuf.at[last], inb_out)]

    for d in far:
        for c in direct[d] + to_x[d] + to_z[d] + list(pass_on[d].values()):
            c.wait_send()
    for c in core_in + [core_ffn] + bias + t_sum + t_inb + t_qv + sum(d_sum + d_inb + d_qv, []):
        c.wait_send()
    c_grad = [pltpu.make_async_copy(f1.at[:, cols(t)], grad_out.at[:, cols(t)], lsem.at[20 + t]) for t in range(tiles)]
    for c in [c_act] + c_grad + outs:
        c.wait()
    assert count[0] <= send.shape[0]


def finish(act, grad, sums, qv, inb, act_out, grad_out, qv_out, outb_out, shift1_out, inb_out, ffnb_out, shift2_out, abuf, gbuf, sbuf, qbuf, ibuf, into, out):
    pieces = 4
    size = act.shape[0] // pieces
    plan = [(sums, sbuf, None), (qv, qbuf, qv_out), (inb, ibuf, inb_out)]
    for i in range(pieces):
        r = pl.ds(i * size, size)
        plan.append((grad.at[r, :], gbuf.at[r, :], grad_out.at[r, :]))
        plan.append((act.at[r, :], abuf.at[r, :], act_out.at[r, :]))
    first = [pltpu.make_async_copy(src, mid, into.at[i]) for i, (src, mid, _) in enumerate(plan)]
    for c in first:
        c.start()
    second = []
    for i, (_, mid, dst) in enumerate(plan):
        first[i].wait()
        if dst is not None:
            second.append(pltpu.make_async_copy(mid, dst, out.at[i]))
            second[-1].start()
        else:
            for j, ref in enumerate((shift2_out, ffnb_out, shift1_out, outb_out)):
                second.append(pltpu.make_async_copy(mid.at[j : j + 1, :], ref, out.at[len(plan) + j]))
                second[-1].start()
    for c in second:
        c.wait()


def step(
    ranks, group,
    tokens, segments, separators, lengths, type_table, qkv_weight, qv_bias, out_weight, out_bias, gain_one, shift_one,
    in_weight, in_bias, ffn_weight, ffn_bias, gain_two, shift_two, cotangent,
):
    pairs, rows, width = tokens.shape
    units = in_weight.shape[1]
    hidden = units * group
    chunks, tiles = hidden // TILE, width // TILE
    brow = units // LANES
    line = group // 2
    near = min(ranks, 8)
    far_bits = (ranks // near).bit_length() - 1
    slots = near + 2 * far_bits + 1
    copies = (line - 1) * 36 + units // TILE + 1 + 4 * (group - 1) + 3 * (near - 1 + far_bits)
    vectors = (type_table, qv_bias, out_bias, gain_one, shift_one, ffn_bias, gain_two, shift_two)
    V = pltpu.VMEM
    outside = pl.BlockSpec(memory_space=pl.ANY)
    act, grad, sums, qv, inb = pl.pallas_call(
        functools.partial(kernel, ranks, group),
        out_shape=(
            jax.ShapeDtypeStruct((rows, width), BF16),
            jax.ShapeDtypeStruct((rows, width), F32),
            jax.ShapeDtypeStruct((4, width), F32),
            jax.ShapeDtypeStruct((2, width), F32),
            jax.ShapeDtypeStruct((brow, 1, LANES), F32),
        ),
        in_specs=[outside] * 17,
        out_specs=(outside,) * 5,
        scratch_shapes=[
            V((3 * tiles, width, TILE), BF16),
            V((width, width), BF16),
            V((chunks, width, TILE), BF16),
            V((hidden, width), BF16),
            V((hidden // LANES, 1, LANES), F32),
            V((tiles, rows, TILE), BF16),
            V((tiles, rows, TILE), BF16),
            V((tiles, rows, TILE), BF16),
            V((HEADS, rows, rows), BF16),
            V((chunks, rows, TILE), F32),
            V((chunks, rows, TILE), BF16),
            V((rows, width), BF16),
            V((rows, width), BF16),
            V((rows, width), F32),
            V((rows, width), F32),
            V((rows, width), F32),
            V((rows, width), BF16),
            V((rows, width), BF16),
            V((rows, LANES), F32),
            V((4, 8, width), F32),
            V((2, 8, width), F32),
            V((10, width), F32),
            V((hidden // LANES, 1, LANES), F32),
            V((group, brow, 1, LANES), F32),
            V((slots, brow, 1, LANES), F32),
            V((group, 4, width), F32),
            V((slots, 4, width), F32),
            V((group, 2, width), F32),
            V((slots, 2, width), F32),
            [V(x.shape, x.dtype) for x in vectors],
            [V((units,), BF16)] * group,
            pltpu.SMEM((1,), jnp.int32),
            pltpu.SMEM((1, 2), jnp.int32),
            V((rows, LANES), F32),
            V((tiles, TILE, rows), F32),
            pltpu.SemaphoreType.DMA((3 * tiles + units // TILE,)),
            pltpu.SemaphoreType.DMA((20 + tiles,)),
            pltpu.SemaphoreType.DMA((copies,)),
            pltpu.SemaphoreType.DMA((copies,)),
        ],
        compiler_params=pltpu.CompilerParams(collective_id=0, has_side_effects=True, vmem_limit_bytes=67043328),
    )(
        lengths,
        separators,
        *vectors,
        in_bias,
        tokens.reshape(rows, width),
        cotangent.reshape(rows, width),
        qkv_weight,
        out_weight,
        in_weight,
        ffn_weight,
    )
    vector = jax.ShapeDtypeStruct((1, width), F32)
    act, grad, qv, outb, shift1, inb, ffnb, shift2 = pl.pallas_call(
        finish,
        out_shape=(
            jax.ShapeDtypeStruct((rows, width), BF16),
            jax.ShapeDtypeStruct((rows, width), F32),
            jax.ShapeDtypeStruct((2, width), F32),
            vector,
            vector,
            jax.ShapeDtypeStruct((brow, 1, LANES), F32),
            vector,
            vector,
        ),
        in_specs=[outside] * 5,
        out_specs=(outside,) * 8,
        scratch_shapes=[
            V((rows, width), BF16),
            V((rows, width), F32),
            V((4, width), F32),
            V((2, width), F32),
            V((brow, 1, LANES), F32),
            pltpu.SemaphoreType.DMA((16,)),
            pltpu.SemaphoreType.DMA((16,)),
        ],
    )(act, grad, sums, qv, inb)
    return (
        act.reshape(pairs, rows, width),
        grad.reshape(pairs, rows, width),
        qv,
        outb.reshape(width),
        shift1.reshape(width),
        inb.reshape(units),
        ffnb.reshape(width),
        shift2.reshape(width),
    )


def solution(mesh):
    both = ("dp", "tensor")
    rows = P(both, None, None)
    return jax.shard_map(
        functools.partial(step, mesh.shape["dp"], mesh.shape["tensor"]),
        mesh=mesh,
        in_specs=(rows, P(both, None), P(both, None), P(both))
        + (P(),) * 7
        + (P(None, "tensor"), P("tensor"), P("tensor", None))
        + (P(),) * 3
        + (rows,),
        out_specs=(rows, rows, P(), P(), P(), P("tensor"), P(), P()),
        check_vma=False,
    )
```

```python
import functools

import jax
import jax.numpy as jnp
from jax import lax
from jax.experimental import pallas as pl
from jax.experimental.pallas import tpu as pltpu
from jax.sharding import PartitionSpec as P

HEADS = 16
TILE = 256
LANES = 128
BLOCK = 64
F32 = jnp.float32
BF16 = jnp.bfloat16
MESH = pl.DeviceIdType.MESH
NT = (((1,), (1,)), ((), ()))
root_half = 0.7071067811865476
inv_root_tau = 0.3989422804014327
eps_norm = 1e-06
STOP = 99


def dot(a, b):
    return jnp.dot(a, b, preferred_element_type=F32)


def dot_nt(a, b):
    return lax.dot_general(a, b, NT, preferred_element_type=F32)


def mean_rows(value):
    return jnp.sum(value, axis=-1, keepdims=True) * (1.0 / value.shape[-1])


def cols(n, size=TILE):
    return pl.ds(pl.multiple_of(n * size, size), size)


def fold8(value):
    return jnp.sum(value.reshape(value.shape[0] // 8, 8, value.shape[1]), axis=0)


def total8(value):
    return jnp.sum(value, axis=0, keepdims=True)


def flip(index, bit):
    return index + bit * (1 - 2 * (index // bit % 2))


def kernel(
    ranks, group,
    lengths, separators, table, qv_b, out_b, gain1, shift1, ffn_b, gain2, shift2, in_b, tokens, cot, qkv_w, out_w, in_w, ffn_w,
    act_out, grad_out, sums_out, qv_out, inb_out,
    qkvw, outw, inw, ffw, inb, q, k, v, pt, slope, hid, a0, a1, f0, f1, f2, tok, cotb, sc1, cs, csqv,
    small, ginb, rinb, ibuf, tsum, sbuf, tqv, qbuf,
    raw, inraw, len_s, sep_s, mask, mixt, wsem, lsem, send, recv,
):
    rows, width = tok.shape
    tiles = width // TILE
    hd = width // HEADS
    chunks = inw.shape[0]
    units = in_w.shape[1]
    part = units // 4
    line = group // 2
    brow = units // LANES
    prow = part // LANES
    per = units // TILE
    dp, tensor = lax.axis_index("dp"), lax.axis_index("tensor")
    y, core = tensor // 2, tensor % 2
    near = min(ranks, 8)
    bits = [1 << b for b in range(near.bit_length() - 1)]
    wide = [1 << b for b in range(ranks.bit_length() - 1) if 1 << b >= near]

    def place(d, other):
        return (dp, (y + d + line) % line * 2 + (core + other) % 2)

    def mixed(offset):
        return sum((offset // b + dp // b) % 2 * b for b in bits)

    def rank(offset):
        return (dp // near * near + mixed(offset) if offset < near else flip(dp, offset), tensor)

    barrier = pltpu.get_barrier_semaphore()
    friends = [place(s // 2, s % 2) for s in range(1, group)] + [rank(o) for o in list(range(1, near)) + wide]
    for f in friends:
        pl.semaphore_signal(barrier, inc=1, device_id=f, device_id_type=MESH)

    sent, got = {}, {}

    def remote(src, dst, device, out, into):
        s = sent.setdefault(out, len(sent))
        r = got.setdefault(into, len(got))
        return pltpu.make_async_remote_copy(
            src_ref=src, dst_ref=dst, send_sem=send.at[s], recv_sem=recv.at[r], device_id=device, device_id_type=MESH
        )

    def all_here(name, ref):
        pltpu.make_async_copy(ref, ref, recv.at[got[name]]).wait()

    def all_gone(name, ref):
        pltpu.make_async_copy(ref, ref, send.at[sent[name]]).wait()

    def natural(p):
        return (p + dp) % 2 + (p // 2 + dp // 2) % 2 * 2

    cut = width // 4

    def piece(slot, p, i):
        u = slot * units + p * part
        if i in ("in", "top", "low"):
            r = pl.ds(width // 2 if i == "low" else 0, width if i == "in" else width // 2)
            return inw.at[u // TILE, r, pl.ds(u % TILE, part)]
        if i == "ffn":
            return ffw.at[pl.ds(u, part), :]
        if i < 4:
            return inw.at[u // TILE, pl.ds(i * cut, cut), pl.ds(u % TILE, part)]
        return ffw.at[pl.ds(u + (i - 4) * part // 2, part // 2), :]

    def source(p, i):
        u = pl.multiple_of(natural(p) * part, part)
        if i < 4:
            return in_w.at[pl.ds(i * cut, cut), pl.ds(u, part)]
        return ffn_w.at[pl.ds(u + (i - 4) * part // 2, part // 2), :]

    def loaded(i, ref):
        pltpu.make_async_copy(ref, ref, wsem.at[i]).wait()

    def load(i, src, dst):
        c = pltpu.make_async_copy(src, dst, lsem.at[i])
        c.start()
        return c

    c_small = [load(5 + i, src, dst) for i, (src, dst) in enumerate(zip((table, qv_b, out_b, gain1, shift1, ffn_b, gain2, shift2), raw))]
    c_tok = load(0, tokens, tok)
    c_small += [load(13, lengths, len_s), load(14, separators, sep_s)]
    c_qkv = [pltpu.make_async_copy(qkv_w.at[:, n * TILE : (n + 1) * TILE], qkvw.at[n], wsem.at[n // tiles]) for n in range(3 * tiles)]
    for c in c_qkv[:tiles]:
        c.start()

    far = range(1, line)
    near_pieces = [(0, i) for i in range(6)]
    direct, to_x, to_z, pass_on = {}, {}, {}, {}
    for d in far:
        e = 2 * d
        direct[d] = [
            remote(source(p, i), piece(e, p, i), place(-d, 0), "y", ("y", d, p, i)) for p, i in near_pieces + [(3, 4), (3, 5)]
        ]
        to_x[d] = [
            remote(piece(e, p, i), piece(e, p + 1, i), rank(1), "x", ("x", d, p, "in" if i < 4 else i))
            for p, i in near_pieces + [(2, 0), (2, 1)]
        ]
        to_z[d] = [
            remote(piece(e, p, i), piece(e, p + 2, i), rank(2), "z", ("z", d, p, i if i > 3 else "low" if i > 1 else "top"))
            for p, i in near_pieces + [(1, 2), (1, 3)]
        ]
        for p in range(4):
            for i in ("in", 4, 5):
                name = ("on", d, p, "ffn" if p == 0 and i != "in" else i)
                pass_on[d, p, i] = remote(piece(e, p, i), piece(e + 1, p, i), place(0, 1), "on", name)
    core_in = [remote(in_w.at[:, n * TILE : (n + 1) * TILE], inw.at[per + n], place(0, 1), "core", "core") for n in range(per)]
    core_ffn = remote(ffn_w, ffw.at[pl.ds(units, units), :], place(0, 1), "core", "core_ffn")
    bias = [remote(in_b, inraw[s], place(-(s // 2), s % 2), ("bias", s), ("bias", s)) for s in range(1, group)]

    def relay(step):
        for d in far:
            e = 2 * d
            yd, xd, zd = direct[d], to_x[d], to_z[d]
            if step in range(6):
                yd[step].wait_recv()
                xd[step].start()
                zd[step].start()
                if step >= 3:
                    pass_on[d, 0, "in" if step == 3 else step].start()
            if step == "dx":
                all_here(("z", d, 0, "top"), piece(e, 2, "top"))
                xd[6].start()
                xd[7].start()
            if step == "dz":
                all_here(("x", d, 0, "in"), piece(e, 1, "in"))
                zd[6].start()
                zd[7].start()
                pass_on[d, 1, "in"].start()
                all_here(("z", d, 0, "low"), piece(e, 2, "low"))
                pass_on[d, 2, "in"].start()
            if step == "diag":
                all_here(("x", d, 2, "in"), piece(e, 3, "top"))
                all_here(("z", d, 1, "low"), piece(e, 3, "low"))
                pass_on[d, 3, "in"].start()
            if step in ("f4", "f5"):
                i = int(step[1])
                yd[i + 2].wait_recv()
                pass_on[d, 3, i].start()
                xd[i].wait_recv()
                pass_on[d, 1, i].start()
                zd[i].wait_recv()
                pass_on[d, 2, i].start()

    pl.semaphore_wait(barrier, len(friends))
    for c in bias:
        c.start()
    for d in far:
        for c in direct[d]:
            c.start()
    for c in c_qkv[tiles:]:
        c.start()
    for c in core_in + [core_ffn]:
        c.start()
    c_out = load(1, out_w, outw)
    c_in = [pltpu.make_async_copy(in_w.at[:, n * TILE : (n + 1) * TILE], inw.at[n], wsem.at[3]) for n in range(per)]
    for c in c_in:
        c.start()
    c_b = load(3, in_b, inraw[0])
    c_ffn = load(2, ffn_w, ffw.at[pl.ds(0, units), :])
    c_cot = load(4, cot, cotb)

    for c in c_small:
        c.wait()
    length = len_s[0]
    sep0, sep1 = sep_s[0, 0], sep_s[0, 1]
    small[0:2, :] = raw[0][...].astype(F32)
    small[2:4, :] = raw[1][...].astype(F32)
    for i in range(2, 8):
        small[2 + i : 3 + i, :] = raw[i][...].astype(F32).reshape(1, width)
    c_tok.wait()

    @pl.loop(0, rows // BLOCK, unroll=2)
    def _(i):
        r = cols(i, BLOCK)
        pos = lax.broadcasted_iota(jnp.int32, (BLOCK, width), 0) + i * BLOCK
        second = (pos > sep0) & (pos < length)
        e = tok[r, :].astype(F32) + jnp.where(second, small[1:2, :], small[0:1, :])
        f0[r, :] = e
        a0[r, :] = e.astype(BF16)

    loaded(0, qkvw.at[pl.ds(0, tiles)])

    @pl.loop(0, tiles, unroll=2)
    def _(n):
        q[n] = (dot(a0[...], qkvw[n]) + small[2:3, cols(n)]).astype(BF16) * jnp.asarray(hd**-0.5, BF16)

    loaded(1, qkvw.at[pl.ds(tiles, tiles)])

    @pl.loop(0, tiles, unroll=2)
    def _(n):
        k[n] = dot(a0[...], qkvw[n + tiles]).astype(BF16)

    @pl.when(core == 1)
    def _():
        relay(0)

    loaded(2, qkvw.at[pl.ds(2 * tiles, tiles)])

    @pl.loop(0, tiles, unroll=2)
    def _(n):
        v[n] = (dot(a0[...], qkvw[n + 2 * tiles]) + small[3:4, cols(n)]).astype(BF16)

    @pl.when(core == 0)
    def _():
        relay(0)

    mask[...] = jnp.where(lax.broadcasted_iota(jnp.int32, (rows, LANES), 0) < length, 0.0, -1e30)
    low_half = lax.broadcasted_iota(jnp.int32, (rows, LANES), 1) < hd
    zero = jnp.zeros((rows, LANES), BF16)
    heads = TILE // hd

    def halves(pair):
        return jnp.where(low_half, pair, zero), jnp.where(low_half, zero, pair)

    @pl.loop(0, tiles)
    def _(n):
        vt = v[n].T
        hide = jnp.concatenate([mask[...]] * (rows // LANES), axis=1)
        pairs = [(k[n, :, p * LANES : (p + 1) * LANES], qm) for p in range(TILE // LANES) for qm in halves(q[n, :, p * LANES : (p + 1) * LANES])]
        scores = [dot_nt(*pairs[0])]
        for h in range(heads):
            if h + 1 < heads:
                scores.append(dot_nt(*pairs[h + 1]))
            s = scores[h] + hide
            ex = jnp.exp(s - jnp.max(s, axis=0, keepdims=True))
            prob = (ex * (1.0 / jnp.sum(ex, axis=0, keepdims=True))).astype(BF16)
            pt[n * heads + h] = prob
            mixt[n, h * hd : (h + 1) * hd] = dot(vt[h * hd : (h + 1) * hd], prob)
        a1[:, cols(n)] = mixt[n].astype(BF16).T

        for i, at in enumerate((0, 1, 2)):

            @pl.when(n == at)
            def _(i=i):
                relay(i + 1)

    relay("dx")

    c_out.wait()

    @pl.loop(0, tiles, unroll=2)
    def _(n):
        f1[:, cols(n)] = dot(a1[...], outw[:, cols(n)]) + small[4:5, cols(n)] + f0[:, cols(n)]

    relay("dz")

    @pl.loop(0, rows // BLOCK, unroll=2)
    def _(i):
        r = cols(i, BLOCK)
        x = f1[r, :]
        x = x - mean_rows(x)
        scale = lax.rsqrt(mean_rows(x * x) + eps_norm)
        normed = x * scale
        f0[r, :] = normed
        a0[r, :] = (normed * small[5:6, :] + small[6:7, :]).astype(BF16)
        sc1[r, :] = jnp.broadcast_to(scale, (BLOCK, LANES))

    relay(4)

    def hidden_units(c, first, second):
        x = dot(a0[...], inw[c]) + jnp.concatenate([inb[first], inb[second]], axis=1)
        cdf = 0.5 * (1.0 + lax.erf(x * root_half))
        hid[c] = (x * cdf).astype(BF16)
        slope[c] = cdf + x * (inv_root_tau * jnp.exp(-0.5 * x * x))

    loaded(3, inw.at[pl.ds(0, per)])
    c_b.wait()
    all_here("core", inw.at[pl.ds(per, per)])
    for c in bias:
        c.wait_recv()
    for t in range(group):
        b = inraw[t][...].astype(F32).reshape(1, units)
        for r in range(brow):
            inb[t * brow + r] = b[:, r * LANES : (r + 1) * LANES]

    @pl.loop(0, 2 * per, unroll=2)
    def _(c):
        hidden_units(c, 2 * c, 2 * c + 1)

    def shuffled(r):
        return r // brow * brow + natural(r % brow // prow) * prow + r % prow

    def units_of(i):
        for d in far:
            for p in range(4):
                if (p * part) // TILE == i:
                    pass_on[d, p, "in"].wait_recv()

        @pl.loop(2, group, unroll=2)
        def _(t):
            c = t * per + i
            hidden_units(c, shuffled(2 * c), shuffled(2 * c + 1))

    units_of(0)
    relay(5)
    for i in range(1, per - 1):
        units_of(i)
    relay("diag")
    c_ffn.wait()
    core_ffn.wait_recv()

    @pl.loop(0, tiles)
    def _(t):
        acc = dot(hid[0], ffw[0:TILE, cols(t)])
        for c in range(1, 2 * per):
            acc += dot(hid[c], ffw[c * TILE : (c + 1) * TILE, cols(t)])
        f1[:, cols(t)] = acc

    units_of(per - 1)
    relay("f4")

    half = part // 2
    blocks = [(t, p, h, t * units + p * part + h * half) for t in range(2, group) for p in range(4) for h in range(2)]

    def phase(t, p, h):
        if half % LANES:
            return 3
        return 2 * h + t % 2 if p else 0

    waves = [[u for t, p, h, u in blocks if phase(t, p, h) == w] for w in range(4)]

    def contract(t, acc, starts):
        step = max(1, TILE // half)
        for i in range(0, len(starts), step):
            us = starts[i : i + step]
            if us == list(range(us[0], us[0] + TILE, half)) and us[0] % TILE == 0:
                left, right = hid[us[0] // TILE], ffw[us[0] : us[0] + TILE, cols(t)]
            else:
                left = jnp.concatenate([hid[u // TILE, :, u % TILE : u % TILE + half] for u in us], axis=1)
                right = jnp.concatenate([ffw[u : u + half, cols(t)] for u in us], axis=0)
            acc += dot(left, right)
        return acc

    def add_wave(starts):
        if starts:

            @pl.loop(0, tiles, unroll=2)
            def _(t):
                f1[:, cols(t)] = contract(t, f1[:, cols(t)], starts)

    for d in far:
        all_here(("on", d, 0, "ffn"), piece(2 * d + 1, 0, "ffn"))
    add_wave(waves[0])
    for d in far:
        for p in range(1, 4):
            pass_on[d, p, 4].wait_recv()
    add_wave(waves[1])
    relay("f5")
    add_wave(waves[2])
    for d in far:
        for p in range(1, 4):
            pass_on[d, p, 5].wait_recv()
    add_wave(waves[3])

    c_cot.wait()
    cs[...] = jnp.zeros_like(cs)

    @pl.loop(0, rows // BLOCK, unroll=4)
    def _(i):
        r = cols(i, BLOCK)
        pos = lax.broadcasted_iota(jnp.int32, (BLOCK, 1), 0) + i * BLOCK
        keep = ((pos > 0) & (pos < length) & (pos != sep0) & (pos != sep1)).astype(F32)
        x = f0[r, :] * small[5:6, :] + small[6:7, :] + f1[r, :] + small[7:8, :]
        x = x - mean_rows(x)
        scale = lax.rsqrt(mean_rows(x * x) + eps_norm)
        normed = x * scale
        tok[r, :] = (normed * small[8:9, :] + small[9:10, :]).astype(BF16)
        g = cotb[r, :].astype(F32) * keep
        s = g * small[8:9, :]
        gs = scale * (s - mean_rows(s) - normed * mean_rows(s * normed))
        low = gs.astype(BF16)
        f2[r, :] = gs
        a1[r, :] = low
        cs[0] += fold8(g)
        cs[1] += fold8(low.astype(F32))

    c_act = load(4, tok, act_out)

    @pl.loop(0, chunks, unroll=8)
    def _(c):
        gi = (dot_nt(a1[...], ffw[cols(c), :]) * slope[c]).astype(BF16)
        hid[c] = gi
        s = total8(gi.astype(F32))
        ginb[2 * c] = s[:, :LANES]
        ginb[2 * c + 1] = s[:, LANES:]

    @pl.loop(0, tiles)
    def _(t):
        acc = dot_nt(hid[0], inw[0, cols(t), :])
        for c in range(1, chunks):
            acc += dot_nt(hid[c], inw[c, cols(t), :])
        f1[:, cols(t)] = acc

    @pl.loop(0, rows // BLOCK, unroll=4)
    def _(i):
        r = cols(i, BLOCK)
        g = f1[r, :] + f2[r, :]
        s = g * small[5:6, :]
        normed = f0[r, :]
        gs = sc1[r, 0:1] * (s - mean_rows(s) - normed * mean_rows(s * normed))
        low = gs.astype(BF16)
        f2[r, :] = gs
        a0[r, :] = low
        cs[2] += fold8(g)
        cs[3] += fold8(low.astype(F32))

    for i in range(4):
        tsum[0, i : i + 1, :] = total8(cs[i])
    peers = [(s, place(s // 2, s % 2)) for s in range(1, group)]
    t_sum = [remote(tsum.at[0], tsum.at[s], dev, "t_sum", "t_sum") for s, dev in peers]
    t_inb = [remote(ginb.at[pl.ds(s * brow, brow)], rinb.at[s], dev, "t_inb", "t_inb") for s, dev in peers]
    hops = [list(range(1, near))] + [[w] for w in wide]
    steps = len(hops) + 1

    bases = [0] + [near + 2 * i for i in range(len(wide))]

    def spread(name, ref):
        return [
            [remote(ref.at[base], ref.at[base + i + 1], rank(o), (name, base), (name, base)) for i, o in enumerate(hop)]
            for base, hop in zip(bases, hops)
        ]

    d_sum, d_inb, d_qv = spread("sum", sbuf), spread("inb", ibuf), spread("qv", qbuf)
    t_qv = [remote(tqv.at[0], tqv.at[s], dev, "t_qv", "t_qv") for s, dev in peers]
    others = pl.ds(1, group - 1)

    def over_tensor(ref):
        acc = None
        for t in range(group):
            s = (y - t // 2 + line) % line * 2 + (core + t) % 2
            acc = ref[s] if acc is None else acc + ref[s]
        return acc

    def over_hop(ref, hop):
        if hop == 0:
            acc = ref[mixed(0)]
            for o in range(1, near):
                acc += ref[mixed(o)]
            return acc
        base = near + 2 * (hop - 1)
        return ref[base] + ref[base + 1]

    def go(step, names, buffers, copies, totals):
        if step == 0:
            for ref, value in zip(buffers, totals()):
                ref[0] = value
        else:
            for name, ref in zip(names, buffers):
                base = bases[step - 1]
                all_here((name, base), ref.at[pl.ds(base + 1, len(hops[step - 1]))])
                ref[near + 2 * (step - 1)] = over_hop(ref, step - 1)
        if step < steps - 1:
            for cs_ in copies:
                for c in cs_[step]:
                    c.start()

    def first_sums():
        all_here("t_sum", tsum.at[others])
        all_here("t_inb", rinb.at[others])
        parts = []
        for r in range(brow):
            u = natural(r // prow) * prow + r % prow
            acc = ginb[r] + rinb[1, r]
            for s in range(2, group):
                acc += rinb[s, u]
            parts.append(acc)
        return over_tensor(tsum), jnp.stack(parts)

    def first_qv():
        all_here("t_qv", tqv.at[others])
        return (over_tensor(tqv),)

    def reduce_sums(step):
        go(step, ("sum", "inb"), (sbuf, ibuf), (d_sum, d_inb), first_sums)

    def reduce_qv(step):
        go(step, ("qv",), (qbuf,), (d_qv,), first_qv)

    for c in t_sum + t_inb:
        c.start()

    @pl.loop(0, tiles, unroll=2)
    def _(n):
        a1[:, cols(n)] = dot_nt(a0[...], outw[cols(n), :]).astype(BF16)

    @pl.loop(0, tiles)
    def _(n):
        kt = k[n].T
        gt = a1[:, cols(n)].T.astype(F32)
        inner = jnp.sum((gt * mixt[n]).reshape(heads, hd, rows), axis=1)
        pairs = [(v[n, :, p * LANES : (p + 1) * LANES], gm) for p in range(TILE // LANES) for gm in halves(a1[:, cols(2 * n + p, LANES)])]
        dqs, dvh = [], []
        dprobs = [dot_nt(*pairs[0])]
        for h in range(heads):
            if h + 1 < heads:
                dprobs.append(dot_nt(*pairs[h + 1]))
            low = pt[n * heads + h]
            ds = (low.astype(F32) * (dprobs[h] - inner[h : h + 1])).astype(BF16)
            dvh.append(dot(low, pairs[h][1]))
            pt[n * heads + h] = ds
            dqs.append(dot(kt[h * hd : (h + 1) * hd], ds))
        dvs = [dvh[2 * p] + dvh[2 * p + 1] for p in range(TILE // LANES)]
        dq = (jnp.concatenate(dqs, axis=0) * hd**-0.5).astype(BF16).T
        dv = jnp.concatenate(dvs, axis=1).astype(BF16)
        hid[n] = dq
        v[n] = dv
        csqv[0, :, cols(n)] = fold8(dq.astype(F32))
        csqv[1, :, cols(n)] = fold8(dv.astype(F32))
        @pl.when(n == 0)
        def _():
            reduce_sums(0)

    for i in range(2):
        tqv[0, i : i + 1, :] = total8(csqv[i])
    for c in t_qv:
        c.start()

    @pl.loop(0, tiles, unroll=4)
    def _(n):
        dks = []
        for p in range(TILE // LANES):
            lo, hi = halves(q[n, :, p * LANES : (p + 1) * LANES])
            dks.append(dot(pt[n * heads + 2 * p], lo) + dot(pt[n * heads + 2 * p + 1], hi))
        k[n] = jnp.concatenate(dks, axis=1).astype(BF16)

    reduce_qv(0)

    @pl.loop(0, tiles, unroll=4)
    def _(t):
        acc = f2[:, cols(t)]
        for n in range(tiles):
            for i, ref in enumerate((hid, k, v)):
                acc += dot_nt(ref[n], qkvw[n + i * tiles, cols(t), :])
        f1[:, cols(t)] = acc
        pltpu.make_async_copy(f1.at[:, cols(t)], grad_out.at[:, cols(t)], lsem.at[0]).start()

    for s in range(1, steps):
        reduce_sums(s)
        reduce_qv(s)
    last = near + 2 * (steps - 2)
    outs = [load(1, sbuf.at[last], sums_out), load(2, qbuf.at[last], qv_out), load(3, ibuf.at[last], inb_out)]

    hops_far = len(far)
    gone = {"y": 3 * part, "x": part * 5 // 2, "z": part * 5 // 2, "on": 8 * part}
    for name, size in gone.items():
        if hops_far:
            all_gone(name, ffw.at[pl.ds(0, size * hops_far), :])
    all_gone("core", ffw.at[pl.ds(0, 2 * units), :])
    for c in bias:
        c.wait_send()
    for name, ref in (("t_sum", tsum), ("t_inb", rinb), ("t_qv", tqv)):
        all_gone(name, ref.at[others])
    for base, hop in zip(bases, hops):
        for name, ref in (("sum", sbuf), ("inb", ibuf), ("qv", qbuf)):
            all_gone((name, base), ref.at[pl.ds(base + 1, len(hop))])
    pltpu.make_async_copy(f1, grad_out, lsem.at[0]).wait()
    for c in [c_act] + outs:
        c.wait()
    assert len(sent) == send.shape[0] and len(got) == recv.shape[0]


def finish(act, grad, sums, qv, inb, act_out, grad_out, qv_out, outb_out, shift1_out, inb_out, ffnb_out, shift2_out, abuf, gbuf, sbuf, qbuf, ibuf, into, out):
    pieces = 4
    size = act.shape[0] // pieces
    plan = [(sums, sbuf, None), (qv, qbuf, qv_out), (inb, ibuf, inb_out)]
    for i in range(pieces):
        r = pl.ds(i * size, size)
        plan.append((grad.at[r, :], gbuf.at[r, :], grad_out.at[r, :]))
        plan.append((act.at[r, :], abuf.at[r, :], act_out.at[r, :]))
    first = [pltpu.make_async_copy(src, mid, into.at[i]) for i, (src, mid, _) in enumerate(plan)]
    for c in first:
        c.start()
    second = []
    for i, (_, mid, dst) in enumerate(plan):
        first[i].wait()
        if dst is not None:
            second.append(pltpu.make_async_copy(mid, dst, out.at[i]))
            second[-1].start()
        else:
            for j, ref in enumerate((shift2_out, ffnb_out, shift1_out, outb_out)):
                second.append(pltpu.make_async_copy(mid.at[j : j + 1, :], ref, out.at[len(plan) + j]))
                second[-1].start()
    for c in second:
        c.wait()


def step(
    ranks, group,
    tokens, segments, separators, lengths, type_table, qkv_weight, qv_bias, out_weight, out_bias, gain_one, shift_one,
    in_weight, in_bias, ffn_weight, ffn_bias, gain_two, shift_two, cotangent,
):
    pairs, rows, width = tokens.shape
    units = in_weight.shape[1]
    hidden = units * group
    chunks, tiles = hidden // TILE, width // TILE
    brow = units // LANES
    line = group // 2
    near = min(ranks, 8)
    far_bits = (ranks // near).bit_length() - 1
    slots = near + 2 * far_bits + 1
    sends = 4 * (line > 1) + 1 + (group - 1) + 3 + 3 * (1 + far_bits)
    recvs = (line - 1) * 28 + 2 + (group - 1) + 3 + 3 * (1 + far_bits)
    vectors = (type_table, qv_bias, out_bias, gain_one, shift_one, ffn_bias, gain_two, shift_two)
    V = pltpu.VMEM
    outside = pl.BlockSpec(memory_space=pl.ANY)
    act, grad, sums, qv, inb = pl.pallas_call(
        functools.partial(kernel, ranks, group),
        out_shape=(
            jax.ShapeDtypeStruct((rows, width), BF16),
            jax.ShapeDtypeStruct((rows, width), F32),
            jax.ShapeDtypeStruct((4, width), F32),
            jax.ShapeDtypeStruct((2, width), F32),
            jax.ShapeDtypeStruct((brow, 1, LANES), F32),
        ),
        in_specs=[outside] * 17,
        out_specs=(outside,) * 5,
        scratch_shapes=[
            V((3 * tiles, width, TILE), BF16),
            V((width, width), BF16),
            V((chunks, width, TILE), BF16),
            V((hidden, width), BF16),
            V((hidden // LANES, 1, LANES), F32),
            V((tiles, rows, TILE), BF16),
            V((tiles, rows, TILE), BF16),
            V((tiles, rows, TILE), BF16),
            V((HEADS, rows, rows), BF16),
            V((chunks, rows, TILE), F32),
            V((chunks, rows, TILE), BF16),
            V((rows, width), BF16),
            V((rows, width), BF16),
            V((rows, width), F32),
            V((rows, width), F32),
            V((rows, width), F32),
            V((rows, width), BF16),
            V((rows, width), BF16),
            V((rows, LANES), F32),
            V((4, 8, width), F32),
            V((2, 8, width), F32),
            V((10, width), F32),
            V((hidden // LANES, 1, LANES), F32),
            V((group, brow, 1, LANES), F32),
            V((slots, brow, 1, LANES), F32),
            V((group, 4, width), F32),
            V((slots, 4, width), F32),
            V((group, 2, width), F32),
            V((slots, 2, width), F32),
            [V(x.shape, x.dtype) for x in vectors],
            [V((units,), BF16)] * group,
            pltpu.SMEM((1,), jnp.int32),
            pltpu.SMEM((1, 2), jnp.int32),
            V((rows, LANES), F32),
            V((tiles, TILE, rows), F32),
            pltpu.SemaphoreType.DMA((4,)),
            pltpu.SemaphoreType.DMA((15,)),
            pltpu.SemaphoreType.DMA((sends,)),
            pltpu.SemaphoreType.DMA((recvs,)),
        ],
        compiler_params=pltpu.CompilerParams(collective_id=0, has_side_effects=True, vmem_limit_bytes=67043328),
    )(
        lengths,
        separators,
        *vectors,
        in_bias,
        tokens.reshape(rows, width),
        cotangent.reshape(rows, width),
        qkv_weight,
        out_weight,
        in_weight,
        ffn_weight,
    )
    vector = jax.ShapeDtypeStruct((1, width), F32)
    act, grad, qv, outb, shift1, inb, ffnb, shift2 = pl.pallas_call(
        finish,
        out_shape=(
            jax.ShapeDtypeStruct((rows, width), BF16),
            jax.ShapeDtypeStruct((rows, width), F32),
            jax.ShapeDtypeStruct((2, width), F32),
            vector,
            vector,
            jax.ShapeDtypeStruct((brow, 1, LANES), F32),
            vector,
            vector,
        ),
        in_specs=[outside] * 5,
        out_specs=(outside,) * 8,
        scratch_shapes=[
            V((rows, width), BF16),
            V((rows, width), F32),
            V((4, width), F32),
            V((2, width), F32),
            V((brow, 1, LANES), F32),
            pltpu.SemaphoreType.DMA((11,)),
            pltpu.SemaphoreType.DMA((15,)),
        ],
    )(act, grad, sums, qv, inb)
    return (
        act.reshape(pairs, rows, width),
        grad.reshape(pairs, rows, width),
        qv,
        outb.reshape(width),
        shift1.reshape(width),
        inb.reshape(units),
        ffnb.reshape(width),
        shift2.reshape(width),
    )


def solution(mesh):
    both = ("dp", "tensor")
    rows = P(both, None, None)
    return jax.shard_map(
        functools.partial(step, mesh.shape["dp"], mesh.shape["tensor"]),
        mesh=mesh,
        in_specs=(rows, P(both, None), P(both, None), P(both))
        + (P(),) * 7
        + (P(None, "tensor"), P("tensor"), P("tensor", None))
        + (P(),) * 3
        + (rows,),
        out_specs=(rows, rows, P(), P(), P(), P("tensor"), P(), P()),
        check_vma=False,
    )
```
